8 devices in a mesh: tp: 4 (over z, y, x), dp: 2 (over core).
Axes of the slice: x: 2, y: 2, z: 1, core: 2. Of those that a mesh axis runs over, the one named last changes fastest.
Arguments:
- hidden_in: bfloat16 [4096, 2560], P('dp')
- targets: bfloat16 [4096, 2560], P('dp')
- w_up: bfloat16 [4, 2560, 10240], P(None, None, 'tp')
- w_down: bfloat16 [4, 10240, 2560], P(None, 'tp')
Outputs:
- output 1: float32 [4, 2560, 10240], P(None, None, 'tp')
- output 2: float32 [4, 10240, 2560], P(None, 'tp')
All inputs are finite; a program needn't handle non-finite values.
Results may differ from the reference program's by a relative error of at most 0.0121431.
Values are sent between devices in bfloat16 or wider.
A program may use at most 1.25 GiB of HBM per device.

```python
import math
import jax
import jax.numpy as jnp
from jax import lax

D = 2560
FF = 10240
TOKENS = 4096
BLOCK_ROWS = 512
LAYERS = 4


def setup_inputs(seed: int = 0) -> dict:
    keys = jax.random.split(jax.random.key(seed), 4)
    tgt_scale = 2.0 * math.sqrt(TOKENS)
    hidden_in = jax.random.normal(keys[0], (TOKENS, D), jnp.float32)
    targets = tgt_scale * jax.random.normal(keys[1], (TOKENS, D), jnp.float32)
    w_up = jax.random.normal(keys[2], (LAYERS, D, FF), jnp.float32) * (D ** -0.5)
    w_down = jax.random.normal(keys[3], (LAYERS, FF, D), jnp.float32) * (FF ** -0.5)
    return {"hidden_in": hidden_in.astype(jnp.bfloat16), "targets": targets.astype(jnp.bfloat16), "w_up": w_up.astype(jnp.bfloat16), "w_down": w_down.astype(jnp.bfloat16)}


def gelu_tanh(value):
    return jax.nn.gelu(value, approximate=True)


def block_grads(hidden, target, w_up, w_down):
    def fwd_layer(h_cur, weights):
        up_w, down_w = weights
        pre_act = jnp.dot(h_cur, up_w, preferred_element_type=jnp.float32).astype(jnp.bfloat16)
        act_val = gelu_tanh(pre_act.astype(jnp.float32)).astype(jnp.bfloat16)
        branch = jnp.dot(act_val, down_w, preferred_element_type=jnp.float32).astype(jnp.bfloat16)
        return h_cur + branch, (h_cur, pre_act, act_val)

    h_last, saved = lax.scan(fwd_layer, hidden, (w_up, w_down))
    err_f32 = (h_last.astype(jnp.float32) - target.astype(jnp.float32)) / TOKENS

    def bwd_layer(g_cur, layer_in):
        h_in, pre_act, act_val, up_w, down_w = layer_in
        g_down = jnp.dot(act_val.T, g_cur, preferred_element_type=jnp.float32)
        d_act = jnp.dot(g_cur, down_w.T, preferred_element_type=jnp.float32)
        _, gelu_vjp = jax.vjp(gelu_tanh, pre_act.astype(jnp.float32))
        d_pre = gelu_vjp(d_act)[0].astype(jnp.bfloat16)
        g_up = jnp.dot(h_in.T, d_pre, preferred_element_type=jnp.float32)
        back_sum = g_cur.astype(jnp.float32) + jnp.dot(d_pre, up_w.T, preferred_element_type=jnp.float32)
        return back_sum.astype(jnp.bfloat16), (g_up, g_down)

    _, grads = lax.scan(bwd_layer, err_f32.astype(jnp.bfloat16), (saved[0], saved[1], saved[2], w_up, w_down), reverse=True)
    return grads


def reference(hidden_in, targets, w_up, w_down):
    num_blocks = TOKENS // BLOCK_ROWS
    hid_blocks = hidden_in.reshape(num_blocks, BLOCK_ROWS, D)
    tgt_blocks = targets.reshape(num_blocks, BLOCK_ROWS, D)

    def accumulate(acc_grads, block_pair):
        g_up, g_down = block_grads(block_pair[0], block_pair[1], w_up, w_down)
        return (acc_grads[0] + g_up, acc_grads[1] + g_down), None

    zero_grads = (jnp.zeros((LAYERS, D, FF), jnp.float32), jnp.zeros((LAYERS, FF, D), jnp.float32))
    (grad_up, grad_down), _ = lax.scan(accumulate, zero_grads, (hid_blocks, tgt_blocks))
    return grad_up, grad_down
```

```python
import functools
import jax
import jax.numpy as jnp
from jax import lax
from jax.sharding import PartitionSpec as P

ROW_CONTRACT = (((0,), (0,)), ((), ()))
COL_CONTRACT = (((1,), (1,)), ((), ()))
CHUNKS = 2


def gelu_tanh(value):
    return jax.nn.gelu(value, approximate=True)


def dot_f32(lhs, rhs):
    return jnp.dot(lhs, rhs, preferred_element_type=jnp.float32)


def scatter_sum(part):
    return lax.psum_scatter(part, "tp", scatter_dimension=0, tiled=True)


def gather_rows(own):
    return lax.all_gather(own, "tp", axis=0, tiled=True)


def local_step(hidden, targets, w_up, w_down, total_tokens):
    layers = w_up.shape[0]
    tp = lax.axis_size("tp")
    me = lax.axis_index("tp")
    rows = hidden.shape[0] // CHUNKS
    own_rows = rows // tp

    def own_slice(arr, chunk):
        return lax.dynamic_slice_in_dim(arr, chunk * rows + me * own_rows, own_rows, 0)

    h_full = [hidden[c * rows:(c + 1) * rows] for c in range(CHUNKS)]
    h_own = [own_slice(hidden, c) for c in range(CHUNKS)]
    t_own = [own_slice(targets, c) for c in range(CHUNKS)]
    saved = []
    g_own = [None] * CHUNKS
    g_full = [None] * CHUNKS
    for layer in range(layers):
        keep = []
        nxt = [None] * CHUNKS
        for c in range(CHUNKS):
            pre = dot_f32(h_full[c], w_up[layer]).astype(jnp.bfloat16)
            act = gelu_tanh(pre.astype(jnp.float32)).astype(jnp.bfloat16)
            part = dot_f32(act, w_down[layer])
            branch = scatter_sum(part).astype(jnp.bfloat16)
            keep.append((h_full[c], pre, act))
            h_own[c] = h_own[c] + branch
            if layer < layers - 1:
                nxt[c] = gather_rows(h_own[c])
            else:
                err = (h_own[c].astype(jnp.float32) - t_own[c].astype(jnp.float32)) / total_tokens
                g_own[c] = err.astype(jnp.bfloat16)
                g_full[c] = gather_rows(g_own[c])
        saved.append(keep)
        h_full = nxt
    grads_up = [None] * layers
    grads_down = [None] * layers
    for layer in reversed(range(layers)):
        nxt = [None] * CHUNKS
        sum_down = 0.0
        sum_up = 0.0
        for c in range(CHUNKS):
            h_in, pre, act = saved[layer][c]
            d_act = lax.dot_general(g_full[c], w_down[layer], COL_CONTRACT, preferred_element_type=jnp.float32)
            _, gelu_vjp = jax.vjp(gelu_tanh, pre.astype(jnp.float32))
            d_pre = gelu_vjp(d_act)[0].astype(jnp.bfloat16)
            if layer > 0:
                back = lax.dot_general(d_pre, w_up[layer], COL_CONTRACT, preferred_element_type=jnp.float32)
                g_own[c] = (g_own[c].astype(jnp.float32) + scatter_sum(back)).astype(jnp.bfloat16)
                nxt[c] = gather_rows(g_own[c])
            saved[layer][c] = (h_in, d_pre, act, g_full[c])
        h_all, d_all, a_all, g_all = [jnp.concatenate([saved[layer][c][i] for c in range(CHUNKS)], 0) for i in range(4)]
        sum_down = lax.dot_general(a_all, g_all, ROW_CONTRACT, preferred_element_type=jnp.float32)
        sum_up = lax.dot_general(h_all, d_all, ROW_CONTRACT, preferred_element_type=jnp.float32)
        grads_down[layer] = lax.psum(sum_down, "dp")
        grads_up[layer] = lax.psum(sum_up, "dp")
        g_full = nxt
    return jnp.stack(grads_up), jnp.stack(grads_down)


def solution(mesh):
    def grad_step(hidden_in, targets, w_up, w_down):
        step_fn = functools.partial(local_step, total_tokens=hidden_in.shape[0])
        mapped = jax.shard_map(step_fn, mesh=mesh, in_specs=(P("dp", None), P("dp", None), P(None, None, "tp"), P(None, "tp", None)), out_specs=(P(None, None, "tp"), P(None, "tp", None)), check_vma=False)
        return mapped(hidden_in, targets, w_up, w_down)

    return grad_step
```

```python
import functools
import jax
import jax.numpy as jnp
from jax import lax
from jax.experimental import pallas as pl
from jax.experimental.pallas import tpu as pltpu
from jax.sharding import PartitionSpec as P

ROW_CONTRACT = (((0,), (0,)), ((), ()))
COL_CONTRACT = (((1,), (1,)), ((), ()))
MESH = pl.DeviceIdType.MESH
SLOTS = 4
TILE = 512
BWD_CHUNKS = 2
RED1_X, RED1_Y, RED2_X, RED2_Y, GAT1_X, GAT1_Y, GAT2_X, GAT2_Y = range(8)


def gelu_tanh(value):
    return jax.nn.gelu(value, approximate=True)


def dot_f32(lhs, rhs, dims=(((1,), (0,)), ((), ()))):
    return lax.dot_general(lhs, rhs, dims, preferred_element_type=jnp.float32)


def forward_kernel(layers, total_tokens, x_ref, t_ref, wu_ref, wd_ref, h_out, u_out, a_out, g_out,
                   hbuf, abuf, ubuf, wbuf, pbuf, tbuf, red1, red2, send_sem, recv_sem, w_sem, u_sem, a_sem, h_sem, t_sem):
    rows, d_model = hbuf.shape[1:]
    block = rows // 4
    half = block // 2
    tiles = d_model // TILE
    steps = layers * SLOTS
    me = lax.axis_index("tp")
    mx, my = me % 2, me // 2
    x_nbr = my * 2 + (1 - mx)
    y_nbr = (1 - my) * 2 + mx
    diag = (1 - my) * 2 + (1 - mx)

    def rows_of(owner, part=None):
        if part is None:
            return pl.ds(pl.multiple_of(owner * block, block), block)
        return pl.ds(pl.multiple_of(owner * block + part * half, half), half)

    def remote(kind, slot, src, dst, target):
        return pltpu.make_async_remote_copy(src_ref=src, dst_ref=dst, send_sem=send_sem.at[kind, slot], recv_sem=recv_sem.at[kind, slot], device_id={"tp": target}, device_id_type=MESH)

    def red1_copies(slot):
        return (remote(RED1_X, slot, pbuf.at[slot, rows_of(diag, 0)], red1.at[slot, 0], x_nbr),
                remote(RED1_Y, slot, pbuf.at[slot, rows_of(diag, 1)], red1.at[slot, 1], y_nbr))

    def red2_copies(slot):
        return (remote(RED2_X, slot, pbuf.at[slot, rows_of(x_nbr)], red2.at[slot, 0], x_nbr),
                remote(RED2_Y, slot, pbuf.at[slot, rows_of(y_nbr)], red2.at[slot, 1], y_nbr))

    def gat1_copies(slot):
        mine = hbuf.at[slot, rows_of(me)]
        return (remote(GAT1_X, slot, mine, mine, x_nbr), remote(GAT1_Y, slot, mine, mine, y_nbr))

    def gat2_copies(slot):
        from_y = hbuf.at[slot, rows_of(y_nbr, 0)]
        from_x = hbuf.at[slot, rows_of(x_nbr, 1)]
        return (remote(GAT2_X, slot, from_y, from_y, x_nbr), remote(GAT2_Y, slot, from_x, from_x, y_nbr))

    def w_copy(ref, layer, tile, slot):
        return pltpu.make_async_copy(ref.at[layer, :, pl.ds(pl.multiple_of(tile * TILE, TILE), TILE)], wbuf.at[slot], w_sem.at[slot])

    def chunk_rows(slot):
        return pl.ds(pl.multiple_of(slot * rows, rows), rows)

    def u_copy(layer, slot, tile, stage):
        return pltpu.make_async_copy(ubuf.at[stage], u_out.at[layer, chunk_rows(slot), pl.ds(pl.multiple_of(tile * TILE, TILE), TILE)], u_sem.at[stage])

    def a_copy(layer, slot, stage):
        return pltpu.make_async_copy(abuf.at[stage], a_out.at[layer, chunk_rows(slot)], a_sem.at[stage])

    def x_copy(slot):
        return pltpu.make_async_copy(x_ref.at[chunk_rows(slot)], hbuf.at[slot], h_sem.at[slot])

    def h_save(layer, slot):
        return pltpu.make_async_copy(hbuf.at[slot], h_out.at[layer, chunk_rows(slot)], h_sem.at[slot])

    def g_save(slot):
        return pltpu.make_async_copy(hbuf.at[slot], g_out.at[chunk_rows(slot)], h_sem.at[slot])

    def t_copy(slot):
        return pltpu.make_async_copy(t_ref.at[pl.ds(pl.multiple_of(slot * rows + me * block, block), block)], tbuf.at[slot % 2], t_sem.at[slot % 2])

    barrier = pltpu.get_barrier_semaphore()
    for target in (x_nbr, y_nbr):
        pl.semaphore_signal(barrier, inc=1, device_id={"tp": target}, device_id_type=MESH)

    for slot in range(SLOTS):
        x_copy(slot).start()
    w_copy(wu_ref, 0, 0, 0).start()
    w_copy(wu_ref, 0, 1, 1).start()
    pl.semaphore_wait(barrier, 2)

    def up_stage(n):
        layer, slot, stage = n // SLOTS, n % SLOTS, n % 2

        @pl.when(n < SLOTS)
        def _():
            x_copy(slot).wait()

        @pl.when(n >= SLOTS)
        def _():
            for copy in gat2_copies(slot):
                copy.wait()
            for copy in gat1_copies(slot):
                copy.wait_send()
            h_save(layer - 1, slot).start()

        @pl.when(n >= 2)
        def _():
            a_copy(layer, slot, stage).wait()

        def tile_step(tile, carry):
            count = n * 2 * tiles + tile
            nxt = (count + 2) % 3
            u_stage = (n * tiles + tile) % 2

            @pl.when(tile + 2 < tiles)
            def _():
                w_copy(wu_ref, layer, tile + 2, nxt).start()

            @pl.when(tile + 2 >= tiles)
            def _():
                w_copy(wd_ref, layer, tile + 2 - tiles, nxt).start()

            w_copy(wu_ref, layer, tile, count % 3).wait()
            pre = dot_f32(hbuf[slot], wbuf[count % 3]).astype(jnp.bfloat16)

            @pl.when(n * tiles + tile >= 2)
            def _():
                u_copy(layer, slot, tile, u_stage).wait()

            ubuf[u_stage] = pre
            abuf[stage, :, pl.ds(pl.multiple_of(tile * TILE, TILE), TILE)] = gelu_tanh(pre.astype(jnp.float32)).astype(jnp.bfloat16)
            u_copy(layer, slot, tile, u_stage).start()
            return carry

        lax.fori_loop(0, tiles, tile_step, 0)
        a_copy(layer, slot, stage).start()

    def down_stage(n):
        layer, slot, stage = n // SLOTS, n % SLOTS, n % 2

        def tile_step(tile, carry):
            count = n * 2 * tiles + tiles + tile
            nxt = (count + 2) % 3

            @pl.when(tile + 2 < tiles)
            def _():
                w_copy(wd_ref, layer, tile + 2, nxt).start()

            @pl.when((tile + 2 >= tiles) & (n + 1 < steps))
            def _():
                w_copy(wu_ref, (n + 1) // SLOTS, tile + 2 - tiles, nxt).start()

            w_copy(wd_ref, layer, tile, count % 3).wait()
            pbuf[slot, :, pl.ds(pl.multiple_of(tile * TILE, TILE), TILE)] = dot_f32(abuf[stage], wbuf[count % 3])
            return carry

        lax.fori_loop(0, tiles, tile_step, 0)

        @pl.when(n >= SLOTS)
        def _():
            h_save(layer - 1, slot).wait()

        for copy in red1_copies(slot):
            copy.start()

    def reduce_step(k):
        slot = k % SLOTS
        first, second = red1_copies(slot)
        first.wait_recv()
        pbuf[slot, rows_of(y_nbr, 0)] += red1[slot, 0]
        second.wait_recv()
        pbuf[slot, rows_of(x_nbr, 1)] += red1[slot, 1]
        for copy in red2_copies(slot):
            copy.start()

        @pl.when(k >= steps - SLOTS)
        def _():
            t_copy(slot).start()

    def finish_step(k):
        layer, slot = k // SLOTS, k % SLOTS
        for copy in red2_copies(slot):
            copy.wait()
        for copy in red1_copies(slot):
            copy.wait_send()
        branch = (pbuf[slot, rows_of(me)] + red2[slot, 0] + red2[slot, 1]).astype(jnp.bfloat16)
        h_new = (hbuf[slot, rows_of(me)].astype(jnp.float32) + branch.astype(jnp.float32)).astype(jnp.bfloat16)

        @pl.when(layer < layers - 1)
        def _():
            hbuf[slot, rows_of(me)] = h_new

        @pl.when(layer == layers - 1)
        def _():
            t_copy(slot).wait()
            err = (h_new.astype(jnp.float32) - tbuf[slot % 2].astype(jnp.float32)) * (1.0 / total_tokens)
            hbuf[slot, rows_of(me)] = err.astype(jnp.bfloat16)

        for copy in gat1_copies(slot):
            copy.start()

    def forward_step(k):
        slot = k % SLOTS
        for copy in gat1_copies(slot):
            copy.wait_recv()
        for copy in gat2_copies(slot):
            copy.start()

    def when_step(k, fn):
        @pl.when((k >= 0) & (k < steps))
        def _():
            fn(k)

    def body(n, carry):
        when_step(n, up_stage)
        when_step(n - 1, reduce_step)
        when_step(n - 3, forward_step)
        when_step(n, down_stage)
        when_step(n - 1, finish_step)
        return carry

    lax.fori_loop(0, steps + 3, body, 0)
    for slot in range(SLOTS):
        for copy in gat2_copies(slot):
            copy.wait()
        for copy in gat1_copies(slot):
            copy.wait_send()
        g_save(slot).start()
    for stage in range(2):
        u_copy(0, 0, 0, stage).wait()
        a_copy(0, 0, stage).wait()
    for slot in range(SLOTS):
        g_save(slot).wait()


def run_forward(hidden, targets, w_up, w_down, total_tokens):
    layers, d_model, width = w_up.shape
    tokens = hidden.shape[0]
    rows = tokens // SLOTS
    block = rows // 4
    bf16, f32 = jnp.bfloat16, jnp.float32
    flops = 4 * layers * tokens * d_model * width
    anywhere = pl.BlockSpec(memory_space=pl.ANY)
    return pl.pallas_call(
        functools.partial(forward_kernel, layers, total_tokens),
        out_shape=(jax.ShapeDtypeStruct((layers - 1, tokens, d_model), bf16), jax.ShapeDtypeStruct((layers, tokens, width), bf16),
                   jax.ShapeDtypeStruct((layers, tokens, width), bf16), jax.ShapeDtypeStruct((tokens, d_model), bf16)),
        in_specs=[anywhere] * 4,
        out_specs=(anywhere,) * 4,
        scratch_shapes=[
            pltpu.VMEM((SLOTS, rows, d_model), bf16),
            pltpu.VMEM((2, rows, width), bf16),
            pltpu.VMEM((2, rows, TILE), bf16),
            pltpu.VMEM((3, d_model, TILE), bf16),
            pltpu.VMEM((SLOTS, rows, d_model), f32),
            pltpu.VMEM((2, block, d_model), bf16),
            pltpu.VMEM((SLOTS, 2, block // 2, d_model), f32),
            pltpu.VMEM((SLOTS, 2, block, d_model), f32),
            pltpu.SemaphoreType.DMA((8, SLOTS)),
            pltpu.SemaphoreType.DMA((8, SLOTS)),
            pltpu.SemaphoreType.DMA((3,)),
            pltpu.SemaphoreType.DMA((2,)),
            pltpu.SemaphoreType.DMA((2,)),
            pltpu.SemaphoreType.DMA((SLOTS,)),
            pltpu.SemaphoreType.DMA((2,)),
        ],
        compiler_params=pltpu.CompilerParams(collective_id=0, has_side_effects=True, vmem_limit_bytes=67043328),
        cost_estimate=pl.CostEstimate(flops=flops, bytes_accessed=layers * tokens * d_model * 8, transcendentals=layers * tokens * width),
        name="forward_chain",
    )(hidden, targets, w_up, w_down)


def scatter_sum(part):
    return lax.psum_scatter(part, "tp", scatter_dimension=0, tiled=True)


def gather_rows(own):
    return lax.all_gather(own, "tp", axis=0, tiled=True)


def swap(value):
    return lax.ppermute(value, "dp", [(0, 1), (1, 0)])


def empty_kernel(out_ref):
    del out_ref


def empty_array(shape, dtype):
    return pl.pallas_call(empty_kernel, out_shape=jax.ShapeDtypeStruct(shape, dtype), out_specs=pl.BlockSpec(memory_space=pl.ANY))()


def local_step(hidden, targets, w_up, w_down, total_tokens):
    layers, d_model, width = w_up.shape
    tp = lax.axis_size("tp")
    me = lax.axis_index("tp")
    core = lax.axis_index("dp")
    half = width // 2
    rows = hidden.shape[0] // BWD_CHUNKS
    own_rows = rows // tp

    def my_half(arr):
        return lax.dynamic_slice_in_dim(arr, core * half, half, 1)

    def other_half(arr):
        return lax.dynamic_slice_in_dim(arr, (1 - core) * half, half, 1)

    h_mid, pre_all, act_all, g_last = run_forward(hidden, targets, w_up, w_down, total_tokens)
    g_full = [g_last[c * rows:(c + 1) * rows] for c in range(BWD_CHUNKS)]
    g_own = [lax.dynamic_slice_in_dim(g_last, c * rows + me * own_rows, own_rows, 0) for c in range(BWD_CHUNKS)]
    grad_up = empty_array((layers, d_model, width), jnp.float32)
    grad_down = empty_array((layers, width, d_model), jnp.float32)
    for layer in reversed(range(layers)):
        nxt = [None] * BWD_CHUNKS
        d_pres = [None] * BWD_CHUNKS
        h_all = hidden if layer == 0 else h_mid[layer - 1]
        a_all = act_all[layer]
        a_other = swap(other_half(a_all))
        h_other = swap(h_all)
        for c in range(BWD_CHUNKS):
            pre = pre_all[layer, c * rows:(c + 1) * rows]
            d_act = dot_f32(g_full[c], w_down[layer], COL_CONTRACT)
            _, gelu_vjp = jax.vjp(gelu_tanh, pre.astype(jnp.float32))
            d_pres[c] = gelu_vjp(d_act)[0].astype(jnp.bfloat16)
            if layer > 0:
                back = dot_f32(d_pres[c], w_up[layer], COL_CONTRACT)
                g_own[c] = (g_own[c].astype(jnp.float32) + scatter_sum(back)).astype(jnp.bfloat16)
                nxt[c] = gather_rows(g_own[c])
        g_all = g_last if layer == layers - 1 else jnp.concatenate(g_full, 0)
        d_all = jnp.concatenate(d_pres, 0)
        g_other = swap(g_all)
        d_other = swap(other_half(d_all))
        mine_down = dot_f32(my_half(a_all), g_all, ROW_CONTRACT) + dot_f32(a_other, g_other, ROW_CONTRACT)
        mine_up = dot_f32(h_all, my_half(d_all), ROW_CONTRACT) + dot_f32(h_other, d_other, ROW_CONTRACT)
        far_down = swap(mine_down)
        far_up = swap(mine_up)
        grad_down = lax.dynamic_update_slice(grad_down, mine_down[None], (layer, core * half, 0))
        grad_down = lax.dynamic_update_slice(grad_down, far_down[None], (layer, (1 - core) * half, 0))
        grad_up = lax.dynamic_update_slice(grad_up, mine_up[None], (layer, 0, core * half))
        grad_up = lax.dynamic_update_slice(grad_up, far_up[None], (layer, 0, (1 - core) * half))
        g_full = nxt
    return grad_up, grad_down


def solution(mesh):
    def grad_step(hidden_in, targets, w_up, w_down):
        step_fn = functools.partial(local_step, total_tokens=hidden_in.shape[0])
        mapped = jax.shard_map(step_fn, mesh=mesh, in_specs=(P("dp", None), P("dp", None), P(None, None, "tp"), P(None, "tp", None)), out_specs=(P(None, None, "tp"), P(None, "tp", None)), check_vma=False)
        return mapped(hidden_in, targets, w_up, w_down)

    return grad_step
```

```python
import functools
import jax
import jax.numpy as jnp
from jax import lax
from jax.experimental import pallas as pl
from jax.experimental.pallas import tpu as pltpu
from jax.sharding import PartitionSpec as P

ROW_CONTRACT = (((0,), (0,)), ((), ()))
COL_CONTRACT = (((1,), (1,)), ((), ()))
MESH = pl.DeviceIdType.MESH
SLOTS = 4
TILE = 512
RED1_X, RED1_Y, RED2_X, RED2_Y, GAT1_X, GAT1_Y, GAT2_X, GAT2_Y = range(8)


def gelu_tanh(value):
    return jax.nn.gelu(value, approximate=True)


def dot_f32(lhs, rhs, dims=(((1,), (0,)), ((), ()))):
    return lax.dot_general(lhs, rhs, dims, preferred_element_type=jnp.float32)


PUSH_A, PUSH_D, PUSH_G, PUSH_H = range(4)


def chain_kernel(layers, total_tokens, x_ref, t_ref, wu_ref, wd_ref,
                 h_out, u_out, a_out, g_out, du_out, td_out, tu_out, pa_out, pd_out, pg_out, ph_out, pa0_out, pd0_out,
                 hbuf, abuf, ubuf, wbuf, pbuf, tbuf, red1, red2, acc, ops,
                 send_sem, recv_sem, push_send, push_recv, res_send, res_recv, w_sem, u_sem, a_sem, h_sem, t_sem, l_sem, o_sem):
    rows, d_model = hbuf.shape[1:]
    block = rows // 4
    half = block // 2
    tiles = d_model // TILE
    side_w = d_model // 2
    turn = layers * SLOTS
    steps = turn + (layers - 1) * SLOTS
    every = steps + SLOTS
    top = layers - 1
    granules = 2 * (layers - 1) * 2 * SLOTS
    me = lax.axis_index("tp")
    core = lax.axis_index("dp")
    peer = 1 - core
    mx, my = me % 2, me // 2
    x_nbr = my * 2 + (1 - mx)
    y_nbr = (1 - my) * 2 + mx
    diag = (1 - my) * 2 + (1 - mx)

    def rows_of(owner, part=None):
        if part is None:
            return pl.ds(pl.multiple_of(owner * block, block), block)
        return pl.ds(pl.multiple_of(owner * block + part * half, half), half)

    def chunk_rows(slot):
        return pl.ds(pl.multiple_of(slot * rows, rows), rows)

    def half_of(which):
        return pl.ds(pl.multiple_of(which * side_w, side_w), side_w)

    def tile_of(tile):
        return pl.ds(pl.multiple_of(tile * TILE, TILE), TILE)

    def layer_of(n):
        back = n // turn
        return (1 - back) * (n // SLOTS) + back * (2 * layers - 1 - n // SLOTS)

    def remote(kind, k, src, dst, target):
        return pltpu.make_async_remote_copy(src_ref=src, dst_ref=dst, send_sem=send_sem.at[kind, k % SLOTS], recv_sem=recv_sem.at[kind, k % SLOTS], device_id={"tp": target}, device_id_type=MESH)

    def red1_copies(k):
        return (remote(RED1_X, k, pbuf.at[k % 2, rows_of(diag, 0)], red1.at[k % 2, 0], x_nbr),
                remote(RED1_Y, k, pbuf.at[k % 2, rows_of(diag, 1)], red1.at[k % 2, 1], y_nbr))

    def red2_copies(k):
        return (remote(RED2_X, k, pbuf.at[k % 2, rows_of(x_nbr)], red2.at[k % 2, 0], x_nbr),
                remote(RED2_Y, k, pbuf.at[k % 2, rows_of(y_nbr)], red2.at[k % 2, 1], y_nbr))

    def gat1_copies(k):
        mine = hbuf.at[k % SLOTS, rows_of(me)]
        return (remote(GAT1_X, k, mine, mine, x_nbr), remote(GAT1_Y, k, mine, mine, y_nbr))

    def gat2_copies(k):
        from_y = hbuf.at[k % SLOTS, rows_of(y_nbr, 0)]
        from_x = hbuf.at[k % SLOTS, rows_of(x_nbr, 1)]
        return (remote(GAT2_X, k, from_y, from_y, x_nbr), remote(GAT2_Y, k, from_x, from_x, y_nbr))

    def push(kind, layer, slot, src, dst):
        return pltpu.make_async_remote_copy(src_ref=src, dst_ref=dst, send_sem=push_send.at[kind, layer, slot], recv_sem=push_recv.at[kind, layer, slot], device_id={"dp": peer}, device_id_type=MESH)

    def push_a(layer, slot):
        return push(PUSH_A, layer, slot, abuf.at[:, half_of(peer)], pa_out.at[layer, chunk_rows(slot)])

    def push_d(layer, slot):
        return push(PUSH_D, layer, slot, abuf.at[:, half_of(peer)], pd_out.at[layer, chunk_rows(slot)])

    def push_a0(slot):
        return push(PUSH_A, 0, slot, abuf, pa0_out.at[chunk_rows(slot)])

    def push_d0(slot):
        return push(PUSH_D, 0, slot, abuf, pd0_out.at[chunk_rows(slot)])

    def push_g(layer, slot):
        return push(PUSH_G, layer, slot, hbuf.at[slot], pg_out.at[layer, chunk_rows(slot)])

    def push_h(layer, slot):
        return push(PUSH_H, layer, slot, hbuf.at[slot], ph_out.at[layer, chunk_rows(slot)])

    def weight_copy(ref, layer, tile, stage):
        return pltpu.make_async_copy(ref.at[layer, tile_of(tile)], wbuf.at[stage], w_sem.at[stage])

    def weight_start(index):
        main = steps * 2 * tiles
        n, place = index // (2 * tiles), index % (2 * tiles)
        up = 1 - place // tiles
        use_up = (1 - n // turn) * up + (n // turn) * (1 - up)

        @pl.when((index < main) & (use_up == 1))
        def _():
            weight_copy(wu_ref, layer_of(n), place % tiles, index % 3).start()

        @pl.when((index < main) & (use_up == 0))
        def _():
            weight_copy(wd_ref, layer_of(n), place % tiles, index % 3).start()

        @pl.when((index >= main) & (index < main + SLOTS * tiles))
        def _():
            weight_copy(wd_ref, 0, (index - main) % tiles, index % 3).start()

    def weight_wait(index):
        weight_copy(wu_ref, 0, 0, index % 3).wait()

    def weight_base(n):
        late = (n // steps) * (n - steps)
        return (n - late) * 2 * tiles + late * tiles

    def u_save(n, tile, stage):
        return pltpu.make_async_copy(ubuf.at[stage], u_out.at[layer_of(n), chunk_rows(n % SLOTS), tile_of(tile)], u_sem.at[stage])

    def u_load(n, tile, stage):
        return pltpu.make_async_copy(u_out.at[layer_of(n), chunk_rows(n % SLOTS), tile_of(tile)], ubuf.at[stage], u_sem.at[stage])

    def x_load(slot):
        return pltpu.make_async_copy(x_ref.at[chunk_rows(slot)], hbuf.at[slot], h_sem.at[slot])

    def h_save(layer, slot):
        return pltpu.make_async_copy(hbuf.at[slot], h_out.at[layer - 1, chunk_rows(slot)], h_sem.at[slot])

    def g_save(layer, slot):
        return pltpu.make_async_copy(hbuf.at[slot], g_out.at[layer, chunk_rows(slot)], h_sem.at[slot])

    def a_save(layer, slot):
        return pltpu.make_async_copy(abuf, a_out.at[layer, chunk_rows(slot)], a_sem)

    def d_save(layer, slot):
        return pltpu.make_async_copy(abuf, du_out.at[layer, chunk_rows(slot)], a_sem)

    def t_load(slot):
        return pltpu.make_async_copy(t_ref.at[pl.ds(pl.multiple_of(slot * rows + me * block, block), block)], tbuf, t_sem)

    def half_load(src, side):
        return pltpu.make_async_copy(src, ops.at[side, 0], l_sem.at[side, 0])

    def full_load(src, side, part):
        return pltpu.make_async_copy(src.at[:, pl.ds(part * side_w, side_w)], ops.at[side, 1 + part], l_sem.at[side, 1 + part])

    def out_copy(dst, part):
        return pltpu.make_async_copy(acc.at[part], dst, o_sem.at[part])

    def out_push(dst, index, part):
        return pltpu.make_async_remote_copy(src_ref=acc.at[part], dst_ref=dst, send_sem=res_send.at[index, part], recv_sem=res_recv.at[index, part], device_id={"dp": peer}, device_id_type=MESH)

    def td_part(layer, part):
        return td_out.at[layer - 1, half_of(core), pl.ds(part * side_w, side_w)]

    def tu_part(layer, part):
        return tu_out.at[layer - 1, pl.ds(part * side_w, side_w), half_of(core)]

    def load_granule(q):
        index = q // (2 * SLOTS)
        kind, layer, slot, side = index % 2, top - index // 2, (q % (2 * SLOTS)) // 2, q % 2

        def start(half_src, full_src):
            half_load(half_src, side).start()
            for part in range(2):
                full_load(full_src, side, part).start()

        @pl.when((kind == 0) & (side == 0))
        def _():
            start(a_out.at[layer, chunk_rows(slot), half_of(core)], g_out.at[layer, chunk_rows(slot)])

        @pl.when((kind == 0) & (side == 1))
        def _():
            push_a(layer, slot).wait_recv()
            push_g(layer, slot).wait_recv()
            start(pa_out.at[layer, chunk_rows(slot)], pg_out.at[layer, chunk_rows(slot)])

        @pl.when((kind == 1) & (side == 0))
        def _():
            start(du_out.at[layer, chunk_rows(slot), half_of(core)], h_out.at[layer - 1, chunk_rows(slot)])

        @pl.when((kind == 1) & (side == 1))
        def _():
            push_d(layer, slot).wait_recv()
            push_h(layer, slot).wait_recv()
            start(pd_out.at[layer, chunk_rows(slot)], ph_out.at[layer, chunk_rows(slot)])

    def wait_outs(index):
        for part in range(2):
            out_copy(td_part(1, part), part).wait()
            out_push(td_part(1, part), index, part).wait_send()

    def run_granule(q):
        index = q // (2 * SLOTS)
        kind, layer, side = index % 2, top - index // 2, q % 2

        @pl.when((q % (2 * SLOTS) == 0) & (q > 0))
        def _():
            wait_outs(index - 1)

        @pl.when(q % (2 * SLOTS) == 0)
        def _():
            def clear(i, carry):
                strip = pl.ds(pl.multiple_of(i * 64, 64), 64)
                acc[:, strip, :] = jnp.zeros((2, 64, side_w), jnp.float32)
                return carry

            lax.fori_loop(0, side_w // 64, clear, 0)

        half_load(pa_out.at[0, chunk_rows(0)], side).wait()
        for part in range(2):
            full_load(pg_out.at[0, chunk_rows(0)], side, part).wait()

        def part_step(i, carry):
            part, strip = i // 2, pl.ds(pl.multiple_of(i % 2 * (side_w // 2), side_w // 2), side_w // 2)
            acc[part, strip] += dot_f32(ops[side, kind * (1 + part), :, strip], ops[side, (1 - kind) * (1 + part)], ROW_CONTRACT)
            return carry

        lax.fori_loop(0, 4, part_step, 0)

        @pl.when((q % (2 * SLOTS) == 2 * SLOTS - 1) & (kind == 0))
        def _():
            for part in range(2):
                out_copy(td_part(layer, part), part).start()
                out_push(td_part(layer, part), index, part).start()

        @pl.when((q % (2 * SLOTS) == 2 * SLOTS - 1) & (kind == 1))
        def _():
            for part in range(2):
                out_copy(tu_part(layer, part), part).start()
                out_push(tu_part(layer, part), index, part).start()

    def granule_of(b, i):
        return 4 * b - 4 + i - 2 * ((b + 13) // 16) - 2 * ((b + 12) // 16)

    def granule_runs(b, i):
        q = granule_of(b, i)
        return (b >= 1) & (q < granules) & (((b != 2) & (b != 3)) | (i < 2))

    def granule_load(n, i):
        @pl.when((i < 4) & granule_runs(n - turn, i))
        def _():
            load_granule(granule_of(n - turn, i))

    def granules_of(n, first, last):
        def step(i, carry):
            granule_load(n, i + 1)

            @pl.when(granule_runs(n - turn, i))
            def _():
                run_granule(granule_of(n - turn, i))

            return carry

        lax.fori_loop(first, last, step, 0)

    def receive_rows(n):
        layer, slot = layer_of(n), n % SLOTS

        @pl.when(n < SLOTS)
        def _():
            x_load(slot).wait()

        @pl.when(n >= SLOTS)
        def _():
            for copy in gat2_copies(n):
                copy.wait()
            for copy in gat1_copies(n):
                copy.wait_send()

        @pl.when(n < turn)
        def _():
            push_h(layer, slot).start()

        @pl.when((n >= SLOTS) & (n < turn))
        def _():
            h_save(layer, slot).start()

        @pl.when(n >= turn)
        def _():
            push_g(layer, slot).start()
            g_save(layer, slot).start()

    def settle_rows(n):
        layer, slot = layer_of(n), n % SLOTS

        @pl.when(n < turn)
        def _():
            push_h(layer, slot).wait_send()

        @pl.when((n >= SLOTS) & (n < turn))
        def _():
            h_save(layer, slot).wait()

        @pl.when(n >= turn)
        def _():
            push_g(layer, slot).wait_send()
            g_save(layer, slot).wait()

    def settle_acts(n):
        layer, slot = layer_of(n), n % SLOTS
        a_save(layer, slot).wait()

        @pl.when(n < SLOTS)
        def _():
            push_a0(slot).wait_send()

        @pl.when((n >= SLOTS) & (n < turn))
        def _():
            push_a(layer, slot).wait_send()

        @pl.when((n >= turn) & (n < steps))
        def _():
            push_d(layer, slot).wait_send()

        @pl.when(n >= steps)
        def _():
            push_d0(slot).wait_send()

    def accumulate(n, first, source):
        def row_step(tile, carry):
            index = first + tile
            weight_start(index + 2)
            weight_wait(index)

            def column_step(j, carry):
                part = dot_f32(source(tile), wbuf[index % 3, :, tile_of(j)])

                @pl.when(tile == 0)
                def _():
                    pbuf[n % 2, :, tile_of(j)] = part

                @pl.when(tile > 0)
                def _():
                    pbuf[n % 2, :, tile_of(j)] += part

                return carry

            lax.fori_loop(0, tiles, column_step, 0)
            return carry

        lax.fori_loop(0, tiles, row_step, 0)

    def forward_up(n):
        layer, slot = layer_of(n), n % SLOTS
        accumulate(n, weight_base(n), lambda tile: hbuf[slot, :, tile_of(tile)])

        def act_step(tile, carry):
            count = n * tiles + tile

            @pl.when(count >= 2)
            def _():
                u_save(0, 0, count % 2).wait()

            pre = pbuf[n % 2, :, tile_of(tile)].astype(jnp.bfloat16)
            ubuf[count % 2] = pre
            abuf[:, tile_of(tile)] = gelu_tanh(pre.astype(jnp.float32)).astype(jnp.bfloat16)
            u_save(n, tile, count % 2).start()
            return carry

        lax.fori_loop(0, tiles, act_step, 0)
        a_save(layer, slot).start()

        @pl.when(n < SLOTS)
        def _():
            push_a0(slot).start()

        @pl.when(n >= SLOTS)
        def _():
            push_a(layer, slot).start()

    def forward_down(n):
        accumulate(n, weight_base(n) + tiles, lambda tile: abuf[:, tile_of(tile)])

    def backward_up(n):
        layer, slot = layer_of(n), n % SLOTS

        @pl.when(n == turn)
        def _():
            for stage in range(2):
                u_save(0, 0, stage).wait()
            u_load(n, 0, n * tiles % 2).start()

        def tile_step(tile, carry):
            index = weight_base(n) + tile
            count = n * tiles + tile
            weight_start(index + 2)

            @pl.when(count + 1 < every * tiles)
            def _():
                u_load((count + 1) // tiles, (count + 1) % tiles, (count + 1) % 2).start()

            weight_wait(index)
            u_load(n, tile, count % 2).wait()
            d_act = dot_f32(hbuf[slot], wbuf[index % 3], COL_CONTRACT)
            _, gelu_vjp = jax.vjp(gelu_tanh, ubuf[count % 2].astype(jnp.float32))
            abuf[:, tile_of(tile)] = gelu_vjp(d_act)[0].astype(jnp.bfloat16)
            return carry

        lax.fori_loop(0, tiles, tile_step, 0)
        d_save(layer, slot).start()

        @pl.when(n < steps)
        def _():
            push_d(layer, slot).start()

        @pl.when(n >= steps)
        def _():
            push_d0(slot).start()

    def backward_down(n):
        def tile_step(tile, carry):
            index = weight_base(n) + tiles + tile
            weight_start(index + 2)
            weight_wait(index)
            pbuf[n % 2, :, tile_of(tile)] = dot_f32(abuf[...], wbuf[index % 3], COL_CONTRACT)
            return carry

        lax.fori_loop(0, tiles, tile_step, 0)

    def send_diagonal(n):
        for copy in red1_copies(n):
            copy.start()

    def reduce_step(k):
        first, second = red1_copies(k)
        first.wait_recv()
        pbuf[k % 2, rows_of(y_nbr, 0)] += red1[k % 2, 0]
        second.wait_recv()
        pbuf[k % 2, rows_of(x_nbr, 1)] += red1[k % 2, 1]
        for copy in red2_copies(k):
            copy.start()

        @pl.when((k >= turn - SLOTS) & (k < turn))
        def _():
            t_load(k % SLOTS).start()

    def finish_step(k):
        slot = k % SLOTS
        for copy in red2_copies(k):
            copy.wait()
        for copy in red1_copies(k):
            copy.wait_send()

        def total():
            return pbuf[k % 2, rows_of(me)] + red2[k % 2, 0] + red2[k % 2, 1]

        def h_new():
            return (hbuf[slot, rows_of(me)].astype(jnp.float32) + total().astype(jnp.bfloat16).astype(jnp.float32)).astype(jnp.bfloat16)

        @pl.when(k < turn - SLOTS)
        def _():
            hbuf[slot, rows_of(me)] = h_new()

        @pl.when((k >= turn - SLOTS) & (k < turn))
        def _():
            t_load(slot).wait()
            err = (h_new().astype(jnp.float32) - tbuf[...].astype(jnp.float32)) * (1.0 / total_tokens)
            hbuf[slot, rows_of(me)] = err.astype(jnp.bfloat16)

        @pl.when(k >= turn)
        def _():
            hbuf[slot, rows_of(me)] = (hbuf[slot, rows_of(me)].astype(jnp.float32) + total()).astype(jnp.bfloat16)

        for copy in gat1_copies(k):
            copy.start()

    def forward_rows(k):
        for copy in gat1_copies(k):
            copy.wait_recv()
        for copy in gat2_copies(k):
            copy.start()

    def when_step(k, fn):
        @pl.when((k >= 0) & (k < steps))
        def _():
            fn(k)

    barrier = pltpu.get_barrier_semaphore()
    for target in ({"tp": x_nbr}, {"tp": y_nbr}, {"dp": peer}):
        pl.semaphore_signal(barrier, inc=1, device_id=target, device_id_type=MESH)
    x_load(0).start()
    weight_copy(wu_ref, 0, 0, 0).start()
    weight_copy(wu_ref, 0, 1, 1).start()
    for slot in range(1, SLOTS):
        x_load(slot).start()
    pl.semaphore_wait(barrier, 3)

    def body(n, carry):
        receive_rows(n)

        @pl.when(n >= 1)
        def _():
            settle_acts(n - 1)

        @pl.when(n < turn)
        def _():
            forward_up(n)

        @pl.when(n >= turn)
        def _():
            backward_up(n)

        when_step(n - 2, forward_rows)
        settle_rows(n)
        granule_load(n, 0)

        @pl.when(n < turn)
        def _():
            forward_down(n)

        @pl.when((n >= turn) & (n < steps))
        def _():
            backward_down(n)

        when_step(n, send_diagonal)
        granules_of(n, 0, 1)
        when_step(n - 1, finish_step)
        granules_of(n, 1, 3)
        when_step(n, reduce_step)
        granules_of(n, 3, 4)
        return carry

    lax.fori_loop(0, every, body, 0)
    settle_acts(every - 1)
    wait_outs(2 * (layers - 1) - 1)
    for slot in range(SLOTS):
        push_a0(slot).wait_recv()
        push_d0(slot).wait_recv()
        push_g(0, slot).wait_recv()
        push_h(0, slot).wait_recv()
    for index in range(2 * (layers - 1)):
        for part in range(2):
            out_push(td_part(1, part), index, part).wait_recv()


def run_chain(hidden, targets, w_up, w_down, total_tokens):
    layers, d_model, width = w_up.shape
    tokens = hidden.shape[0]
    rows = tokens // SLOTS
    block = rows // 4
    half = width // 2
    bf16, f32 = jnp.bfloat16, jnp.float32
    flops = 2 * tokens * d_model * width * (6 * layers - 3)
    anywhere = pl.BlockSpec(memory_space=pl.ANY)
    like = jax.ShapeDtypeStruct
    outs = (like((layers - 1, tokens, d_model), bf16), like((layers, tokens, width), bf16), like((layers, tokens, width), bf16),
            like((layers, tokens, d_model), bf16), like((layers, tokens, width), bf16),
            like((layers - 1, width, d_model), f32), like((layers - 1, d_model, width), f32),
            like((layers, tokens, half), bf16), like((layers, tokens, half), bf16),
            like((layers, tokens, d_model), bf16), like((layers, tokens, d_model), bf16),
            like((tokens, width), bf16), like((tokens, width), bf16))
    return pl.pallas_call(
        functools.partial(chain_kernel, layers, total_tokens),
        out_shape=outs,
        in_specs=[anywhere] * 4,
        out_specs=(anywhere,) * len(outs),
        scratch_shapes=[
            pltpu.VMEM((SLOTS, rows, d_model), bf16),
            pltpu.VMEM((rows, width), bf16),
            pltpu.VMEM((2, rows, TILE), bf16),
            pltpu.VMEM((3, TILE, d_model), bf16),
            pltpu.VMEM((2, rows, d_model), f32),
            pltpu.VMEM((block, d_model), bf16),
            pltpu.VMEM((2, 2, block // 2, d_model), f32),
            pltpu.VMEM((2, 2, block, d_model), f32),
            pltpu.VMEM((2, half, half), f32),
            pltpu.VMEM((2, 3, rows, half), bf16),
            pltpu.SemaphoreType.DMA((8, SLOTS)),
            pltpu.SemaphoreType.DMA((8, SLOTS)),
            pltpu.SemaphoreType.DMA((4, layers, SLOTS)),
            pltpu.SemaphoreType.DMA((4, layers, SLOTS)),
            pltpu.SemaphoreType.DMA((2 * (layers - 1), 2)),
            pltpu.SemaphoreType.DMA((2 * (layers - 1), 2)),
            pltpu.SemaphoreType.DMA((3,)),
            pltpu.SemaphoreType.DMA((2,)),
            pltpu.SemaphoreType.DMA,
            pltpu.SemaphoreType.DMA((SLOTS,)),
            pltpu.SemaphoreType.DMA,
            pltpu.SemaphoreType.DMA((2, 3)),
            pltpu.SemaphoreType.DMA((2,)),
        ],
        compiler_params=pltpu.CompilerParams(collective_id=0, has_side_effects=True, vmem_limit_bytes=67043328),
        cost_estimate=pl.CostEstimate(flops=flops, bytes_accessed=layers * tokens * d_model * 16, transcendentals=2 * layers * tokens * width),
        name="step_chain",
    )(hidden, targets, w_up, w_down)


def final_kernel(a_ref, pa_ref, g_ref, pg_ref, x_ref, px_ref, d_ref, pd_ref, td_ref, tu_ref, gd_out, gu_out, acc, lhs, rhs, ring, l_sem, r_sem, o_sem, in_sem, out_sem):
    rows, side_w = lhs.shape[2:]
    strip = ring.shape[1]
    depth = ring.shape[0]
    done_layers, height, _ = td_ref.shape
    per_layer = height // strip
    per_array = done_layers * per_layer
    strips = 2 * per_array
    lag = depth // 2
    core = lax.axis_index("dp")
    a_ref, g_ref, pg_ref, px_ref, d_ref = (ref.at[0] for ref in (a_ref, g_ref, pg_ref, px_ref, d_ref))
    parts = 4
    granules = 4 * SLOTS
    per_grad = granules // 2

    def chunk_rows(slot):
        return pl.ds(pl.multiple_of(slot * rows, rows), rows)

    def half_of(which):
        return pl.ds(pl.multiple_of(which * side_w, side_w), side_w)

    def operand_copies(left, right, slot, stage):
        for part in range(2):
            cols = pl.ds(part * side_w, side_w)
            yield pltpu.make_async_copy(left.at[chunk_rows(slot), cols], lhs.at[stage, part], l_sem.at[stage, part])
            yield pltpu.make_async_copy(right.at[chunk_rows(slot), cols], rhs.at[stage, part], r_sem.at[stage, part])

    def load(q):
        grad, slot, side = q // per_grad, (q % per_grad) // 2, q % 2
        for which, mine, theirs in ((0, (a_ref, g_ref), (pa_ref, pg_ref)), (1, (x_ref, d_ref), (px_ref, pd_ref))):
            @pl.when((grad == which) & (side == core))
            def _():
                for copy in operand_copies(*mine, slot, q % 2):
                    copy.start()

            @pl.when((grad == which) & (side != core))
            def _():
                for copy in operand_copies(*theirs, slot, q % 2):
                    copy.start()

    def out_copy(dst, part):
        return pltpu.make_async_copy(acc.at[part], dst.at[0, half_of(part // 2), half_of(part % 2)], o_sem.at[part])

    def strip_copies(t, src, dst):
        layer, row = (t % per_array) // per_layer, pl.multiple_of((t % per_layer) * strip, strip)
        return (pltpu.make_async_copy(src.at[layer, pl.ds(row, strip)], ring.at[t % depth], in_sem.at[t % depth]),
                pltpu.make_async_copy(ring.at[t % depth], dst.at[layer + 1, pl.ds(row, strip)], out_sem.at[t % depth]))

    def move(t):
        @pl.when((t >= depth) & (t < strips + depth))
        def _():
            strip_copies(t - depth, td_ref, gd_out)[1].wait()

        @pl.when(t < per_array)
        def _():
            strip_copies(t, td_ref, gd_out)[0].start()

        @pl.when((t >= per_array) & (t < strips))
        def _():
            strip_copies(t, tu_ref, gu_out)[0].start()

        late = t - lag

        @pl.when((late >= 0) & (late < per_array))
        def _():
            strip_copies(late, td_ref, gd_out)[0].wait()
            strip_copies(late, td_ref, gd_out)[1].start()

        @pl.when((late >= per_array) & (late < strips))
        def _():
            strip_copies(late, tu_ref, gu_out)[0].wait()
            strip_copies(late, tu_ref, gu_out)[1].start()

    def compute(p):
        q, part = p // parts, p % parts
        stage = q % 2

        @pl.when((part == 0) & (q + 1 < granules))
        def _():
            load(q + 1)

        @pl.when(part == 0)
        def _():
            for copy in operand_copies(a_ref, g_ref, 0, stage):
                copy.wait()

        @pl.when(q == per_grad)
        def _():
            out_copy(gd_out, part).wait()

        @pl.when(q % per_grad == 0)
        def _():
            acc[part] = dot_f32(lhs[stage, part // 2], rhs[stage, part % 2], ROW_CONTRACT)

        @pl.when(q % per_grad > 0)
        def _():
            acc[part] += dot_f32(lhs[stage, part // 2], rhs[stage, part % 2], ROW_CONTRACT)

        @pl.when(q == per_grad - 1)
        def _():
            out_copy(gd_out, part).start()

        @pl.when(q == granules - 1)
        def _():
            out_copy(gu_out, part).start()

    load(0)

    def body(p, carry):
        for k in range(2):
            move(2 * p + k)
        compute(p)
        return carry

    lax.fori_loop(0, parts * granules, body, 0)

    def flush(t, carry):
        move(t)
        return carry

    lax.fori_loop(2 * parts * granules, max(strips + depth, 2 * parts * granules), flush, 0)
    for part in range(parts):
        out_copy(gu_out, part).wait()


def run_final(operands, t_down, t_up):
    layers, width, d_model = t_down.shape[0] + 1, t_down.shape[1], t_down.shape[2]
    tokens = operands[1].shape[0]
    rows, side_w = tokens // SLOTS, width // 2
    bf16, f32 = jnp.bfloat16, jnp.float32
    anywhere = pl.BlockSpec(memory_space=pl.ANY)
    return pl.pallas_call(
        final_kernel,
        out_shape=(jax.ShapeDtypeStruct((layers, width, d_model), f32), jax.ShapeDtypeStruct((layers, d_model, width), f32)),
        in_specs=[anywhere] * 10,
        out_specs=(anywhere,) * 2,
        scratch_shapes=[
            pltpu.VMEM((4, side_w, side_w), f32),
            pltpu.VMEM((2, 2, rows, side_w), bf16),
            pltpu.VMEM((2, 2, rows, side_w), bf16),
            pltpu.VMEM((12, 128, d_model), f32),
            pltpu.SemaphoreType.DMA((2, 2)),
            pltpu.SemaphoreType.DMA((2, 2)),
            pltpu.SemaphoreType.DMA((4,)),
            pltpu.SemaphoreType.DMA((12,)),
            pltpu.SemaphoreType.DMA((12,)),
        ],
        compiler_params=pltpu.CompilerParams(vmem_limit_bytes=67043328),
        cost_estimate=pl.CostEstimate(flops=8 * tokens * d_model * width, bytes_accessed=16 * layers * d_model * width, transcendentals=0),
        name="final_grads",
    )(*operands, t_down, t_up)


def local_step(hidden, targets, w_up, w_down, total_tokens):
    _, _, act_all, g_all, d_all, t_down, t_up, _, _, pg, ph, pa0, pd0 = run_chain(hidden, targets, w_up, w_down, total_tokens)
    grad_down, grad_up = run_final((act_all, pa0, g_all, pg, hidden, ph, d_all, pd0), t_down, t_up)
    return grad_up, grad_down


def solution(mesh):
    def grad_step(hidden_in, targets, w_up, w_down):
        step_fn = functools.partial(local_step, total_tokens=hidden_in.shape[0])
        mapped = jax.shard_map(step_fn, mesh=mesh, in_specs=(P("dp", None), P("dp", None), P(None, None, "tp"), P(None, "tp", None)), out_specs=(P(None, None, "tp"), P(None, "tp", None)), check_vma=False)
        return mapped(hidden_in, targets, w_up, w_down)

    return grad_step
```

```python
import functools
import jax
import jax.numpy as jnp
from jax import lax
from jax.experimental import pallas as pl
from jax.experimental.pallas import tpu as pltpu
from jax.sharding import PartitionSpec as P

ROW_CONTRACT = (((0,), (0,)), ((), ()))
COL_CONTRACT = (((1,), (1,)), ((), ()))
MESH = pl.DeviceIdType.MESH
SLOTS = 4
TILE = 512
RED1_X, RED1_Y, RED2_X, RED2_Y, GAT1_X, GAT1_Y, GAT2_X, GAT2_Y = range(8)


def gelu_tanh(value):
    return jax.nn.gelu(value, approximate=True)


def dot_f32(lhs, rhs, dims=(((1,), (0,)), ((), ()))):
    return lax.dot_general(lhs, rhs, dims, preferred_element_type=jnp.float32)


PUSH_A, PUSH_D, PUSH_G, PUSH_H = range(4)


def chain_kernel(layers, total_tokens, x_ref, t_ref, wu_ref, wd_ref,
                 h_out, u_out, a_out, g_out, du_out, td_out, tu_out, pa_out, pd_out, pg_out, ph_out, pa0_out, pd0_out,
                 hbuf, abuf, ubuf, wbuf, pbuf, red1, red2, acc, ops,
                 send_sem, recv_sem, push_send, push_recv, res_send, res_recv, w_sem, u_sem, a_sem, h_sem, t_sem, l_sem, o_sem):
    rows, d_model = hbuf.shape[1:]
    block = rows // 4
    half = block // 2
    tiles = d_model // TILE
    side_w = d_model // 2
    turn = layers * SLOTS
    steps = turn + (layers - 1) * SLOTS
    every = steps + SLOTS
    top = layers - 1
    granules = 2 * (layers - 1) * 2 * SLOTS
    me = lax.axis_index("tp")
    core = lax.axis_index("dp")
    peer = 1 - core
    mx, my = me % 2, me // 2
    x_nbr = my * 2 + (1 - mx)
    y_nbr = (1 - my) * 2 + mx
    diag = (1 - my) * 2 + (1 - mx)

    def rows_of(owner, part=None):
        if part is None:
            return pl.ds(pl.multiple_of(owner * block, block), block)
        return pl.ds(pl.multiple_of(owner * block + part * half, half), half)

    def chunk_rows(slot):
        return pl.ds(pl.multiple_of(slot * rows, rows), rows)

    def half_of(which):
        return pl.ds(pl.multiple_of(which * side_w, side_w), side_w)

    def tile_of(tile):
        return pl.ds(pl.multiple_of(tile * TILE, TILE), TILE)

    def layer_of(n):
        back = n // turn
        return (1 - back) * (n // SLOTS) + back * (2 * layers - 1 - n // SLOTS)

    def remote(kind, k, src, dst, target):
        return pltpu.make_async_remote_copy(src_ref=src, dst_ref=dst, send_sem=send_sem.at[kind, k % SLOTS], recv_sem=recv_sem.at[kind, k % SLOTS], device_id={"tp": target}, device_id_type=MESH)

    def red1_copies(k):
        return (remote(RED1_X, k, pbuf.at[k % 2, rows_of(diag, 0)], red1.at[k % 2, 0], x_nbr),
                remote(RED1_Y, k, pbuf.at[k % 2, rows_of(diag, 1)], red1.at[k % 2, 1], y_nbr))

    def red2_copies(k):
        return (remote(RED2_X, k, pbuf.at[k % 2, rows_of(x_nbr)], red2.at[k % 2, 0], x_nbr),
                remote(RED2_Y, k, pbuf.at[k % 2, rows_of(y_nbr)], red2.at[k % 2, 1], y_nbr))

    def gat1_copies(k):
        mine = hbuf.at[k % SLOTS, rows_of(me)]
        return (remote(GAT1_X, k, mine, mine, x_nbr), remote(GAT1_Y, k, mine, mine, y_nbr))

    def gat2_copies(k):
        from_y = hbuf.at[k % SLOTS, rows_of(y_nbr, 0)]
        from_x = hbuf.at[k % SLOTS, rows_of(x_nbr, 1)]
        return (remote(GAT2_X, k, from_y, from_y, x_nbr), remote(GAT2_Y, k, from_x, from_x, y_nbr))

    def push(kind, layer, slot, src, dst):
        return pltpu.make_async_remote_copy(src_ref=src, dst_ref=dst, send_sem=push_send.at[kind, layer, slot], recv_sem=push_recv.at[kind, layer, slot], device_id={"dp": peer}, device_id_type=MESH)

    def push_a(layer, slot):
        return push(PUSH_A, layer, slot, abuf.at[:, half_of(peer)], pa_out.at[layer, chunk_rows(slot)])

    def push_d(layer, slot):
        return push(PUSH_D, layer, slot, abuf.at[:, half_of(peer)], pd_out.at[layer, chunk_rows(slot)])

    def push_a0(slot):
        return push(PUSH_A, 0, slot, abuf, pa0_out.at[chunk_rows(slot)])

    def push_d0(slot):
        return push(PUSH_D, 0, slot, abuf, pd0_out.at[chunk_rows(slot)])

    def push_g(layer, slot):
        return push(PUSH_G, layer, slot, hbuf.at[slot], pg_out.at[layer, chunk_rows(slot)])

    def push_h(layer, slot):
        return push(PUSH_H, layer, slot, hbuf.at[slot], ph_out.at[layer, chunk_rows(slot)])

    def weight_copy(ref, layer, tile, stage):
        return pltpu.make_async_copy(ref.at[layer, tile_of(tile)], wbuf.at[stage], w_sem.at[stage])

    def column_copies(ref, layer, tile, stage):
        for i in range(tiles):
            block_rows = pl.ds(i * TILE, TILE)
            pltpu.make_async_copy(ref.at[layer, block_rows, tile_of(tile)], wbuf.at[stage, :, block_rows], w_sem.at[stage]).start()

    def weight_start(index):
        main = steps * 2 * tiles
        n, place = index // (2 * tiles), index % (2 * tiles)
        up = 1 - place // tiles
        use_up = (1 - n // turn) * up + (n // turn) * (1 - up)

        @pl.when((n < turn) & (use_up == 1))
        def _():
            column_copies(wu_ref, layer_of(n), place % tiles, index % 3)

        @pl.when((n < turn) & (use_up == 0))
        def _():
            column_copies(wd_ref, layer_of(n), place % tiles, index % 3)

        @pl.when((n >= turn) & (index < main) & (use_up == 1))
        def _():
            weight_copy(wu_ref, layer_of(n), place % tiles, index % 3).start()

        @pl.when((n >= turn) & (index < main) & (use_up == 0))
        def _():
            weight_copy(wd_ref, layer_of(n), place % tiles, index % 3).start()

        @pl.when((index >= main) & (index < main + SLOTS * tiles))
        def _():
            weight_copy(wd_ref, 0, (index - main) % tiles, index % 3).start()

    def weight_wait(index):
        weight_copy(wu_ref, 0, 0, index % 3).wait()

    def weight_base(n):
        late = (n // steps) * (n - steps)
        return (n - late) * 2 * tiles + late * tiles

    def u_save(n, tile, stage):
        return pltpu.make_async_copy(ubuf.at[stage], u_out.at[layer_of(n), chunk_rows(n % SLOTS), tile_of(tile)], u_sem.at[stage])

    def u_load(n, tile, stage):
        return pltpu.make_async_copy(u_out.at[layer_of(n), chunk_rows(n % SLOTS), tile_of(tile)], ubuf.at[stage], u_sem.at[stage])

    def x_load(slot):
        return pltpu.make_async_copy(x_ref.at[chunk_rows(slot)], hbuf.at[slot], h_sem.at[slot])

    def h_save(layer, slot):
        return pltpu.make_async_copy(hbuf.at[slot], h_out.at[layer - 1, chunk_rows(slot)], h_sem.at[slot])

    def g_save(layer, slot):
        return pltpu.make_async_copy(hbuf.at[slot], g_out.at[layer, chunk_rows(slot)], h_sem.at[slot])

    def a_save(layer, slot):
        return pltpu.make_async_copy(abuf, a_out.at[layer, chunk_rows(slot)], a_sem)

    def d_save(layer, slot):
        return pltpu.make_async_copy(abuf, du_out.at[layer, chunk_rows(slot)], a_sem)

    def t_loads(slot):
        own = pl.ds(pl.multiple_of(slot * rows + me * block, block), block)
        return [pltpu.make_async_copy(t_ref.at[own, pl.ds(part * side_w, side_w)], ops.at[0, 1 + part, pl.ds(0, block)], t_sem.at[part]) for part in range(2)]

    def half_load(src, side):
        return pltpu.make_async_copy(src, ops.at[side, 0], l_sem.at[side, 0])

    def full_load(src, side, part):
        return pltpu.make_async_copy(src.at[:, pl.ds(part * side_w, side_w)], ops.at[side, 1 + part], l_sem.at[side, 1 + part])

    def out_copy(dst, part):
        return pltpu.make_async_copy(acc.at[part], dst, o_sem.at[part])

    def out_push(dst, index, part):
        return pltpu.make_async_remote_copy(src_ref=acc.at[part], dst_ref=dst, send_sem=res_send.at[index, part], recv_sem=res_recv.at[index, part], device_id={"dp": peer}, device_id_type=MESH)

    def td_part(layer, part):
        return td_out.at[layer - 1, half_of(core), pl.ds(part * side_w, side_w)]

    def tu_part(layer, part):
        return tu_out.at[layer - 1, pl.ds(part * side_w, side_w), half_of(core)]

    def load_granule(q):
        index = q // (2 * SLOTS)
        kind, layer, slot, side = index % 2, top - index // 2, (q % (2 * SLOTS)) // 2, q % 2

        def start(half_src, full_src):
            half_load(half_src, side).start()
            for part in range(2):
                full_load(full_src, side, part).start()

        @pl.when((kind == 0) & (side == 0))
        def _():
            start(a_out.at[layer, chunk_rows(slot), half_of(core)], g_out.at[layer, chunk_rows(slot)])

        @pl.when((kind == 0) & (side == 1))
        def _():
            push_a(layer, slot).wait_recv()
            push_g(layer, slot).wait_recv()
            start(pa_out.at[layer, chunk_rows(slot)], pg_out.at[layer, chunk_rows(slot)])

        @pl.when((kind == 1) & (side == 0))
        def _():
            start(du_out.at[layer, chunk_rows(slot), half_of(core)], h_out.at[layer - 1, chunk_rows(slot)])

        @pl.when((kind == 1) & (side == 1))
        def _():
            push_d(layer, slot).wait_recv()
            push_h(layer, slot).wait_recv()
            start(pd_out.at[layer, chunk_rows(slot)], ph_out.at[layer, chunk_rows(slot)])

    def wait_outs(index):
        for part in range(2):
            out_copy(td_part(1, part), part).wait()
            out_push(td_part(1, part), index, part).wait_send()

    def run_granule(q):
        index = q // (2 * SLOTS)
        kind, layer, side = index % 2, top - index // 2, q % 2

        @pl.when((q % (2 * SLOTS) == 0) & (q > 0))
        def _():
            wait_outs(index - 1)

        @pl.when(q % (2 * SLOTS) == 0)
        def _():
            def clear(i, carry):
                strip = pl.ds(pl.multiple_of(i * 64, 64), 64)
                acc[:, strip, :] = jnp.zeros((2, 64, side_w), jnp.float32)
                return carry

            lax.fori_loop(0, side_w // 64, clear, 0)

        half_load(pa_out.at[0, chunk_rows(0)], side).wait()
        for part in range(2):
            full_load(pg_out.at[0, chunk_rows(0)], side, part).wait()

        def part_step(i, carry):
            part, strip = i // 2, pl.ds(pl.multiple_of(i % 2 * (side_w // 2), side_w // 2), side_w // 2)
            acc[part, strip] += dot_f32(ops[side, kind * (1 + part), :, strip], ops[side, (1 - kind) * (1 + part)], ROW_CONTRACT)
            return carry

        lax.fori_loop(0, 4, part_step, 0)

        @pl.when((q % (2 * SLOTS) == 2 * SLOTS - 1) & (kind == 0))
        def _():
            for part in range(2):
                out_copy(td_part(layer, part), part).start()
                out_push(td_part(layer, part), index, part).start()

        @pl.when((q % (2 * SLOTS) == 2 * SLOTS - 1) & (kind == 1))
        def _():
            for part in range(2):
                out_copy(tu_part(layer, part), part).start()
                out_push(tu_part(layer, part), index, part).start()

    counts = {1: 4, 2: 2, 3: 2, 4: 4, 5: 4, 6: 4, 7: 4, 8: 6, 9: 6, 10: 2, 11: 8}

    def plan_of(n):
        first, count = 0, 0
        for b, number in counts.items():
            reached, passed = (n - b) // turn, (n - b - 1) // turn
            first = first + number * passed
            count = count + number * (reached - passed)
        count = (n // turn) * count
        one = first + (count + 2) // 4
        return first, one, one + (count + 2) // 3, first + count

    def run_granules(begin, end, stop):
        def step(q, carry):
            @pl.when(q + 1 < stop)
            def _():
                load_granule(q + 1)

            run_granule(q)
            return carry

        lax.fori_loop(begin, end, step, 0)

    def receive_rows(n):
        layer, slot = layer_of(n), n % SLOTS

        @pl.when(n < SLOTS)
        def _():
            x_load(slot).wait()

        @pl.when(n >= SLOTS)
        def _():
            for copy in gat2_copies(n):
                copy.wait()
            for copy in gat1_copies(n):
                copy.wait_send()

        @pl.when(n < turn)
        def _():
            push_h(layer, slot).start()

        @pl.when((n >= SLOTS) & (n < turn))
        def _():
            h_save(layer, slot).start()

        @pl.when(n >= turn)
        def _():
            push_g(layer, slot).start()
            g_save(layer, slot).start()

    def settle_rows(n):
        layer, slot = layer_of(n), n % SLOTS

        @pl.when(n < turn)
        def _():
            push_h(layer, slot).wait_send()

        @pl.when((n >= SLOTS) & (n < turn))
        def _():
            h_save(layer, slot).wait()

        @pl.when(n >= turn)
        def _():
            push_g(layer, slot).wait_send()
            g_save(layer, slot).wait()

    def share_acts(n):
        layer, slot = layer_of(n), n % SLOTS

        @pl.when(n < turn)
        def _():
            a_save(layer, slot).start()

        @pl.when(n >= turn)
        def _():
            d_save(layer, slot).start()

        @pl.when(n < SLOTS)
        def _():
            push_a0(slot).start()

        @pl.when((n >= SLOTS) & (n < turn))
        def _():
            push_a(layer, slot).start()

        @pl.when((n >= turn) & (n < steps))
        def _():
            push_d(layer, slot).start()

        @pl.when(n >= steps)
        def _():
            push_d0(slot).start()

    def settle_acts(n):
        layer, slot = layer_of(n), n % SLOTS
        a_save(layer, slot).wait()

        @pl.when(n < SLOTS)
        def _():
            push_a0(slot).wait_send()

        @pl.when((n >= SLOTS) & (n < turn))
        def _():
            push_a(layer, slot).wait_send()

        @pl.when((n >= turn) & (n < steps))
        def _():
            push_d(layer, slot).wait_send()

        @pl.when(n >= steps)
        def _():
            push_d0(slot).wait_send()

    def times_columns(source, stage):
        total = None
        for i in range(tiles):
            cols = pl.ds(i * TILE, TILE)
            part = dot_f32(source(cols), wbuf[stage, :, cols])
            total = part if total is None else total + part
        return total

    def forward_up(n):
        slot = n % SLOTS

        def tile_step(tile, carry):
            index = weight_base(n) + tile
            count = n * tiles + tile
            weight_start(index + 2)
            weight_wait(index)
            pre = times_columns(lambda cols: hbuf[slot, :, cols], index % 3).astype(jnp.bfloat16)

            @pl.when(count >= 2)
            def _():
                u_save(0, 0, count % 2).wait()

            ubuf[count % 2] = pre
            abuf[:, tile_of(tile)] = gelu_tanh(pre.astype(jnp.float32)).astype(jnp.bfloat16)
            u_save(n, tile, count % 2).start()
            return carry

        lax.fori_loop(0, tiles, tile_step, 0)

    def forward_down(n):
        def tile_step(tile, carry):
            index = weight_base(n) + tiles + tile
            weight_start(index + 2)
            weight_wait(index)
            pbuf[n % 2, :, tile_of(tile)] = times_columns(lambda cols: abuf[:, cols], index % 3)
            return carry

        lax.fori_loop(0, tiles, tile_step, 0)

    def backward_up(n):
        slot = n % SLOTS

        @pl.when(n == turn)
        def _():
            for stage in range(2):
                u_save(0, 0, stage).wait()
            u_load(n, 0, n * tiles % 2).start()

        def tile_step(tile, carry):
            index = weight_base(n) + tile
            count = n * tiles + tile
            weight_start(index + 2)

            @pl.when(count + 1 < every * tiles)
            def _():
                u_load((count + 1) // tiles, (count + 1) % tiles, (count + 1) % 2).start()

            weight_wait(index)
            u_load(n, tile, count % 2).wait()
            d_act = dot_f32(hbuf[slot], wbuf[index % 3], COL_CONTRACT)
            _, gelu_vjp = jax.vjp(gelu_tanh, ubuf[count % 2].astype(jnp.float32))
            abuf[:, tile_of(tile)] = gelu_vjp(d_act)[0].astype(jnp.bfloat16)
            return carry

        lax.fori_loop(0, tiles, tile_step, 0)

    def backward_down(n):
        def tile_step(tile, carry):
            index = weight_base(n) + tiles + tile
            weight_start(index + 2)
            weight_wait(index)
            pbuf[n % 2, :, tile_of(tile)] = dot_f32(abuf[...], wbuf[index % 3], COL_CONTRACT)
            return carry

        lax.fori_loop(0, tiles, tile_step, 0)

    def send_diagonal(n):
        for copy in red1_copies(n):
            copy.start()

    def reduce_step(k):
        first, second = red1_copies(k)
        first.wait_recv()
        pbuf[k % 2, rows_of(y_nbr, 0)] += red1[k % 2, 0]
        second.wait_recv()
        pbuf[k % 2, rows_of(x_nbr, 1)] += red1[k % 2, 1]
        for copy in red2_copies(k):
            copy.start()

        @pl.when((k >= turn - SLOTS) & (k < turn))
        def _():
            for copy in t_loads(k % SLOTS):
                copy.start()

    def finish_step(k):
        slot = k % SLOTS
        for copy in red2_copies(k):
            copy.wait()
        for copy in red1_copies(k):
            copy.wait_send()

        def total():
            return pbuf[k % 2, rows_of(me)] + red2[k % 2, 0] + red2[k % 2, 1]

        def h_new():
            return (hbuf[slot, rows_of(me)].astype(jnp.float32) + total().astype(jnp.bfloat16).astype(jnp.float32)).astype(jnp.bfloat16)

        @pl.when(k < turn - SLOTS)
        def _():
            hbuf[slot, rows_of(me)] = h_new()

        @pl.when((k >= turn - SLOTS) & (k < turn))
        def _():
            for copy in t_loads(slot):
                copy.wait()
            target = jnp.concatenate([ops[0, 1, :block], ops[0, 2, :block]], 1)
            err = (h_new().astype(jnp.float32) - target.astype(jnp.float32)) * (1.0 / total_tokens)
            hbuf[slot, rows_of(me)] = err.astype(jnp.bfloat16)

        @pl.when(k >= turn)
        def _():
            hbuf[slot, rows_of(me)] = (hbuf[slot, rows_of(me)].astype(jnp.float32) + total()).astype(jnp.bfloat16)

        for copy in gat1_copies(k):
            copy.start()

    def forward_rows(k):
        for copy in gat1_copies(k):
            copy.wait_recv()
        for copy in gat2_copies(k):
            copy.start()

    def when_step(k, fn):
        @pl.when((k >= 0) & (k < steps))
        def _():
            fn(k)

    barrier = pltpu.get_barrier_semaphore()
    for target in ({"tp": x_nbr}, {"tp": y_nbr}, {"dp": peer}):
        pl.semaphore_signal(barrier, inc=1, device_id=target, device_id_type=MESH)
    x_load(0).start()
    weight_start(0)
    weight_start(1)
    for slot in range(1, SLOTS):
        x_load(slot).start()
    pl.semaphore_wait(barrier, 3)

    def body(n, carry):
        begin, one, two, stop = plan_of(n)
        receive_rows(n)

        @pl.when(n >= 1)
        def _():
            settle_acts(n - 1)

        @pl.when(n < turn)
        def _():
            forward_up(n)

        @pl.when(n >= turn)
        def _():
            backward_up(n)

        when_step(n - 2, forward_rows)
        share_acts(n)
        settle_rows(n)

        @pl.when(begin < stop)
        def _():
            load_granule(begin)

        @pl.when(n < turn)
        def _():
            forward_down(n)

        @pl.when(n >= turn)
        def _():
            backward_down(n)

        send_diagonal(n)
        run_granules(begin, one, stop)
        when_step(n - 1, finish_step)
        run_granules(one, two, stop)
        reduce_step(n)
        run_granules(two, stop, stop)
        return carry

    lax.fori_loop(0, steps, body, 0)
    forward_rows(steps - 2)
    ran = sum(counts.values())

    def last_body(n, carry):
        receive_rows(n)
        settle_acts(n - 1)

        @pl.when(n == steps)
        def _():
            load_granule(ran)

        backward_up(n)
        share_acts(n)

        @pl.when(n == steps)
        def _():
            finish_step(steps - 1)
            run_granules(ran, granules, granules)

        @pl.when(n == steps + 1)
        def _():
            forward_rows(steps - 1)

        settle_rows(n)
        return carry

    lax.fori_loop(steps, every, last_body, 0)
    settle_acts(every - 1)
    wait_outs(2 * (layers - 1) - 1)
    for slot in range(SLOTS):
        push_a0(slot).wait_recv()
        push_d0(slot).wait_recv()
        push_g(0, slot).wait_recv()
        push_h(0, slot).wait_recv()
    for index in range(2 * (layers - 1)):
        for part in range(2):
            out_push(td_part(1, part), index, part).wait_recv()


def run_chain(hidden, targets, w_up, w_down, total_tokens):
    layers, d_model, width = w_up.shape
    tokens = hidden.shape[0]
    rows = tokens // SLOTS
    block = rows // 4
    half = width // 2
    bf16, f32 = jnp.bfloat16, jnp.float32
    flops = 2 * tokens * d_model * width * (6 * layers - 3)
    anywhere = pl.BlockSpec(memory_space=pl.ANY)
    like = jax.ShapeDtypeStruct
    outs = (like((layers - 1, tokens, d_model), bf16), like((layers, tokens, width), bf16), like((layers, tokens, width), bf16),
            like((layers, tokens, d_model), bf16), like((layers, tokens, width), bf16),
            like((layers - 1, width, d_model), f32), like((layers - 1, d_model, width), f32),
            like((layers, tokens, half), bf16), like((layers, tokens, half), bf16),
            like((layers, tokens, d_model), bf16), like((layers, tokens, d_model), bf16),
            like((tokens, width), bf16), like((tokens, width), bf16))
    return pl.pallas_call(
        functools.partial(chain_kernel, layers, total_tokens),
        out_shape=outs,
        in_specs=[anywhere] * 4,
        out_specs=(anywhere,) * len(outs),
        scratch_shapes=[
            pltpu.VMEM((SLOTS, rows, d_model), bf16),
            pltpu.VMEM((rows, width), bf16),
            pltpu.VMEM((2, rows, TILE), bf16),
            pltpu.VMEM((3, TILE, d_model), bf16),
            pltpu.VMEM((2, rows, d_model), f32),
            pltpu.VMEM((2, 2, block // 2, d_model), f32),
            pltpu.VMEM((2, 2, block, d_model), f32),
            pltpu.VMEM((2, half, half), f32),
            pltpu.VMEM((2, 3, rows, half), bf16),
            pltpu.SemaphoreType.DMA((8, SLOTS)),
            pltpu.SemaphoreType.DMA((8, SLOTS)),
            pltpu.SemaphoreType.DMA((4, layers, SLOTS)),
            pltpu.SemaphoreType.DMA((4, layers, SLOTS)),
            pltpu.SemaphoreType.DMA((2 * (layers - 1), 2)),
            pltpu.SemaphoreType.DMA((2 * (layers - 1), 2)),
            pltpu.SemaphoreType.DMA((3,)),
            pltpu.SemaphoreType.DMA((2,)),
            pltpu.SemaphoreType.DMA,
            pltpu.SemaphoreType.DMA((SLOTS,)),
            pltpu.SemaphoreType.DMA((2,)),
            pltpu.SemaphoreType.DMA((2, 3)),
            pltpu.SemaphoreType.DMA((2,)),
        ],
        compiler_params=pltpu.CompilerParams(collective_id=0, has_side_effects=True, vmem_limit_bytes=67043328),
        cost_estimate=pl.CostEstimate(flops=flops, bytes_accessed=layers * tokens * d_model * 16, transcendentals=2 * layers * tokens * width),
        name="step_chain",
    )(hidden, targets, w_up, w_down)


def final_kernel(a_ref, pa_ref, g_ref, pg_ref, x_ref, px_ref, d_ref, pd_ref, td_ref, tu_ref, gd_out, gu_out, acc, lhs, rhs, ring, l_sem, r_sem, o_sem, in_sem, out_sem):
    rows, side_w = lhs.shape[2:]
    strip = ring.shape[1]
    depth = ring.shape[0]
    done_layers, height, _ = td_ref.shape
    per_layer = height // strip
    per_array = done_layers * per_layer
    strips = 2 * per_array
    lag = depth // 2
    core = lax.axis_index("dp")
    a_ref, g_ref, pg_ref, px_ref, d_ref = (ref.at[0] for ref in (a_ref, g_ref, pg_ref, px_ref, d_ref))
    parts = 4
    granules = 4 * SLOTS
    per_grad = granules // 2

    def chunk_rows(slot):
        return pl.ds(pl.multiple_of(slot * rows, rows), rows)

    def half_of(which):
        return pl.ds(pl.multiple_of(which * side_w, side_w), side_w)

    def operand_copies(left, right, slot, stage):
        for part in range(2):
            cols = pl.ds(part * side_w, side_w)
            yield pltpu.make_async_copy(left.at[chunk_rows(slot), cols], lhs.at[stage, part], l_sem.at[stage, part])
            yield pltpu.make_async_copy(right.at[chunk_rows(slot), cols], rhs.at[stage, part], r_sem.at[stage, part])

    def load(q):
        grad, slot, side = q // per_grad, (q % per_grad) // 2, q % 2
        for which, mine, theirs in ((0, (a_ref, g_ref), (pa_ref, pg_ref)), (1, (x_ref, d_ref), (px_ref, pd_ref))):
            @pl.when((grad == which) & (side == core))
            def _():
                for copy in operand_copies(*mine, slot, q % 2):
                    copy.start()

            @pl.when((grad == which) & (side != core))
            def _():
                for copy in operand_copies(*theirs, slot, q % 2):
                    copy.start()

    def out_copy(dst, part):
        return pltpu.make_async_copy(acc.at[part], dst.at[0, half_of(part // 2), half_of(part % 2)], o_sem.at[part])

    def strip_copies(t, src, dst):
        layer, row = (t % per_array) // per_layer, pl.multiple_of((t % per_layer) * strip, strip)
        return (pltpu.make_async_copy(src.at[layer, pl.ds(row, strip)], ring.at[t % depth], in_sem.at[t % depth]),
                pltpu.make_async_copy(ring.at[t % depth], dst.at[layer + 1, pl.ds(row, strip)], out_sem.at[t % depth]))

    def move(t):
        @pl.when((t >= depth) & (t < strips + depth))
        def _():
            strip_copies(t - depth, td_ref, gd_out)[1].wait()

        @pl.when(t < per_array)
        def _():
            strip_copies(t, td_ref, gd_out)[0].start()

        @pl.when((t >= per_array) & (t < strips))
        def _():
            strip_copies(t, tu_ref, gu_out)[0].start()

        late = t - lag

        @pl.when((late >= 0) & (late < per_array))
        def _():
            strip_copies(late, td_ref, gd_out)[0].wait()
            strip_copies(late, td_ref, gd_out)[1].start()

        @pl.when((late >= per_array) & (late < strips))
        def _():
            strip_copies(late, tu_ref, gu_out)[0].wait()
            strip_copies(late, tu_ref, gu_out)[1].start()

    def compute(p):
        q, part = p // parts, p % parts
        stage = q % 2

        @pl.when((part == 0) & (q + 1 < granules))
        def _():
            load(q + 1)

        @pl.when(part == 0)
        def _():
            for copy in operand_copies(a_ref, g_ref, 0, stage):
                copy.wait()

        @pl.when(q == per_grad)
        def _():
            out_copy(gd_out, part).wait()

        @pl.when(q % per_grad == 0)
        def _():
            acc[part] = dot_f32(lhs[stage, part // 2], rhs[stage, part % 2], ROW_CONTRACT)

        @pl.when(q % per_grad > 0)
        def _():
            acc[part] += dot_f32(lhs[stage, part // 2], rhs[stage, part % 2], ROW_CONTRACT)

        @pl.when(q == per_grad - 1)
        def _():
            out_copy(gd_out, part).start()

        @pl.when(q == granules - 1)
        def _():
            out_copy(gu_out, part).start()

    load(0)

    def body(p, carry):
        for k in range(2):
            move(2 * p + k)
        compute(p)
        return carry

    lax.fori_loop(0, parts * granules, body, 0)

    def flush(t, carry):
        move(t)
        return carry

    lax.fori_loop(2 * parts * granules, max(strips + depth, 2 * parts * granules), flush, 0)
    for part in range(parts):
        out_copy(gu_out, part).wait()


def run_final(operands, t_down, t_up):
    layers, width, d_model = t_down.shape[0] + 1, t_down.shape[1], t_down.shape[2]
    tokens = operands[1].shape[0]
    rows, side_w = tokens // SLOTS, width // 2
    bf16, f32 = jnp.bfloat16, jnp.float32
    anywhere = pl.BlockSpec(memory_space=pl.ANY)
    return pl.pallas_call(
        final_kernel,
        out_shape=(jax.ShapeDtypeStruct((layers, width, d_model), f32), jax.ShapeDtypeStruct((layers, d_model, width), f32)),
        in_specs=[anywhere] * 10,
        out_specs=(anywhere,) * 2,
        scratch_shapes=[
            pltpu.VMEM((4, side_w, side_w), f32),
            pltpu.VMEM((2, 2, rows, side_w), bf16),
            pltpu.VMEM((2, 2, rows, side_w), bf16),
            pltpu.VMEM((12, 128, d_model), f32),
            pltpu.SemaphoreType.DMA((2, 2)),
            pltpu.SemaphoreType.DMA((2, 2)),
            pltpu.SemaphoreType.DMA((4,)),
            pltpu.SemaphoreType.DMA((12,)),
            pltpu.SemaphoreType.DMA((12,)),
        ],
        compiler_params=pltpu.CompilerParams(vmem_limit_bytes=67043328),
        cost_estimate=pl.CostEstimate(flops=8 * tokens * d_model * width, bytes_accessed=16 * layers * d_model * width, transcendentals=0),
        name="final_grads",
    )(*operands, t_down, t_up)


def local_step(hidden, targets, w_up, w_down, total_tokens):
    _, _, act_all, g_all, d_all, t_down, t_up, _, _, pg, ph, pa0, pd0 = run_chain(hidden, targets, w_up, w_down, total_tokens)
    grad_down, grad_up = run_final((act_all, pa0, g_all, pg, hidden, ph, d_all, pd0), t_down, t_up)
    return grad_up, grad_down


def solution(mesh):
    def grad_step(hidden_in, targets, w_up, w_down):
        step_fn = functools.partial(local_step, total_tokens=hidden_in.shape[0])
        mapped = jax.shard_map(step_fn, mesh=mesh, in_specs=(P("dp", None), P("dp", None), P(None, None, "tp"), P(None, "tp", None)), out_specs=(P(None, None, "tp"), P(None, "tp", None)), check_vma=False)
        return mapped(hidden_in, targets, w_up, w_down)

    return grad_step
```

```python
import functools
import jax
import jax.numpy as jnp
from jax import lax
from jax.experimental import pallas as pl
from jax.experimental.pallas import tpu as pltpu
from jax.sharding import PartitionSpec as P

ROW_CONTRACT = (((0,), (0,)), ((), ()))
COL_CONTRACT = (((1,), (1,)), ((), ()))
MESH = pl.DeviceIdType.MESH
SLOTS = 4
TILE = 512
RED1_X, RED1_Y, RED2_X, RED2_Y, GAT1_X, GAT1_Y, GAT2_X, GAT2_Y = range(8)


def gelu_tanh(value):
    return jax.nn.gelu(value, approximate=True)


def dot_f32(lhs, rhs, dims=(((1,), (0,)), ((), ()))):
    return lax.dot_general(lhs, rhs, dims, preferred_element_type=jnp.float32)


PUSH_A, PUSH_D, PUSH_G, PUSH_H = range(4)


def chain_kernel(layers, total_tokens, x_ref, t_ref, wu_ref, wd_ref,
                 h_out, u_out, a_out, g_out, du_out, td_out, tu_out, pa_out, pd_out, pg_out, ph_out, pa0_out, pd0_out,
                 hbuf, abuf, ubuf, wbuf, pbuf, red1, red2, acc, ops,
                 send_sem, recv_sem, push_send, push_recv, res_send, res_recv, w_sem, u_sem, a_sem, h_sem, t_sem, l_sem, o_sem):
    rows, d_model = hbuf.shape[1:]
    block = rows // 4
    half = block // 2
    tiles = d_model // TILE
    side_w = d_model // 2
    turn = layers * SLOTS
    steps = turn + (layers - 1) * SLOTS
    every = steps + SLOTS
    top = layers - 1
    granules = 2 * (layers - 1) * 2 * SLOTS
    me = lax.axis_index("tp")
    core = lax.axis_index("dp")
    peer = 1 - core
    mx, my = me % 2, me // 2
    x_nbr = my * 2 + (1 - mx)
    y_nbr = (1 - my) * 2 + mx
    diag = (1 - my) * 2 + (1 - mx)

    def rows_of(owner, part=None):
        if part is None:
            return pl.ds(pl.multiple_of(owner * block, block), block)
        return pl.ds(pl.multiple_of(owner * block + part * half, half), half)

    def chunk_rows(slot):
        return pl.ds(pl.multiple_of(slot * rows, rows), rows)

    def half_of(which):
        return pl.ds(pl.multiple_of(which * side_w, side_w), side_w)

    def tile_of(tile):
        return pl.ds(pl.multiple_of(tile * TILE, TILE), TILE)

    def layer_of(n):
        back = n // turn
        return (1 - back) * (n // SLOTS) + back * (2 * layers - 1 - n // SLOTS)

    def remote(kind, k, src, dst, target):
        return pltpu.make_async_remote_copy(src_ref=src, dst_ref=dst, send_sem=send_sem.at[kind, k % SLOTS], recv_sem=recv_sem.at[kind, k % SLOTS], device_id={"tp": target}, device_id_type=MESH)

    def red1_copies(k):
        return (remote(RED1_X, k, pbuf.at[k % 2, rows_of(diag, 0)], red1.at[k % 2, 0], x_nbr),
                remote(RED1_Y, k, pbuf.at[k % 2, rows_of(diag, 1)], red1.at[k % 2, 1], y_nbr))

    def red1_tiles(tile):
        for kind, part, target in ((RED1_X, 0, x_nbr), (RED1_Y, 1, y_nbr)):
            remote(kind, 0, pbuf.at[0, rows_of(diag, part), tile_of(tile)], red1.at[0, part, :, tile_of(tile)], target).start()

    def red2_copies(k):
        return (remote(RED2_X, k, pbuf.at[k % 2, rows_of(x_nbr)], red2.at[k % 2, 0], x_nbr),
                remote(RED2_Y, k, pbuf.at[k % 2, rows_of(y_nbr)], red2.at[k % 2, 1], y_nbr))

    def gat1_copies(k):
        mine = hbuf.at[k % SLOTS, rows_of(me)]
        return (remote(GAT1_X, k, mine, mine, x_nbr), remote(GAT1_Y, k, mine, mine, y_nbr))

    def gat2_copies(k):
        from_y = hbuf.at[k % SLOTS, rows_of(y_nbr, 0)]
        from_x = hbuf.at[k % SLOTS, rows_of(x_nbr, 1)]
        return (remote(GAT2_X, k, from_y, from_y, x_nbr), remote(GAT2_Y, k, from_x, from_x, y_nbr))

    def push(kind, layer, slot, src, dst):
        return pltpu.make_async_remote_copy(src_ref=src, dst_ref=dst, send_sem=push_send.at[kind, layer, slot], recv_sem=push_recv.at[kind, layer, slot], device_id={"dp": peer}, device_id_type=MESH)

    def push_a(layer, slot):
        return push(PUSH_A, layer, slot, abuf.at[:, half_of(peer)], pa_out.at[layer, chunk_rows(slot)])

    def push_d(layer, slot):
        return push(PUSH_D, layer, slot, abuf.at[:, half_of(peer)], pd_out.at[layer, chunk_rows(slot)])

    def push_a0(slot):
        return push(PUSH_A, 0, slot, abuf, pa0_out.at[chunk_rows(slot)])

    def d0_tiles(slot, tile):
        part = abuf.at[:, tile_of(tile)]
        push(PUSH_D, 0, slot, part, pd0_out.at[chunk_rows(slot), tile_of(tile)]).start()
        pltpu.make_async_copy(part, du_out.at[0, chunk_rows(slot), tile_of(tile)], a_sem).start()

    def push_d0(slot):
        return push(PUSH_D, 0, slot, abuf, pd0_out.at[chunk_rows(slot)])

    def push_g(layer, slot):
        return push(PUSH_G, layer, slot, hbuf.at[slot], pg_out.at[layer, chunk_rows(slot)])

    def push_h(layer, slot):
        return push(PUSH_H, layer, slot, hbuf.at[slot], ph_out.at[layer, chunk_rows(slot)])

    def weight_copy(ref, layer, tile, stage):
        return pltpu.make_async_copy(ref.at[layer, tile_of(tile)], wbuf.at[stage], w_sem.at[stage])

    def column_copies(ref, layer, tile, stage):
        for i in range(tiles):
            block_rows = pl.ds(i * TILE, TILE)
            pltpu.make_async_copy(ref.at[layer, block_rows, tile_of(tile)], wbuf.at[stage, :, block_rows], w_sem.at[stage]).start()

    def weight_start(index):
        main = steps * 2 * tiles
        n, place = index // (2 * tiles), index % (2 * tiles)
        up = 1 - place // tiles
        use_up = (1 - n // turn) * up + (n // turn) * (1 - up)

        @pl.when((n < turn) & (use_up == 1))
        def _():
            column_copies(wu_ref, layer_of(n), place % tiles, index % 3)

        @pl.when((n < turn) & (use_up == 0))
        def _():
            column_copies(wd_ref, layer_of(n), place % tiles, index % 3)

        @pl.when((n >= turn) & (index < main) & (use_up == 1))
        def _():
            weight_copy(wu_ref, layer_of(n), place % tiles, index % 3).start()

        @pl.when((n >= turn) & (index < main) & (use_up == 0))
        def _():
            weight_copy(wd_ref, layer_of(n), place % tiles, index % 3).start()

        @pl.when((index >= main) & (index < main + SLOTS * tiles))
        def _():
            weight_copy(wd_ref, 0, (index - main) % tiles, index % 3).start()

    def weight_wait(index):
        weight_copy(wu_ref, 0, 0, index % 3).wait()

    def weight_base(n):
        late = (n // steps) * (n - steps)
        return (n - late) * 2 * tiles + late * tiles

    def u_save(n, tile, stage):
        return pltpu.make_async_copy(ubuf.at[stage], u_out.at[layer_of(n), chunk_rows(n % SLOTS), tile_of(tile)], u_sem.at[stage])

    def u_load(n, tile, stage):
        return pltpu.make_async_copy(u_out.at[layer_of(n), chunk_rows(n % SLOTS), tile_of(tile)], ubuf.at[stage], u_sem.at[stage])

    def x_load(slot):
        return pltpu.make_async_copy(x_ref.at[chunk_rows(slot)], hbuf.at[slot], h_sem.at[slot])

    def h_save(layer, slot):
        return pltpu.make_async_copy(hbuf.at[slot], h_out.at[layer - 1, chunk_rows(slot)], h_sem.at[slot])

    def g_save(layer, slot):
        return pltpu.make_async_copy(hbuf.at[slot], g_out.at[layer, chunk_rows(slot)], h_sem.at[slot])

    def a_save(layer, slot):
        return pltpu.make_async_copy(abuf, a_out.at[layer, chunk_rows(slot)], a_sem)

    def d_save(layer, slot):
        return pltpu.make_async_copy(abuf, du_out.at[layer, chunk_rows(slot)], a_sem)

    def t_loads(slot):
        own = pl.ds(pl.multiple_of(slot * rows + me * block, block), block)
        return [pltpu.make_async_copy(t_ref.at[own, pl.ds(part * side_w, side_w)], ops.at[0, 1 + part, pl.ds(0, block)], t_sem.at[part]) for part in range(2)]

    def half_load(src, side):
        return pltpu.make_async_copy(src, ops.at[side, 0], l_sem.at[side, 0])

    def full_load(src, side, part):
        return pltpu.make_async_copy(src.at[:, pl.ds(part * side_w, side_w)], ops.at[side, 1 + part], l_sem.at[side, 1 + part])

    def out_copy(dst, part):
        return pltpu.make_async_copy(acc.at[part], dst, o_sem.at[part])

    def out_push(dst, index, part):
        return pltpu.make_async_remote_copy(src_ref=acc.at[part], dst_ref=dst, send_sem=res_send.at[index, part], recv_sem=res_recv.at[index, part], device_id={"dp": peer}, device_id_type=MESH)

    def td_part(layer, part):
        return td_out.at[layer - 1, half_of(core), pl.ds(part * side_w, side_w)]

    def tu_part(layer, part):
        return tu_out.at[layer - 1, pl.ds(part * side_w, side_w), half_of(core)]

    def load_granule(q):
        index = q // (2 * SLOTS)
        kind, layer, slot, side = index % 2, top - index // 2, (q % (2 * SLOTS)) // 2, q % 2

        def start(half_src, full_src):
            half_load(half_src, side).start()
            for part in range(2):
                full_load(full_src, side, part).start()

        @pl.when((kind == 0) & (side == 0))
        def _():
            start(a_out.at[layer, chunk_rows(slot), half_of(core)], g_out.at[layer, chunk_rows(slot)])

        @pl.when((kind == 0) & (side == 1))
        def _():
            push_a(layer, slot).wait_recv()
            push_g(layer, slot).wait_recv()
            start(pa_out.at[layer, chunk_rows(slot)], pg_out.at[layer, chunk_rows(slot)])

        @pl.when((kind == 1) & (side == 0))
        def _():
            start(du_out.at[layer, chunk_rows(slot), half_of(core)], h_out.at[layer - 1, chunk_rows(slot)])

        @pl.when((kind == 1) & (side == 1))
        def _():
            push_d(layer, slot).wait_recv()
            push_h(layer, slot).wait_recv()
            start(pd_out.at[layer, chunk_rows(slot)], ph_out.at[layer, chunk_rows(slot)])

    def wait_outs(index):
        for part in range(2):
            out_copy(td_part(1, part), part).wait()
            out_push(td_part(1, part), index, part).wait_send()

    def run_granule(q):
        index = q // (2 * SLOTS)
        kind, layer, side = index % 2, top - index // 2, q % 2

        @pl.when((q % (2 * SLOTS) == 0) & (q > 0))
        def _():
            wait_outs(index - 1)

        @pl.when(q % (2 * SLOTS) == 0)
        def _():
            def clear(i, carry):
                strip = pl.ds(pl.multiple_of(i * 64, 64), 64)
                acc[:, strip, :] = jnp.zeros((2, 64, side_w), jnp.float32)
                return carry

            lax.fori_loop(0, side_w // 64, clear, 0)

        half_load(pa_out.at[0, chunk_rows(0)], side).wait()
        for part in range(2):
            full_load(pg_out.at[0, chunk_rows(0)], side, part).wait()

        def part_step(i, carry):
            part, strip = i // 2, pl.ds(pl.multiple_of(i % 2 * (side_w // 2), side_w // 2), side_w // 2)
            acc[part, strip] += dot_f32(ops[side, kind * (1 + part), :, strip], ops[side, (1 - kind) * (1 + part)], ROW_CONTRACT)
            return carry

        lax.fori_loop(0, 4, part_step, 0)

        @pl.when((q % (2 * SLOTS) == 2 * SLOTS - 1) & (kind == 0))
        def _():
            for part in range(2):
                out_copy(td_part(layer, part), part).start()
                out_push(td_part(layer, part), index, part).start()

        @pl.when((q % (2 * SLOTS) == 2 * SLOTS - 1) & (kind == 1))
        def _():
            for part in range(2):
                out_copy(tu_part(layer, part), part).start()
                out_push(tu_part(layer, part), index, part).start()

    plan = {1: (1, 0, 3), 2: (2, 0, 0), 3: (2, 0, 0), 4: (1, 2, 0), 5: (4, 1, 0), 6: (0, 3, 2), 7: (3, 0, 0), 8: (1, 4, 0), 9: (3, 0, 0), 10: (3, 3, 0), 11: (2, 0, 6)}
    ran = sum(sum(groups) for groups in plan.values())

    def plan_of(n):
        ends = [0, 0, 0, 0]
        for b, groups in plan.items():
            reached, passed = (n - b) // turn, (n - b - 1) // turn
            here = (n // turn) * (reached - passed)
            ends[0] = ends[0] + sum(groups) * passed
            for i, number in enumerate(groups):
                ends[i + 1] = ends[i + 1] + number * here
        for i in range(3):
            ends[i + 1] = ends[i + 1] + ends[i]
        return ends

    def run_granules(begin, end, stop):
        def step(q, carry):
            @pl.when(q + 1 < stop)
            def _():
                load_granule(q + 1)

            run_granule(q)
            return carry

        lax.fori_loop(begin, end, step, 0)

    def receive_rows(n):
        layer, slot = layer_of(n), n % SLOTS

        @pl.when(n < SLOTS)
        def _():
            x_load(slot).wait()

        @pl.when(n >= SLOTS)
        def _():
            for copy in gat2_copies(n):
                copy.wait()
            for copy in gat1_copies(n):
                copy.wait_send()

        @pl.when(n < turn)
        def _():
            push_h(layer, slot).start()

        @pl.when((n >= SLOTS) & (n < turn))
        def _():
            h_save(layer, slot).start()

        @pl.when(n >= turn)
        def _():
            push_g(layer, slot).start()
            g_save(layer, slot).start()

    def settle_rows(n):
        layer, slot = layer_of(n), n % SLOTS

        @pl.when(n < turn)
        def _():
            push_h(layer, slot).wait_send()

        @pl.when((n >= SLOTS) & (n < turn))
        def _():
            h_save(layer, slot).wait()

        @pl.when(n >= turn)
        def _():
            push_g(layer, slot).wait_send()
            g_save(layer, slot).wait()

    def share_acts(n):
        layer, slot = layer_of(n), n % SLOTS

        @pl.when(n < turn)
        def _():
            a_save(layer, slot).start()

        @pl.when((n >= turn) & (n < steps))
        def _():
            d_save(layer, slot).start()

        @pl.when(n < SLOTS)
        def _():
            push_a0(slot).start()

        @pl.when((n >= SLOTS) & (n < turn))
        def _():
            push_a(layer, slot).start()

        @pl.when((n >= turn) & (n < steps))
        def _():
            push_d(layer, slot).start()

    def settle_acts(n):
        layer, slot = layer_of(n), n % SLOTS
        a_save(layer, slot).wait()

        @pl.when(n < SLOTS)
        def _():
            push_a0(slot).wait_send()

        @pl.when((n >= SLOTS) & (n < turn))
        def _():
            push_a(layer, slot).wait_send()

        @pl.when((n >= turn) & (n < steps))
        def _():
            push_d(layer, slot).wait_send()

        @pl.when(n >= steps)
        def _():
            push_d0(slot).wait_send()

    def times_columns(source, stage):
        total = None
        for i in range(tiles):
            cols = pl.ds(i * TILE, TILE)
            part = dot_f32(source(cols), wbuf[stage, :, cols])
            total = part if total is None else total + part
        return total

    def forward_up(n):
        slot = n % SLOTS

        def tile_step(tile, carry):
            index = weight_base(n) + tile
            count = n * tiles + tile
            weight_start(index + 2)
            weight_wait(index)
            pre = times_columns(lambda cols: hbuf[slot, :, cols], index % 3).astype(jnp.bfloat16)

            @pl.when(count >= 2)
            def _():
                u_save(0, 0, count % 2).wait()

            ubuf[count % 2] = pre
            abuf[:, tile_of(tile)] = gelu_tanh(pre.astype(jnp.float32)).astype(jnp.bfloat16)
            u_save(n, tile, count % 2).start()
            return carry

        lax.fori_loop(0, tiles, tile_step, 0)

    def forward_down(n):
        def tile_step(tile, carry):
            index = weight_base(n) + tiles + tile
            weight_start(index + 2)
            weight_wait(index)
            pbuf[n % 2, :, tile_of(tile)] = times_columns(lambda cols: abuf[:, cols], index % 3)

            @pl.when(n == 0)
            def _():
                red1_tiles(tile)

            return carry

        lax.fori_loop(0, tiles, tile_step, 0)

    def backward_up(n):
        slot = n % SLOTS

        @pl.when(n == turn)
        def _():
            for stage in range(2):
                u_save(0, 0, stage).wait()
            u_load(n, 0, n * tiles % 2).start()

        def tile_step(tile, carry):
            index = weight_base(n) + tile
            count = n * tiles + tile
            weight_start(index + 2)

            @pl.when(count + 1 < every * tiles)
            def _():
                u_load((count + 1) // tiles, (count + 1) % tiles, (count + 1) % 2).start()

            weight_wait(index)
            u_load(n, tile, count % 2).wait()
            d_act = dot_f32(hbuf[slot], wbuf[index % 3], COL_CONTRACT)
            _, gelu_vjp = jax.vjp(gelu_tanh, ubuf[count % 2].astype(jnp.float32))
            abuf[:, tile_of(tile)] = gelu_vjp(d_act)[0].astype(jnp.bfloat16)

            @pl.when(n >= steps)
            def _():
                d0_tiles(slot, tile)

            return carry

        lax.fori_loop(0, tiles, tile_step, 0)

    def backward_down(n):
        def tile_step(tile, carry):
            index = weight_base(n) + tiles + tile
            weight_start(index + 2)
            weight_wait(index)
            pbuf[n % 2, :, tile_of(tile)] = dot_f32(abuf[...], wbuf[index % 3], COL_CONTRACT)
            return carry

        lax.fori_loop(0, tiles, tile_step, 0)

    def send_diagonal(n):
        @pl.when(n > 0)
        def _():
            for copy in red1_copies(n):
                copy.start()

    def reduce_step(k):
        first, second = red1_copies(k)
        first.wait_recv()
        pbuf[k % 2, rows_of(y_nbr, 0)] += red1[k % 2, 0]
        second.wait_recv()
        pbuf[k % 2, rows_of(x_nbr, 1)] += red1[k % 2, 1]
        for copy in red2_copies(k):
            copy.start()

        @pl.when((k >= turn - SLOTS) & (k < turn))
        def _():
            for copy in t_loads(k % SLOTS):
                copy.start()

    def finish_step(k):
        slot = k % SLOTS
        for copy in red2_copies(k):
            copy.wait()
        for copy in red1_copies(k):
            copy.wait_send()

        def total():
            return pbuf[k % 2, rows_of(me)] + red2[k % 2, 0] + red2[k % 2, 1]

        def h_new():
            return (hbuf[slot, rows_of(me)].astype(jnp.float32) + total().astype(jnp.bfloat16).astype(jnp.float32)).astype(jnp.bfloat16)

        @pl.when(k < turn - SLOTS)
        def _():
            hbuf[slot, rows_of(me)] = h_new()

        @pl.when((k >= turn - SLOTS) & (k < turn))
        def _():
            for copy in t_loads(slot):
                copy.wait()
            target = jnp.concatenate([ops[0, 1, :block], ops[0, 2, :block]], 1)
            err = (h_new().astype(jnp.float32) - target.astype(jnp.float32)) * (1.0 / total_tokens)
            hbuf[slot, rows_of(me)] = err.astype(jnp.bfloat16)

        @pl.when(k >= turn)
        def _():
            hbuf[slot, rows_of(me)] = (hbuf[slot, rows_of(me)].astype(jnp.float32) + total()).astype(jnp.bfloat16)

        for copy in gat1_copies(k):
            copy.start()

    def forward_rows(k):
        for copy in gat1_copies(k):
            copy.wait_recv()
        for copy in gat2_copies(k):
            copy.start()

    def when_step(k, fn):
        @pl.when((k >= 0) & (k < steps))
        def _():
            fn(k)

    barrier = pltpu.get_barrier_semaphore()
    for target in ({"tp": x_nbr}, {"tp": y_nbr}, {"dp": peer}):
        pl.semaphore_signal(barrier, inc=1, device_id=target, device_id_type=MESH)
    x_load(0).start()
    weight_start(0)
    weight_start(1)
    for slot in range(1, SLOTS):
        x_load(slot).start()
    pl.semaphore_wait(barrier, 3)

    def body(n, carry):
        begin, one, two, stop = plan_of(n)
        receive_rows(n)

        @pl.when(n >= 1)
        def _():
            settle_acts(n - 1)

        @pl.when(n < turn)
        def _():
            forward_up(n)

        @pl.when(n >= turn)
        def _():
            backward_up(n)

        when_step(n - 2, forward_rows)
        share_acts(n)
        settle_rows(n)

        @pl.when(begin < stop)
        def _():
            load_granule(begin)

        @pl.when(n < turn)
        def _():
            forward_down(n)

        @pl.when(n >= turn)
        def _():
            backward_down(n)

        send_diagonal(n)
        run_granules(begin, one, stop)
        when_step(n - 1, finish_step)
        run_granules(one, two, stop)
        reduce_step(n)
        run_granules(two, stop, stop)
        return carry

    lax.fori_loop(0, steps, body, 0)
    forward_rows(steps - 2)

    def last_body(n, carry):
        receive_rows(n)
        settle_acts(n - 1)

        @pl.when(n == steps)
        def _():
            load_granule(ran)

        backward_up(n)

        @pl.when(n == steps)
        def _():
            finish_step(steps - 1)
            run_granules(ran, granules, granules)

        @pl.when(n == steps + 1)
        def _():
            forward_rows(steps - 1)

        settle_rows(n)
        return carry

    lax.fori_loop(steps, every, last_body, 0)
    settle_acts(every - 1)
    wait_outs(2 * (layers - 1) - 1)
    for slot in range(SLOTS):
        push_a0(slot).wait_recv()
        push_d0(slot).wait_recv()
        push_g(0, slot).wait_recv()
        push_h(0, slot).wait_recv()
    for index in range(2 * (layers - 1)):
        for part in range(2):
            out_push(td_part(1, part), index, part).wait_recv()


def run_chain(hidden, targets, w_up, w_down, total_tokens):
    layers, d_model, width = w_up.shape
    tokens = hidden.shape[0]
    rows = tokens // SLOTS
    block = rows // 4
    half = width // 2
    bf16, f32 = jnp.bfloat16, jnp.float32
    flops = 2 * tokens * d_model * width * (6 * layers - 3)
    anywhere = pl.BlockSpec(memory_space=pl.ANY)
    like = jax.ShapeDtypeStruct
    outs = (like((layers - 1, tokens, d_model), bf16), like((layers, tokens, width), bf16), like((layers, tokens, width), bf16),
            like((layers, tokens, d_model), bf16), like((layers, tokens, width), bf16),
            like((layers - 1, width, d_model), f32), like((layers - 1, d_model, width), f32),
            like((layers, tokens, half), bf16), like((layers, tokens, half), bf16),
            like((layers, tokens, d_model), bf16), like((layers, tokens, d_model), bf16),
            like((tokens, width), bf16), like((tokens, width), bf16))
    return pl.pallas_call(
        functools.partial(chain_kernel, layers, total_tokens),
        out_shape=outs,
        in_specs=[anywhere] * 4,
        out_specs=(anywhere,) * len(outs),
        scratch_shapes=[
            pltpu.VMEM((SLOTS, rows, d_model), bf16),
            pltpu.VMEM((rows, width), bf16),
            pltpu.VMEM((2, rows, TILE), bf16),
            pltpu.VMEM((3, TILE, d_model), bf16),
            pltpu.VMEM((2, rows, d_model), f32),
            pltpu.VMEM((2, 2, block // 2, d_model), f32),
            pltpu.VMEM((2, 2, block, d_model), f32),
            pltpu.VMEM((2, half, half), f32),
            pltpu.VMEM((2, 3, rows, half), bf16),
            pltpu.SemaphoreType.DMA((8, SLOTS)),
            pltpu.SemaphoreType.DMA((8, SLOTS)),
            pltpu.SemaphoreType.DMA((4, layers, SLOTS)),
            pltpu.SemaphoreType.DMA((4, layers, SLOTS)),
            pltpu.SemaphoreType.DMA((2 * (layers - 1), 2)),
            pltpu.SemaphoreType.DMA((2 * (layers - 1), 2)),
            pltpu.SemaphoreType.DMA((3,)),
            pltpu.SemaphoreType.DMA((2,)),
            pltpu.SemaphoreType.DMA,
            pltpu.SemaphoreType.DMA((SLOTS,)),
            pltpu.SemaphoreType.DMA((2,)),
            pltpu.SemaphoreType.DMA((2, 3)),
            pltpu.SemaphoreType.DMA((2,)),
        ],
        compiler_params=pltpu.CompilerParams(collective_id=0, has_side_effects=True, vmem_limit_bytes=67043328),
        cost_estimate=pl.CostEstimate(flops=flops, bytes_accessed=layers * tokens * d_model * 16, transcendentals=2 * layers * tokens * width),
        name="step_chain",
    )(hidden, targets, w_up, w_down)


def final_kernel(a_ref, pa_ref, g_ref, pg_ref, x_ref, px_ref, d_ref, pd_ref, td_ref, tu_ref, gd_out, gu_out, acc, lhs, rhs, ring, l_sem, r_sem, o_sem, in_sem, out_sem):
    rows, side_w = lhs.shape[2:]
    strip = ring.shape[1]
    depth = ring.shape[0]
    done_layers, height, _ = td_ref.shape
    per_layer = height // strip
    per_array = done_layers * per_layer
    strips = 2 * per_array
    lag = depth // 2
    core = lax.axis_index("dp")
    a_ref, g_ref, pg_ref, px_ref, d_ref = (ref.at[0] for ref in (a_ref, g_ref, pg_ref, px_ref, d_ref))
    parts = 4
    granules = 4 * SLOTS
    per_grad = granules // 2

    def chunk_rows(slot):
        return pl.ds(pl.multiple_of(slot * rows, rows), rows)

    def half_of(which):
        return pl.ds(pl.multiple_of(which * side_w, side_w), side_w)

    def operand_copies(left, right, slot, stage):
        for part in range(2):
            cols = pl.ds(part * side_w, side_w)
            yield pltpu.make_async_copy(left.at[chunk_rows(slot), cols], lhs.at[stage, part], l_sem.at[stage, part])
            yield pltpu.make_async_copy(right.at[chunk_rows(slot), cols], rhs.at[stage, part], r_sem.at[stage, part])

    def load(q):
        grad, slot, side = q // per_grad, (q % per_grad) // 2, q % 2
        for which, mine, theirs in ((0, (a_ref, g_ref), (pa_ref, pg_ref)), (1, (x_ref, d_ref), (px_ref, pd_ref))):
            @pl.when((grad == which) & (side == core))
            def _():
                for copy in operand_copies(*mine, slot, q % 2):
                    copy.start()

            @pl.when((grad == which) & (side != core))
            def _():
                for copy in operand_copies(*theirs, slot, q % 2):
                    copy.start()

    def out_copy(dst, part):
        return pltpu.make_async_copy(acc.at[part], dst.at[0, half_of(part // 2), half_of(part % 2)], o_sem.at[part])

    def strip_copies(t, src, dst):
        layer, row = (t % per_array) // per_layer, pl.multiple_of((t % per_layer) * strip, strip)
        return (pltpu.make_async_copy(src.at[layer, pl.ds(row, strip)], ring.at[t % depth], in_sem.at[t % depth]),
                pltpu.make_async_copy(ring.at[t % depth], dst.at[layer + 1, pl.ds(row, strip)], out_sem.at[t % depth]))

    def move(t):
        @pl.when((t >= depth) & (t < strips + depth))
        def _():
            strip_copies(t - depth, td_ref, gd_out)[1].wait()

        @pl.when(t < per_array)
        def _():
            strip_copies(t, td_ref, gd_out)[0].start()

        @pl.when((t >= per_array) & (t < strips))
        def _():
            strip_copies(t, tu_ref, gu_out)[0].start()

        late = t - lag

        @pl.when((late >= 0) & (late < per_array))
        def _():
            strip_copies(late, td_ref, gd_out)[0].wait()
            strip_copies(late, td_ref, gd_out)[1].start()

        @pl.when((late >= per_array) & (late < strips))
        def _():
            strip_copies(late, tu_ref, gu_out)[0].wait()
            strip_copies(late, tu_ref, gu_out)[1].start()

    def compute(p):
        q, part = p // parts, p % parts
        stage = q % 2

        @pl.when((part == 0) & (q + 1 < granules))
        def _():
            load(q + 1)

        @pl.when(part == 0)
        def _():
            for copy in operand_copies(a_ref, g_ref, 0, stage):
                copy.wait()

        @pl.when(q == per_grad)
        def _():
            out_copy(gd_out, part).wait()

        @pl.when(q % per_grad == 0)
        def _():
            acc[part] = dot_f32(lhs[stage, part // 2], rhs[stage, part % 2], ROW_CONTRACT)

        @pl.when(q % per_grad > 0)
        def _():
            acc[part] += dot_f32(lhs[stage, part // 2], rhs[stage, part % 2], ROW_CONTRACT)

        @pl.when(q == per_grad - 1)
        def _():
            out_copy(gd_out, part).start()

        @pl.when(q == granules - 1)
        def _():
            out_copy(gu_out, part).start()

    load(0)

    def body(p, carry):
        move(p)
        compute(p)
        return carry

    lax.fori_loop(0, parts * granules, body, 0)

    def flush(t, carry):
        move(t)
        return carry

    lax.fori_loop(parts * granules, max(strips + depth, parts * granules), flush, 0)
    for part in range(parts):
        out_copy(gu_out, part).wait()


def run_final(operands, t_down, t_up):
    layers, width, d_model = t_down.shape[0] + 1, t_down.shape[1], t_down.shape[2]
    tokens = operands[1].shape[0]
    rows, side_w = tokens // SLOTS, width // 2
    bf16, f32 = jnp.bfloat16, jnp.float32
    anywhere = pl.BlockSpec(memory_space=pl.ANY)
    return pl.pallas_call(
        final_kernel,
        out_shape=(jax.ShapeDtypeStruct((layers, width, d_model), f32), jax.ShapeDtypeStruct((layers, d_model, width), f32)),
        in_specs=[anywhere] * 10,
        out_specs=(anywhere,) * 2,
        scratch_shapes=[
            pltpu.VMEM((4, side_w, side_w), f32),
            pltpu.VMEM((2, 2, rows, side_w), bf16),
            pltpu.VMEM((2, 2, rows, side_w), bf16),
            pltpu.VMEM((8, 256, d_model), f32),
            pltpu.SemaphoreType.DMA((2, 2)),
            pltpu.SemaphoreType.DMA((2, 2)),
            pltpu.SemaphoreType.DMA((4,)),
            pltpu.SemaphoreType.DMA((8,)),
            pltpu.SemaphoreType.DMA((8,)),
        ],
        compiler_params=pltpu.CompilerParams(vmem_limit_bytes=67043328),
        cost_estimate=pl.CostEstimate(flops=8 * tokens * d_model * width, bytes_accessed=16 * layers * d_model * width, transcendentals=0),
        name="final_grads",
    )(*operands, t_down, t_up)


def local_step(hidden, targets, w_up, w_down, total_tokens):
    _, _, act_all, g_all, d_all, t_down, t_up, _, _, pg, ph, pa0, pd0 = run_chain(hidden, targets, w_up, w_down, total_tokens)
    grad_down, grad_up = run_final((act_all, pa0, g_all, pg, hidden, ph, d_all, pd0), t_down, t_up)
    return grad_up, grad_down


def solution(mesh):
    def grad_step(hidden_in, targets, w_up, w_down):
        step_fn = functools.partial(local_step, total_tokens=hidden_in.shape[0])
        mapped = jax.shard_map(step_fn, mesh=mesh, in_specs=(P("dp", None), P("dp", None), P(None, None, "tp"), P(None, "tp", None)), out_specs=(P(None, None, "tp"), P(None, "tp", None)), check_vma=False)
        return mapped(hidden_in, targets, w_up, w_down)

    return grad_step
```

```python
import functools
import jax
import jax.numpy as jnp
from jax import lax
from jax.experimental import pallas as pl
from jax.experimental.pallas import tpu as pltpu
from jax.sharding import PartitionSpec as P

ROW_CONTRACT = (((0,), (0,)), ((), ()))
COL_CONTRACT = (((1,), (1,)), ((), ()))
MESH = pl.DeviceIdType.MESH
SLOTS = 4
TILE = 512
RED1_X, RED1_Y, RED2_X, RED2_Y, GAT1_X, GAT1_Y, GAT2_X, GAT2_Y = range(8)


def gelu_tanh(value):
    return jax.nn.gelu(value, approximate=True)


def dot_f32(lhs, rhs, dims=(((1,), (0,)), ((), ()))):
    return lax.dot_general(lhs, rhs, dims, preferred_element_type=jnp.float32)


PUSH_A, PUSH_D, PUSH_G, PUSH_H = range(4)


def chain_kernel(layers, total_tokens, x_ref, t_ref, wu_ref, wd_ref,
                 h_out, u_out, a_out, g_out, du_out, td_out, tu_out, pa_out, pd_out, pg_out, ph_out, pa0_out, pd0_out,
                 hbuf, abuf, ubuf, wbuf, pbuf, red1, red2, acc, ops,
                 send_sem, recv_sem, push_send, push_recv, res_send, res_recv, w_sem, u_sem, a_sem, h_sem, t_sem, l_sem, o_sem):
    rows, d_model = hbuf.shape[1:]
    block = rows // 4
    half = block // 2
    tiles = d_model // TILE
    side_w = d_model // 2
    turn = layers * SLOTS
    steps = turn + (layers - 1) * SLOTS
    every = steps + SLOTS
    top = layers - 1
    granules = 2 * (layers - 1) * 2 * SLOTS
    me = lax.axis_index("tp")
    core = lax.axis_index("dp")
    peer = 1 - core
    mx, my = me % 2, me // 2
    x_nbr = my * 2 + (1 - mx)
    y_nbr = (1 - my) * 2 + mx
    diag = (1 - my) * 2 + (1 - mx)

    def rows_of(owner, part=None):
        if part is None:
            return pl.ds(pl.multiple_of(owner * block, block), block)
        return pl.ds(pl.multiple_of(owner * block + part * half, half), half)

    def chunk_rows(slot):
        return pl.ds(pl.multiple_of(slot * rows, rows), rows)

    def half_of(which):
        return pl.ds(pl.multiple_of(which * side_w, side_w), side_w)

    def tile_of(tile):
        return pl.ds(pl.multiple_of(tile * TILE, TILE), TILE)

    def layer_of(n):
        back = n // turn
        return (1 - back) * (n // SLOTS) + back * (2 * layers - 1 - n // SLOTS)

    def remote(kind, k, src, dst, target):
        return pltpu.make_async_remote_copy(src_ref=src, dst_ref=dst, send_sem=send_sem.at[kind, k % SLOTS], recv_sem=recv_sem.at[kind, k % SLOTS], device_id={"tp": target}, device_id_type=MESH)

    def red1_copies(k):
        return (remote(RED1_X, k, pbuf.at[k % 2, rows_of(diag, 0)], red1.at[k % 2, 0], x_nbr),
                remote(RED1_Y, k, pbuf.at[k % 2, rows_of(diag, 1)], red1.at[k % 2, 1], y_nbr))

    def red1_tiles(tile):
        for kind, part, target in ((RED1_X, 0, x_nbr), (RED1_Y, 1, y_nbr)):
            remote(kind, 0, pbuf.at[0, rows_of(diag, part), tile_of(tile)], red1.at[0, part, :, tile_of(tile)], target).start()

    def red2_copies(k):
        return (remote(RED2_X, k, pbuf.at[k % 2, rows_of(x_nbr)], red2.at[k % 2, 0], x_nbr),
                remote(RED2_Y, k, pbuf.at[k % 2, rows_of(y_nbr)], red2.at[k % 2, 1], y_nbr))

    def gat1_copies(k):
        mine = hbuf.at[k % SLOTS, rows_of(me)]
        return (remote(GAT1_X, k, mine, mine, x_nbr), remote(GAT1_Y, k, mine, mine, y_nbr))

    def gat2_copies(k):
        from_y = hbuf.at[k % SLOTS, rows_of(y_nbr, 0)]
        from_x = hbuf.at[k % SLOTS, rows_of(x_nbr, 1)]
        return (remote(GAT2_X, k, from_y, from_y, x_nbr), remote(GAT2_Y, k, from_x, from_x, y_nbr))

    def push(kind, layer, slot, src, dst):
        return pltpu.make_async_remote_copy(src_ref=src, dst_ref=dst, send_sem=push_send.at[kind, layer, slot], recv_sem=push_recv.at[kind, layer, slot], device_id={"dp": peer}, device_id_type=MESH)

    def push_a(layer, slot):
        return push(PUSH_A, layer, slot, abuf.at[:, half_of(peer)], pa_out.at[layer, chunk_rows(slot)])

    def push_d(layer, slot):
        return push(PUSH_D, layer, slot, abuf.at[:, half_of(peer)], pd_out.at[layer, chunk_rows(slot)])

    def push_a0(slot):
        return push(PUSH_A, 0, slot, abuf, pa0_out.at[chunk_rows(slot)])

    def d0_tiles(slot, tile):
        part = abuf.at[:, tile_of(tile)]
        push(PUSH_D, 0, slot, part, pd0_out.at[chunk_rows(slot), tile_of(tile)]).start()
        pltpu.make_async_copy(part, du_out.at[0, chunk_rows(slot), tile_of(tile)], a_sem).start()

    def push_d0(slot):
        return push(PUSH_D, 0, slot, abuf, pd0_out.at[chunk_rows(slot)])

    def push_g(layer, slot):
        return push(PUSH_G, layer, slot, hbuf.at[slot], pg_out.at[layer, chunk_rows(slot)])

    def push_h(layer, slot):
        return push(PUSH_H, layer, slot, hbuf.at[slot], ph_out.at[layer, chunk_rows(slot)])

    def weight_copy(ref, layer, tile, stage):
        return pltpu.make_async_copy(ref.at[layer, tile_of(tile)], wbuf.at[stage], w_sem.at[stage])

    def column_copies(ref, layer, tile, stage):
        for i in range(tiles):
            block_rows = pl.ds(i * TILE, TILE)
            pltpu.make_async_copy(ref.at[layer, block_rows, tile_of(tile)], wbuf.at[stage, :, block_rows], w_sem.at[stage]).start()

    def weight_start(index):
        main = steps * 2 * tiles
        n, place = index // (2 * tiles), index % (2 * tiles)
        up = 1 - place // tiles
        use_up = (1 - n // turn) * up + (n // turn) * (1 - up)

        @pl.when((n < turn) & (use_up == 1))
        def _():
            column_copies(wu_ref, layer_of(n), place % tiles, index % 3)

        @pl.when((n < turn) & (use_up == 0))
        def _():
            column_copies(wd_ref, layer_of(n), place % tiles, index % 3)

        @pl.when((n >= turn) & (index < main) & (use_up == 1))
        def _():
            weight_copy(wu_ref, layer_of(n), place % tiles, index % 3).start()

        @pl.when((n >= turn) & (index < main) & (use_up == 0))
        def _():
            weight_copy(wd_ref, layer_of(n), place % tiles, index % 3).start()

        @pl.when((index >= main) & (index < main + SLOTS * tiles))
        def _():
            weight_copy(wd_ref, 0, (index - main) % tiles, index % 3).start()

    def weight_wait(index):
        weight_copy(wu_ref, 0, 0, index % 3).wait()

    def weight_base(n):
        late = (n // steps) * (n - steps)
        return (n - late) * 2 * tiles + late * tiles

    def u_save(n, tile, stage):
        return pltpu.make_async_copy(ubuf.at[stage], u_out.at[layer_of(n), chunk_rows(n % SLOTS), tile_of(tile)], u_sem.at[stage])

    def u_load(n, tile, stage):
        return pltpu.make_async_copy(u_out.at[layer_of(n), chunk_rows(n % SLOTS), tile_of(tile)], ubuf.at[stage], u_sem.at[stage])

    def x_load(slot):
        return pltpu.make_async_copy(x_ref.at[chunk_rows(slot)], hbuf.at[slot], h_sem.at[slot])

    def h_save(layer, slot):
        return pltpu.make_async_copy(hbuf.at[slot], h_out.at[layer - 1, chunk_rows(slot)], h_sem.at[slot])

    def g_save(layer, slot):
        return pltpu.make_async_copy(hbuf.at[slot], g_out.at[layer, chunk_rows(slot)], h_sem.at[slot])

    def a_save(layer, slot):
        return pltpu.make_async_copy(abuf, a_out.at[layer, chunk_rows(slot)], a_sem)

    def d_save(layer, slot):
        return pltpu.make_async_copy(abuf, du_out.at[layer, chunk_rows(slot)], a_sem)

    def t_loads(slot):
        own = pl.ds(pl.multiple_of(slot * rows + me * block, block), block)
        return [pltpu.make_async_copy(t_ref.at[own, pl.ds(part * side_w, side_w)], ops.at[0, 1 + part, pl.ds(0, block)], t_sem.at[part]) for part in range(2)]

    def half_load(src, side):
        return pltpu.make_async_copy(src, ops.at[side, 0], l_sem.at[side, 0])

    def full_load(src, side, part):
        return pltpu.make_async_copy(src.at[:, pl.ds(part * side_w, side_w)], ops.at[side, 1 + part], l_sem.at[side, 1 + part])

    def out_copy(dst, part):
        return pltpu.make_async_copy(acc.at[part], dst, o_sem.at[part])

    def out_push(dst, index, part):
        return pltpu.make_async_remote_copy(src_ref=acc.at[part], dst_ref=dst, send_sem=res_send.at[index, part], recv_sem=res_recv.at[index, part], device_id={"dp": peer}, device_id_type=MESH)

    def td_part(layer, part):
        return td_out.at[layer - 1, half_of(core), pl.ds(part * side_w, side_w)]

    def tu_part(layer, part):
        return tu_out.at[layer - 1, pl.ds(part * side_w, side_w), half_of(core)]

    def load_granule(q):
        index = q // (2 * SLOTS)
        kind, layer, slot, side = index % 2, top - index // 2, (q % (2 * SLOTS)) // 2, q % 2

        def start(half_src, full_src):
            half_load(half_src, side).start()
            for part in range(2):
                full_load(full_src, side, part).start()

        @pl.when((kind == 0) & (side == 0))
        def _():
            start(a_out.at[layer, chunk_rows(slot), half_of(core)], g_out.at[layer, chunk_rows(slot)])

        @pl.when((kind == 0) & (side == 1))
        def _():
            push_a(layer, slot).wait_recv()
            push_g(layer, slot).wait_recv()
            start(pa_out.at[layer, chunk_rows(slot)], pg_out.at[layer, chunk_rows(slot)])

        @pl.when((kind == 1) & (side == 0))
        def _():
            start(du_out.at[layer, chunk_rows(slot), half_of(core)], h_out.at[layer - 1, chunk_rows(slot)])

        @pl.when((kind == 1) & (side == 1))
        def _():
            push_d(layer, slot).wait_recv()
            push_h(layer, slot).wait_recv()
            start(pd_out.at[layer, chunk_rows(slot)], ph_out.at[layer, chunk_rows(slot)])

    def wait_out(index, part):
        out_copy(td_part(1, 0), part).wait()
        out_push(td_part(1, 0), index, part).wait_send()

    def run_granule(q):
        index = q // (2 * SLOTS)
        kind, layer, side = index % 2, top - index // 2, q % 2

        def open_part(part):
            @pl.when(q > 0)
            def _():
                wait_out(index - 1, part)

            def clear(i, carry):
                strip = pl.ds(pl.multiple_of(i * 64, 64), 64)
                acc[part, strip, :] = jnp.zeros((64, side_w), jnp.float32)
                return carry

            lax.fori_loop(0, side_w // 64, clear, 0)

        half_load(pa_out.at[0, chunk_rows(0)], side).wait()
        for part in range(2):
            full_load(pg_out.at[0, chunk_rows(0)], side, part).wait()

        def part_step(i, carry):
            part, strip = i // 2, pl.ds(pl.multiple_of(i % 2 * (side_w // 2), side_w // 2), side_w // 2)

            @pl.when((q % (2 * SLOTS) == 0) & (i % 2 == 0))
            def _():
                open_part(part)

            acc[part, strip] += dot_f32(ops[side, kind * (1 + part), :, strip], ops[side, (1 - kind) * (1 + part)], ROW_CONTRACT)
            return carry

        lax.fori_loop(0, 4, part_step, 0)

        @pl.when((q % (2 * SLOTS) == 2 * SLOTS - 1) & (kind == 0))
        def _():
            for part in range(2):
                out_copy(td_part(layer, part), part).start()
                out_push(td_part(layer, part), index, part).start()

        @pl.when((q % (2 * SLOTS) == 2 * SLOTS - 1) & (kind == 1))
        def _():
            for part in range(2):
                out_copy(tu_part(layer, part), part).start()
                out_push(tu_part(layer, part), index, part).start()

    plan = {1: (0, 1, 0, 3), 2: (0, 2, 0, 0), 3: (0, 2, 0, 0), 4: (0, 1, 2, 0), 5: (0, 4, 1, 0), 6: (0, 0, 3, 2), 7: (0, 3, 0, 0), 8: (0, 1, 4, 0), 9: (0, 3, 0, 0), 10: (0, 3, 3, 0), 11: (2, 0, 0, 6)}
    ran = sum(sum(groups) for groups in plan.values())

    def plan_of(n):
        ends = [0, 0, 0, 0, 0]
        for b, groups in plan.items():
            reached, passed = (n - b) // turn, (n - b - 1) // turn
            here = (n // turn) * (reached - passed)
            ends[0] = ends[0] + sum(groups) * passed
            for i, number in enumerate(groups):
                ends[i + 1] = ends[i + 1] + number * here
        for i in range(4):
            ends[i + 1] = ends[i + 1] + ends[i]
        return ends

    def run_granules(begin, end, stop):
        def step(q, carry):
            @pl.when(q + 1 < stop)
            def _():
                load_granule(q + 1)

            run_granule(q)
            return carry

        lax.fori_loop(begin, end, step, 0)

    def receive_rows(n):
        layer, slot = layer_of(n), n % SLOTS

        @pl.when(n < SLOTS)
        def _():
            x_load(slot).wait()

        @pl.when(n >= SLOTS)
        def _():
            for copy in gat2_copies(n):
                copy.wait()
            for copy in gat1_copies(n):
                copy.wait_send()

        @pl.when(n < turn)
        def _():
            push_h(layer, slot).start()

        @pl.when((n >= SLOTS) & (n < turn))
        def _():
            h_save(layer, slot).start()

        @pl.when(n >= turn)
        def _():
            push_g(layer, slot).start()
            g_save(layer, slot).start()

    def settle_rows(n):
        layer, slot = layer_of(n), n % SLOTS

        @pl.when(n < turn)
        def _():
            push_h(layer, slot).wait_send()

        @pl.when((n >= SLOTS) & (n < turn))
        def _():
            h_save(layer, slot).wait()

        @pl.when(n >= turn)
        def _():
            push_g(layer, slot).wait_send()
            g_save(layer, slot).wait()

    def share_acts(n):
        layer, slot = layer_of(n), n % SLOTS

        @pl.when(n < turn)
        def _():
            a_save(layer, slot).start()

        @pl.when((n >= turn) & (n < steps))
        def _():
            d_save(layer, slot).start()

        @pl.when(n < SLOTS)
        def _():
            push_a0(slot).start()

        @pl.when((n >= SLOTS) & (n < turn))
        def _():
            push_a(layer, slot).start()

        @pl.when((n >= turn) & (n < steps))
        def _():
            push_d(layer, slot).start()

    def settle_acts(n):
        layer, slot = layer_of(n), n % SLOTS
        a_save(layer, slot).wait()

        @pl.when(n < SLOTS)
        def _():
            push_a0(slot).wait_send()

        @pl.when((n >= SLOTS) & (n < turn))
        def _():
            push_a(layer, slot).wait_send()

        @pl.when((n >= turn) & (n < steps))
        def _():
            push_d(layer, slot).wait_send()

        @pl.when(n >= steps)
        def _():
            push_d0(slot).wait_send()

    def times_columns(source, stage):
        total = None
        for i in range(tiles):
            cols = pl.ds(i * TILE, TILE)
            part = dot_f32(source(cols), wbuf[stage, :, cols])
            total = part if total is None else total + part
        return total

    def forward_up(n):
        slot = n % SLOTS

        def tile_step(tile, carry):
            index = weight_base(n) + tile
            count = n * tiles + tile
            weight_start(index + 2)
            weight_wait(index)
            pre = times_columns(lambda cols: hbuf[slot, :, cols], index % 3).astype(jnp.bfloat16)

            @pl.when(count >= 2)
            def _():
                u_save(0, 0, count % 2).wait()

            ubuf[count % 2] = pre
            abuf[:, tile_of(tile)] = gelu_tanh(pre.astype(jnp.float32)).astype(jnp.bfloat16)
            u_save(n, tile, count % 2).start()
            return carry

        lax.fori_loop(0, tiles, tile_step, 0)

    def forward_down(n):
        def tile_step(tile, carry):
            index = weight_base(n) + tiles + tile
            weight_start(index + 2)
            weight_wait(index)
            pbuf[n % 2, :, tile_of(tile)] = times_columns(lambda cols: abuf[:, cols], index % 3)

            @pl.when(n == 0)
            def _():
                red1_tiles(tile)

            return carry

        lax.fori_loop(0, tiles, tile_step, 0)

    def backward_up(n):
        slot = n % SLOTS

        @pl.when(n == turn)
        def _():
            for stage in range(2):
                u_save(0, 0, stage).wait()
            u_load(n, 0, n * tiles % 2).start()

        def tile_step(tile, carry):
            index = weight_base(n) + tile
            count = n * tiles + tile
            weight_start(index + 2)

            @pl.when(count + 1 < every * tiles)
            def _():
                u_load((count + 1) // tiles, (count + 1) % tiles, (count + 1) % 2).start()

            weight_wait(index)
            u_load(n, tile, count % 2).wait()
            d_act = dot_f32(hbuf[slot], wbuf[index % 3], COL_CONTRACT)
            _, gelu_vjp = jax.vjp(gelu_tanh, ubuf[count % 2].astype(jnp.float32))
            abuf[:, tile_of(tile)] = gelu_vjp(d_act)[0].astype(jnp.bfloat16)

            @pl.when(n >= steps)
            def _():
                d0_tiles(slot, tile)

            return carry

        lax.fori_loop(0, tiles, tile_step, 0)

    def backward_down(n):
        def tile_step(tile, carry):
            index = weight_base(n) + tiles + tile
            weight_start(index + 2)
            weight_wait(index)
            pbuf[n % 2, :, tile_of(tile)] = dot_f32(abuf[...], wbuf[index % 3], COL_CONTRACT)
            return carry

        lax.fori_loop(0, tiles, tile_step, 0)

    def send_diagonal(n):
        @pl.when(n > 0)
        def _():
            for copy in red1_copies(n):
                copy.start()

    def reduce_step(k):
        first, second = red1_copies(k)
        first.wait_recv()
        pbuf[k % 2, rows_of(y_nbr, 0)] += red1[k % 2, 0]
        second.wait_recv()
        pbuf[k % 2, rows_of(x_nbr, 1)] += red1[k % 2, 1]
        for copy in red2_copies(k):
            copy.start()

        @pl.when((k >= turn - SLOTS) & (k < turn))
        def _():
            for copy in t_loads(k % SLOTS):
                copy.start()

    def finish_step(k):
        slot = k % SLOTS
        for copy in red2_copies(k):
            copy.wait()
        for copy in red1_copies(k):
            copy.wait_send()

        def total():
            return pbuf[k % 2, rows_of(me)] + red2[k % 2, 0] + red2[k % 2, 1]

        def h_new():
            return (hbuf[slot, rows_of(me)].astype(jnp.float32) + total().astype(jnp.bfloat16).astype(jnp.float32)).astype(jnp.bfloat16)

        @pl.when(k < turn - SLOTS)
        def _():
            hbuf[slot, rows_of(me)] = h_new()

        @pl.when((k >= turn - SLOTS) & (k < turn))
        def _():
            for copy in t_loads(slot):
                copy.wait()
            target = jnp.concatenate([ops[0, 1, :block], ops[0, 2, :block]], 1)
            err = (h_new().astype(jnp.float32) - target.astype(jnp.float32)) * (1.0 / total_tokens)
            hbuf[slot, rows_of(me)] = err.astype(jnp.bfloat16)

        @pl.when(k >= turn)
        def _():
            hbuf[slot, rows_of(me)] = (hbuf[slot, rows_of(me)].astype(jnp.float32) + total()).astype(jnp.bfloat16)

        for copy in gat1_copies(k):
            copy.start()

    def forward_rows(k):
        for copy in gat1_copies(k):
            copy.wait_recv()
        for copy in gat2_copies(k):
            copy.start()

    def when_step(k, fn):
        @pl.when((k >= 0) & (k < steps))
        def _():
            fn(k)

    barrier = pltpu.get_barrier_semaphore()
    for target in ({"tp": x_nbr}, {"tp": y_nbr}, {"dp": peer}):
        pl.semaphore_signal(barrier, inc=1, device_id=target, device_id_type=MESH)
    x_load(0).start()
    weight_start(0)
    weight_start(1)
    for slot in range(1, SLOTS):
        x_load(slot).start()
    pl.semaphore_wait(barrier, 3)

    def body(n, carry):
        begin, one, two, three, stop = plan_of(n)
        receive_rows(n)

        @pl.when(n >= 1)
        def _():
            settle_acts(n - 1)

        @pl.when(n < turn)
        def _():
            forward_up(n)

        @pl.when(n >= turn)
        def _():
            backward_up(n)

        when_step(n - 2, forward_rows)
        share_acts(n)
        settle_rows(n)

        @pl.when(begin < stop)
        def _():
            load_granule(begin)

        run_granules(begin, one, stop)

        @pl.when(n < turn)
        def _():
            forward_down(n)

        @pl.when(n >= turn)
        def _():
            backward_down(n)

        send_diagonal(n)
        run_granules(one, two, stop)
        when_step(n - 1, finish_step)
        run_granules(two, three, stop)
        reduce_step(n)
        run_granules(three, stop, stop)
        return carry

    lax.fori_loop(0, steps, body, 0)
    forward_rows(steps - 2)

    def last_body(n, carry):
        receive_rows(n)
        settle_acts(n - 1)

        @pl.when(n == steps)
        def _():
            load_granule(ran)

        backward_up(n)

        @pl.when(n == steps)
        def _():
            finish_step(steps - 1)
            run_granules(ran, granules, granules)

        @pl.when(n == steps + 1)
        def _():
            forward_rows(steps - 1)

        settle_rows(n)
        return carry

    lax.fori_loop(steps, every, last_body, 0)
    settle_acts(every - 1)
    for part in range(2):
        wait_out(2 * (layers - 1) - 1, part)
    for slot in range(SLOTS):
        push_a0(slot).wait_recv()
        push_d0(slot).wait_recv()
        push_g(0, slot).wait_recv()
        push_h(0, slot).wait_recv()
    for index in range(2 * (layers - 1)):
        for part in range(2):
            out_push(td_part(1, part), index, part).wait_recv()


def run_chain(hidden, targets, w_up, w_down, total_tokens):
    layers, d_model, width = w_up.shape
    tokens = hidden.shape[0]
    rows = tokens // SLOTS
    block = rows // 4
    half = width // 2
    bf16, f32 = jnp.bfloat16, jnp.float32
    flops = 2 * tokens * d_model * width * (6 * layers - 3)
    anywhere = pl.BlockSpec(memory_space=pl.ANY)
    like = jax.ShapeDtypeStruct
    outs = (like((layers - 1, tokens, d_model), bf16), like((layers, tokens, width), bf16), like((layers, tokens, width), bf16),
            like((layers, tokens, d_model), bf16), like((layers, tokens, width), bf16),
            like((layers - 1, width, d_model), f32), like((layers - 1, d_model, width), f32),
            like((layers, tokens, half), bf16), like((layers, tokens, half), bf16),
            like((layers, tokens, d_model), bf16), like((layers, tokens, d_model), bf16),
            like((tokens, width), bf16), like((tokens, width), bf16))
    return pl.pallas_call(
        functools.partial(chain_kernel, layers, total_tokens),
        out_shape=outs,
        in_specs=[anywhere] * 4,
        out_specs=(anywhere,) * len(outs),
        scratch_shapes=[
            pltpu.VMEM((SLOTS, rows, d_model), bf16),
            pltpu.VMEM((rows, width), bf16),
            pltpu.VMEM((2, rows, TILE), bf16),
            pltpu.VMEM((3, TILE, d_model), bf16),
            pltpu.VMEM((2, rows, d_model), f32),
            pltpu.VMEM((2, 2, block // 2, d_model), f32),
            pltpu.VMEM((2, 2, block, d_model), f32),
            pltpu.VMEM((2, half, half), f32),
            pltpu.VMEM((2, 3, rows, half), bf16),
            pltpu.SemaphoreType.DMA((8, SLOTS)),
            pltpu.SemaphoreType.DMA((8, SLOTS)),
            pltpu.SemaphoreType.DMA((4, layers, SLOTS)),
            pltpu.SemaphoreType.DMA((4, layers, SLOTS)),
            pltpu.SemaphoreType.DMA((2 * (layers - 1), 2)),
            pltpu.SemaphoreType.DMA((2 * (layers - 1), 2)),
            pltpu.SemaphoreType.DMA((3,)),
            pltpu.SemaphoreType.DMA((2,)),
            pltpu.SemaphoreType.DMA,
            pltpu.SemaphoreType.DMA((SLOTS,)),
            pltpu.SemaphoreType.DMA((2,)),
            pltpu.SemaphoreType.DMA((2, 3)),
            pltpu.SemaphoreType.DMA((2,)),
        ],
        compiler_params=pltpu.CompilerParams(collective_id=0, has_side_effects=True, vmem_limit_bytes=67043328),
        cost_estimate=pl.CostEstimate(flops=flops, bytes_accessed=layers * tokens * d_model * 16, transcendentals=2 * layers * tokens * width),
        name="step_chain",
    )(hidden, targets, w_up, w_down)


def final_kernel(a_ref, pa_ref, g_ref, pg_ref, x_ref, px_ref, d_ref, pd_ref, td_ref, tu_ref, gd_out, gu_out, acc, lhs, rhs, ring, l_sem, r_sem, o_sem, in_sem, out_sem):
    rows, side_w = lhs.shape[2:]
    strip = ring.shape[1]
    depth = ring.shape[0]
    done_layers, height, _ = td_ref.shape
    per_layer = height // strip
    per_array = done_layers * per_layer
    strips = 2 * per_array
    lag = depth // 2
    core = lax.axis_index("dp")
    a_ref, g_ref, pg_ref, px_ref, d_ref = (ref.at[0] for ref in (a_ref, g_ref, pg_ref, px_ref, d_ref))
    parts = 4
    granules = 4 * SLOTS
    per_grad = granules // 2

    def chunk_rows(slot):
        return pl.ds(pl.multiple_of(slot * rows, rows), rows)

    def half_of(which):
        return pl.ds(pl.multiple_of(which * side_w, side_w), side_w)

    def operand_copies(left, right, slot, stage):
        for part in range(2):
            cols = pl.ds(part * side_w, side_w)
            yield pltpu.make_async_copy(left.at[chunk_rows(slot), cols], lhs.at[stage, part], l_sem.at[stage, part])
            yield pltpu.make_async_copy(right.at[chunk_rows(slot), cols], rhs.at[stage, part], r_sem.at[stage, part])

    def load(q):
        grad, slot, side = q // per_grad, (q % per_grad) // 2, q % 2
        for which, mine, theirs in ((0, (a_ref, g_ref), (pa_ref, pg_ref)), (1, (x_ref, d_ref), (px_ref, pd_ref))):
            @pl.when((grad == which) & (side == core))
            def _():
                for copy in operand_copies(*mine, slot, q % 2):
                    copy.start()

            @pl.when((grad == which) & (side != core))
            def _():
                for copy in operand_copies(*theirs, slot, q % 2):
                    copy.start()

    def out_copy(dst, part):
        return pltpu.make_async_copy(acc.at[part], dst.at[0, half_of(part // 2), half_of(part % 2)], o_sem.at[part])

    def strip_copies(t, src, dst):
        layer, row = (t % per_array) // per_layer, pl.multiple_of((t % per_layer) * strip, strip)
        return (pltpu.make_async_copy(src.at[layer, pl.ds(row, strip)], ring.at[t % depth], in_sem.at[t % depth]),
                pltpu.make_async_copy(ring.at[t % depth], dst.at[layer + 1, pl.ds(row, strip)], out_sem.at[t % depth]))

    def move(t):
        @pl.when((t >= depth) & (t < strips + depth))
        def _():
            strip_copies(t - depth, td_ref, gd_out)[1].wait()

        @pl.when(t < per_array)
        def _():
            strip_copies(t, td_ref, gd_out)[0].start()

        @pl.when((t >= per_array) & (t < strips))
        def _():
            strip_copies(t, tu_ref, gu_out)[0].start()

        late = t - lag

        @pl.when((late >= 0) & (late < per_array))
        def _():
            strip_copies(late, td_ref, gd_out)[0].wait()
            strip_copies(late, td_ref, gd_out)[1].start()

        @pl.when((late >= per_array) & (late < strips))
        def _():
            strip_copies(late, tu_ref, gu_out)[0].wait()
            strip_copies(late, tu_ref, gu_out)[1].start()

    def compute(p):
        q, part = p // parts, p % parts
        stage = q % 2

        @pl.when((part == 0) & (q + 1 < granules))
        def _():
            load(q + 1)

        @pl.when(part == 0)
        def _():
            for copy in operand_copies(a_ref, g_ref, 0, stage):
                copy.wait()

        @pl.when(q == per_grad)
        def _():
            out_copy(gd_out, part).wait()

        @pl.when(q % per_grad == 0)
        def _():
            acc[part] = dot_f32(lhs[stage, part // 2], rhs[stage, part % 2], ROW_CONTRACT)

        @pl.when(q % per_grad > 0)
        def _():
            acc[part] += dot_f32(lhs[stage, part // 2], rhs[stage, part % 2], ROW_CONTRACT)

        @pl.when(q == per_grad - 1)
        def _():
            out_copy(gd_out, part).start()

        @pl.when(q == granules - 1)
        def _():
            out_copy(gu_out, part).start()

    load(0)

    def body(p, carry):
        move(p)
        compute(p)
        return carry

    lax.fori_loop(0, parts * granules, body, 0)

    def flush(t, carry):
        move(t)
        return carry

    lax.fori_loop(parts * granules, max(strips + depth, parts * granules), flush, 0)
    for part in range(parts):
        out_copy(gu_out, part).wait()


def run_final(operands, t_down, t_up):
    layers, width, d_model = t_down.shape[0] + 1, t_down.shape[1], t_down.shape[2]
    tokens = operands[1].shape[0]
    rows, side_w = tokens // SLOTS, width // 2
    bf16, f32 = jnp.bfloat16, jnp.float32
    anywhere = pl.BlockSpec(memory_space=pl.ANY)
    return pl.pallas_call(
        final_kernel,
        out_shape=(jax.ShapeDtypeStruct((layers, width, d_model), f32), jax.ShapeDtypeStruct((layers, d_model, width), f32)),
        in_specs=[anywhere] * 10,
        out_specs=(anywhere,) * 2,
        scratch_shapes=[
            pltpu.VMEM((4, side_w, side_w), f32),
            pltpu.VMEM((2, 2, rows, side_w), bf16),
            pltpu.VMEM((2, 2, rows, side_w), bf16),
            pltpu.VMEM((8, 256, d_model), f32),
            pltpu.SemaphoreType.DMA((2, 2)),
            pltpu.SemaphoreType.DMA((2, 2)),
            pltpu.SemaphoreType.DMA((4,)),
            pltpu.SemaphoreType.DMA((8,)),
            pltpu.SemaphoreType.DMA((8,)),
        ],
        compiler_params=pltpu.CompilerParams(vmem_limit_bytes=67043328),
        cost_estimate=pl.CostEstimate(flops=8 * tokens * d_model * width, bytes_accessed=16 * layers * d_model * width, transcendentals=0),
        name="final_grads",
    )(*operands, t_down, t_up)


def local_step(hidden, targets, w_up, w_down, total_tokens):
    _, _, act_all, g_all, d_all, t_down, t_up, _, _, pg, ph, pa0, pd0 = run_chain(hidden, targets, w_up, w_down, total_tokens)
    grad_down, grad_up = run_final((act_all, pa0, g_all, pg, hidden, ph, d_all, pd0), t_down, t_up)
    return grad_up, grad_down


def solution(mesh):
    def grad_step(hidden_in, targets, w_up, w_down):
        step_fn = functools.partial(local_step, total_tokens=hidden_in.shape[0])
        mapped = jax.shard_map(step_fn, mesh=mesh, in_specs=(P("dp", None), P("dp", None), P(None, None, "tp"), P(None, "tp", None)), out_specs=(P(None, None, "tp"), P(None, "tp", None)), check_vma=False)
        return mapped(hidden_in, targets, w_up, w_down)

    return grad_step
```

```python
import functools
import jax
import jax.numpy as jnp
from jax import lax
from jax.experimental import pallas as pl
from jax.experimental.pallas import tpu as pltpu
from jax.sharding import PartitionSpec as P

ROW_CONTRACT = (((0,), (0,)), ((), ()))
COL_CONTRACT = (((1,), (1,)), ((), ()))
MESH = pl.DeviceIdType.MESH
SLOTS = 4
TILE = 512
RED1_X, RED1_Y, RED2_X, RED2_Y, GAT1_X, GAT1_Y, GAT2_X, GAT2_Y = range(8)


def gelu_tanh(value):
    return jax.nn.gelu(value, approximate=True)


def dot_f32(lhs, rhs, dims=(((1,), (0,)), ((), ()))):
    return lax.dot_general(lhs, rhs, dims, preferred_element_type=jnp.float32)


PUSH_A, PUSH_D, PUSH_G, PUSH_H = range(4)


def chain_kernel(layers, total_tokens, x_ref, t_ref, wu_ref, wd_ref,
                 h_out, u_out, a_out, g_out, du_out, td_out, tu_out, pa_out, pd_out, pg_out, ph_out, pa0_out, pd0_out,
                 hbuf, abuf, ubuf, wbuf, pbuf, red1, red2, acc, ops,
                 send_sem, recv_sem, push_send, push_recv, res_send, res_recv, w_sem, u_sem, a_sem, h_sem, t_sem, l_sem, o_sem):
    rows, d_model = hbuf.shape[1:]
    block = rows // 4
    half = block // 2
    tiles = d_model // TILE
    side_w = d_model // 2
    turn = layers * SLOTS
    steps = turn + (layers - 1) * SLOTS
    every = steps + SLOTS
    top = layers - 1
    granules = 2 * (layers - 1) * 2 * SLOTS
    me = lax.axis_index("tp")
    core = lax.axis_index("dp")
    peer = 1 - core
    mx, my = me % 2, me // 2
    x_nbr = my * 2 + (1 - mx)
    y_nbr = (1 - my) * 2 + mx
    diag = (1 - my) * 2 + (1 - mx)

    def rows_of(owner, part=None):
        if part is None:
            return pl.ds(pl.multiple_of(owner * block, block), block)
        return pl.ds(pl.multiple_of(owner * block + part * half, half), half)

    def chunk_rows(slot):
        return pl.ds(pl.multiple_of(slot * rows, rows), rows)

    def half_of(which):
        return pl.ds(pl.multiple_of(which * side_w, side_w), side_w)

    def tile_of(tile):
        return pl.ds(pl.multiple_of(tile * TILE, TILE), TILE)

    def layer_of(n):
        back = n // turn
        return (1 - back) * (n // SLOTS) + back * (2 * layers - 1 - n // SLOTS)

    def remote(kind, k, src, dst, target):
        return pltpu.make_async_remote_copy(src_ref=src, dst_ref=dst, send_sem=send_sem.at[kind, k % SLOTS], recv_sem=recv_sem.at[kind, k % SLOTS], device_id={"tp": target}, device_id_type=MESH)

    def red1_copies(k):
        return (remote(RED1_X, k, pbuf.at[k % 2, rows_of(diag, 0)], red1.at[k % 2, 0], x_nbr),
                remote(RED1_Y, k, pbuf.at[k % 2, rows_of(diag, 1)], red1.at[k % 2, 1], y_nbr))

    def red1_tiles(tile):
        for kind, part, target in ((RED1_X, 0, x_nbr), (RED1_Y, 1, y_nbr)):
            remote(kind, 0, pbuf.at[0, rows_of(diag, part), tile_of(tile)], red1.at[0, part, :, tile_of(tile)], target).start()

    def red2_copies(k):
        return (remote(RED2_X, k, pbuf.at[k % 2, rows_of(x_nbr)], red2.at[k % 2, 0], x_nbr),
                remote(RED2_Y, k, pbuf.at[k % 2, rows_of(y_nbr)], red2.at[k % 2, 1], y_nbr))

    def gat1_copies(k):
        mine = hbuf.at[k % SLOTS, rows_of(me)]
        return (remote(GAT1_X, k, mine, mine, x_nbr), remote(GAT1_Y, k, mine, mine, y_nbr))

    def gat2_copies(k):
        from_y = hbuf.at[k % SLOTS, rows_of(y_nbr, 0)]
        from_x = hbuf.at[k % SLOTS, rows_of(x_nbr, 1)]
        return (remote(GAT2_X, k, from_y, from_y, x_nbr), remote(GAT2_Y, k, from_x, from_x, y_nbr))

    def push(kind, layer, slot, src, dst):
        return pltpu.make_async_remote_copy(src_ref=src, dst_ref=dst, send_sem=push_send.at[kind, layer, slot], recv_sem=push_recv.at[kind, layer, slot], device_id={"dp": peer}, device_id_type=MESH)

    def push_a(layer, slot):
        return push(PUSH_A, layer, slot, a_out.at[layer, chunk_rows(slot), half_of(peer)], pa_out.at[layer, chunk_rows(slot)])

    def push_d(layer, slot):
        return push(PUSH_D, layer, slot, du_out.at[layer, chunk_rows(slot), half_of(peer)], pd_out.at[layer, chunk_rows(slot)])

    def push_a0(slot):
        return push(PUSH_A, 0, slot, a_out.at[0, chunk_rows(slot)], pa0_out.at[chunk_rows(slot)])

    def d0_tiles(slot, tile):
        part = abuf.at[:, tile_of(tile)]
        push(PUSH_D, 0, slot, part, pd0_out.at[chunk_rows(slot), tile_of(tile)]).start()
        pltpu.make_async_copy(part, du_out.at[0, chunk_rows(slot), tile_of(tile)], a_sem).start()

    def push_d0(slot):
        return push(PUSH_D, 0, slot, abuf, pd0_out.at[chunk_rows(slot)])

    def push_g(layer, slot):
        return push(PUSH_G, layer, slot, g_out.at[layer, chunk_rows(slot)], pg_out.at[layer, chunk_rows(slot)])

    def push_h(layer, slot):
        return push(PUSH_H, layer, slot, h_out.at[layer - 1, chunk_rows(slot)], ph_out.at[layer, chunk_rows(slot)])

    def push_h0(slot):
        return push(PUSH_H, 0, slot, x_ref.at[chunk_rows(slot)], ph_out.at[0, chunk_rows(slot)])

    def weight_copy(ref, layer, tile, stage):
        return pltpu.make_async_copy(ref.at[layer, tile_of(tile)], wbuf.at[stage], w_sem.at[stage])

    def column_copies(ref, layer, tile, stage):
        for i in range(tiles):
            block_rows = pl.ds(i * TILE, TILE)
            pltpu.make_async_copy(ref.at[layer, block_rows, tile_of(tile)], wbuf.at[stage, :, block_rows], w_sem.at[stage]).start()

    def weight_start(index):
        main = steps * 2 * tiles
        n, place = index // (2 * tiles), index % (2 * tiles)
        up = 1 - place // tiles
        use_up = (1 - n // turn) * up + (n // turn) * (1 - up)

        @pl.when((n < turn) & (use_up == 1))
        def _():
            column_copies(wu_ref, layer_of(n), place % tiles, index % 3)

        @pl.when((n < turn) & (use_up == 0))
        def _():
            column_copies(wd_ref, layer_of(n), place % tiles, index % 3)

        @pl.when((n >= turn) & (index < main) & (use_up == 1))
        def _():
            weight_copy(wu_ref, layer_of(n), place % tiles, index % 3).start()

        @pl.when((n >= turn) & (index < main) & (use_up == 0))
        def _():
            weight_copy(wd_ref, layer_of(n), place % tiles, index % 3).start()

        @pl.when((index >= main) & (index < main + SLOTS * tiles))
        def _():
            weight_copy(wd_ref, 0, (index - main) % tiles, index % 3).start()

    def weight_wait(index):
        weight_copy(wu_ref, 0, 0, index % 3).wait()

    def weight_base(n):
        late = (n // steps) * (n - steps)
        return (n - late) * 2 * tiles + late * tiles

    def u_save(n, tile, stage):
        return pltpu.make_async_copy(ubuf.at[stage], u_out.at[layer_of(n), chunk_rows(n % SLOTS), tile_of(tile)], u_sem.at[stage])

    def u_load(n, tile, stage):
        return pltpu.make_async_copy(u_out.at[layer_of(n), chunk_rows(n % SLOTS), tile_of(tile)], ubuf.at[stage], u_sem.at[stage])

    def x_load(slot):
        return pltpu.make_async_copy(x_ref.at[chunk_rows(slot)], hbuf.at[slot], h_sem.at[slot])

    def h_save(layer, slot):
        return pltpu.make_async_copy(hbuf.at[slot], h_out.at[layer - 1, chunk_rows(slot)], h_sem.at[slot])

    def g_save(layer, slot):
        return pltpu.make_async_copy(hbuf.at[slot], g_out.at[layer, chunk_rows(slot)], h_sem.at[slot])

    def a_save(layer, slot):
        return pltpu.make_async_copy(abuf, a_out.at[layer, chunk_rows(slot)], a_sem)

    def d_save(layer, slot):
        return pltpu.make_async_copy(abuf, du_out.at[layer, chunk_rows(slot)], a_sem)

    def t_loads(slot):
        own = pl.ds(pl.multiple_of(slot * rows + me * block, block), block)
        return [pltpu.make_async_copy(t_ref.at[own, pl.ds(part * side_w, side_w)], ops.at[0, 1 + part, pl.ds(0, block)], t_sem.at[part]) for part in range(2)]

    def half_load(src, side):
        return pltpu.make_async_copy(src, ops.at[side, 0], l_sem.at[side, 0])

    def full_load(src, side, part):
        return pltpu.make_async_copy(src.at[:, pl.ds(part * side_w, side_w)], ops.at[side, 1 + part], l_sem.at[side, 1 + part])

    def out_copy(dst, part):
        return pltpu.make_async_copy(acc.at[part], dst, o_sem.at[part])

    def out_push(dst, index, part):
        return pltpu.make_async_remote_copy(src_ref=dst, dst_ref=dst, send_sem=res_send.at[index, part], recv_sem=res_recv.at[index, part], device_id={"dp": peer}, device_id_type=MESH)

    def td_part(layer, part):
        return td_out.at[layer - 1, half_of(core), pl.ds(part * side_w, side_w)]

    def tu_part(layer, part):
        return tu_out.at[layer - 1, pl.ds(part * side_w, side_w), half_of(core)]

    def load_granule(q):
        index = q // (2 * SLOTS)
        kind, layer, slot, side = index % 2, top - index // 2, (q % (2 * SLOTS)) // 2, q % 2

        def start(half_src, full_src):
            half_load(half_src, side).start()
            for part in range(2):
                full_load(full_src, side, part).start()

        @pl.when((kind == 0) & (side == 0))
        def _():
            start(a_out.at[layer, chunk_rows(slot), half_of(core)], g_out.at[layer, chunk_rows(slot)])

        @pl.when((kind == 0) & (side == 1))
        def _():
            push_a(layer, slot).wait_recv()
            push_g(layer, slot).wait_recv()
            start(pa_out.at[layer, chunk_rows(slot)], pg_out.at[layer, chunk_rows(slot)])

        @pl.when((kind == 1) & (side == 0))
        def _():
            start(du_out.at[layer, chunk_rows(slot), half_of(core)], h_out.at[layer - 1, chunk_rows(slot)])

        @pl.when((kind == 1) & (side == 1))
        def _():
            push_d(layer, slot).wait_recv()
            push_h(layer, slot).wait_recv()
            start(pd_out.at[layer, chunk_rows(slot)], ph_out.at[layer, chunk_rows(slot)])

    def last_push(part):
        index = 2 * (layers - 1) - 1
        return pltpu.make_async_remote_copy(src_ref=acc.at[part], dst_ref=tu_part(1, part), send_sem=res_send.at[index, part], recv_sem=res_recv.at[index, part], device_id={"dp": peer}, device_id_type=MESH)

    def hand_over(index):
        kind, layer = index % 2, top - index // 2
        for part in range(2):
            out_copy(td_part(1, part), part).wait()

        @pl.when(kind == 0)
        def _():
            for part in range(2):
                out_push(td_part(layer, part), index, part).start()

        @pl.when(kind == 1)
        def _():
            for part in range(2):
                out_push(tu_part(layer, part), index, part).start()

    def run_granule(q):
        index = q // (2 * SLOTS)
        kind, layer, side = index % 2, top - index // 2, q % 2

        @pl.when((q % (2 * SLOTS) == 0) & (q > 0))
        def _():
            hand_over(index - 1)

        @pl.when(q % (2 * SLOTS) == 0)
        def _():
            def clear(i, carry):
                strip = pl.ds(pl.multiple_of(i * 64, 64), 64)
                acc[:, strip, :] = jnp.zeros((2, 64, side_w), jnp.float32)
                return carry

            lax.fori_loop(0, side_w // 64, clear, 0)

        half_load(pa_out.at[0, chunk_rows(0)], side).wait()
        for part in range(2):
            full_load(pg_out.at[0, chunk_rows(0)], side, part).wait()

        def part_step(i, carry):
            part, strip = i // 2, pl.ds(pl.multiple_of(i % 2 * (side_w // 2), side_w // 2), side_w // 2)
            acc[part, strip] += dot_f32(ops[side, kind * (1 + part), :, strip], ops[side, (1 - kind) * (1 + part)], ROW_CONTRACT)
            return carry

        lax.fori_loop(0, 4, part_step, 0)

        @pl.when((q % (2 * SLOTS) == 2 * SLOTS - 1) & (kind == 0))
        def _():
            for part in range(2):
                out_copy(td_part(layer, part), part).start()

        @pl.when((q % (2 * SLOTS) == 2 * SLOTS - 1) & (kind == 1))
        def _():
            for part in range(2):
                out_copy(tu_part(layer, part), part).start()

        @pl.when(q == granules - 1)
        def _():
            for part in range(2):
                last_push(part).start()

    plan = {1: (2, 2, 0), 2: (1, 0, 0), 3: (2, 1, 1), 4: (2, 1, 0), 5: (2, 2, 0), 6: (2, 2, 0), 7: (2, 2, 0), 8: (2, 2, 0), 9: (2, 2, 0), 10: (2, 4, 0), 11: (2, 4, 2)}
    ran = sum(sum(groups) for groups in plan.values())

    def plan_of(n):
        ends = [0, 0, 0, 0]
        for b, groups in plan.items():
            reached, passed = (n - b) // turn, (n - b - 1) // turn
            here = (n // turn) * (reached - passed)
            ends[0] = ends[0] + sum(groups) * passed
            for i, number in enumerate(groups):
                ends[i + 1] = ends[i + 1] + number * here
        for i in range(3):
            ends[i + 1] = ends[i + 1] + ends[i]
        return ends

    def run_granules(begin, end, stop):
        def step(q, carry):
            @pl.when(q + 1 < stop)
            def _():
                load_granule(q + 1)

            run_granule(q)
            return carry

        lax.fori_loop(begin, end, step, 0)

    def receive_rows(n):
        layer, slot = layer_of(n), n % SLOTS

        @pl.when(n < SLOTS)
        def _():
            push_h0(slot).start()
            x_load(slot).wait()

        @pl.when(n >= SLOTS)
        def _():
            for copy in gat2_copies(n):
                copy.wait()
            for copy in gat1_copies(n):
                copy.wait_send()

        @pl.when((n >= SLOTS) & (n < turn))
        def _():
            h_save(layer, slot).start()

        @pl.when(n >= turn)
        def _():
            g_save(layer, slot).start()

    def settle_rows(n):
        layer, slot = layer_of(n), n % SLOTS

        @pl.when((n >= SLOTS) & (n < turn))
        def _():
            h_save(layer, slot).wait()
            push_h(layer, slot).start()

        @pl.when(n >= turn)
        def _():
            g_save(layer, slot).wait()
            push_g(layer, slot).start()

    def share_acts(n):
        layer, slot = layer_of(n), n % SLOTS

        @pl.when(n < turn)
        def _():
            a_save(layer, slot).start()

        @pl.when((n >= turn) & (n < steps))
        def _():
            d_save(layer, slot).start()

    def settle_acts(n):
        layer, slot = layer_of(n), n % SLOTS
        a_save(layer, slot).wait()

        @pl.when(n < SLOTS)
        def _():
            push_a0(slot).start()

        @pl.when((n >= SLOTS) & (n < turn))
        def _():
            push_a(layer, slot).start()

        @pl.when((n >= turn) & (n < steps))
        def _():
            push_d(layer, slot).start()

        @pl.when(n >= steps)
        def _():
            push_d0(slot).wait_send()

    def times_columns(source, stage):
        total = None
        for i in range(tiles):
            cols = pl.ds(i * TILE, TILE)
            part = dot_f32(source(cols), wbuf[stage, :, cols])
            total = part if total is None else total + part
        return total

    def forward_up(n):
        slot = n % SLOTS

        def tile_step(tile, carry):
            index = weight_base(n) + tile
            count = n * tiles + tile
            weight_start(index + 2)
            weight_wait(index)
            pre = times_columns(lambda cols: hbuf[slot, :, cols], index % 3).astype(jnp.bfloat16)

            @pl.when(count >= 2)
            def _():
                u_save(0, 0, count % 2).wait()

            ubuf[count % 2] = pre
            abuf[:, tile_of(tile)] = gelu_tanh(pre.astype(jnp.float32)).astype(jnp.bfloat16)
            u_save(n, tile, count % 2).start()
            return carry

        lax.fori_loop(0, tiles, tile_step, 0)

    def forward_down(n):
        def tile_step(tile, carry):
            index = weight_base(n) + tiles + tile
            weight_start(index + 2)
            weight_wait(index)
            pbuf[n % 2, :, tile_of(tile)] = times_columns(lambda cols: abuf[:, cols], index % 3)

            @pl.when(n == 0)
            def _():
                red1_tiles(tile)

            return carry

        lax.fori_loop(0, tiles, tile_step, 0)

    def backward_up(n):
        slot = n % SLOTS

        @pl.when(n == turn)
        def _():
            for stage in range(2):
                u_save(0, 0, stage).wait()
            u_load(n, 0, n * tiles % 2).start()

        def tile_step(tile, carry):
            index = weight_base(n) + tile
            count = n * tiles + tile
            weight_start(index + 2)

            @pl.when(count + 1 < every * tiles)
            def _():
                u_load((count + 1) // tiles, (count + 1) % tiles, (count + 1) % 2).start()

            weight_wait(index)
            u_load(n, tile, count % 2).wait()
            d_act = dot_f32(hbuf[slot], wbuf[index % 3], COL_CONTRACT)
            _, gelu_vjp = jax.vjp(gelu_tanh, ubuf[count % 2].astype(jnp.float32))
            abuf[:, tile_of(tile)] = gelu_vjp(d_act)[0].astype(jnp.bfloat16)

            @pl.when(n >= steps)
            def _():
                d0_tiles(slot, tile)

            return carry

        lax.fori_loop(0, tiles, tile_step, 0)

    def backward_down(n):
        def tile_step(tile, carry):
            index = weight_base(n) + tiles + tile
            weight_start(index + 2)
            weight_wait(index)
            pbuf[n % 2, :, tile_of(tile)] = dot_f32(abuf[...], wbuf[index % 3], COL_CONTRACT)
            return carry

        lax.fori_loop(0, tiles, tile_step, 0)

    def send_diagonal(n):
        @pl.when(n > 0)
        def _():
            for copy in red1_copies(n):
                copy.start()

    def reduce_step(k):
        first, second = red1_copies(k)
        first.wait_recv()
        pbuf[k % 2, rows_of(y_nbr, 0)] += red1[k % 2, 0]
        second.wait_recv()
        pbuf[k % 2, rows_of(x_nbr, 1)] += red1[k % 2, 1]
        for copy in red2_copies(k):
            copy.start()

        @pl.when((k >= turn - SLOTS) & (k < turn))
        def _():
            for copy in t_loads(k % SLOTS):
                copy.start()

    def finish_step(k):
        slot = k % SLOTS
        for copy in red2_copies(k):
            copy.wait()
        for copy in red1_copies(k):
            copy.wait_send()

        def total():
            return pbuf[k % 2, rows_of(me)] + red2[k % 2, 0] + red2[k % 2, 1]

        def h_new():
            return (hbuf[slot, rows_of(me)].astype(jnp.float32) + total().astype(jnp.bfloat16).astype(jnp.float32)).astype(jnp.bfloat16)

        @pl.when(k < turn - SLOTS)
        def _():
            hbuf[slot, rows_of(me)] = h_new()

        @pl.when((k >= turn - SLOTS) & (k < turn))
        def _():
            for copy in t_loads(slot):
                copy.wait()
            target = jnp.concatenate([ops[0, 1, :block], ops[0, 2, :block]], 1)
            err = (h_new().astype(jnp.float32) - target.astype(jnp.float32)) * (1.0 / total_tokens)
            hbuf[slot, rows_of(me)] = err.astype(jnp.bfloat16)

        @pl.when(k >= turn)
        def _():
            hbuf[slot, rows_of(me)] = (hbuf[slot, rows_of(me)].astype(jnp.float32) + total()).astype(jnp.bfloat16)

        for copy in gat1_copies(k):
            copy.start()

    def forward_rows(k):
        for copy in gat1_copies(k):
            copy.wait_recv()
        for copy in gat2_copies(k):
            copy.start()

    def when_step(k, fn):
        @pl.when((k >= 0) & (k < steps))
        def _():
            fn(k)

    barrier = pltpu.get_barrier_semaphore()
    for target in ({"tp": x_nbr}, {"tp": y_nbr}, {"dp": peer}):
        pl.semaphore_signal(barrier, inc=1, device_id=target, device_id_type=MESH)
    x_load(0).start()
    weight_start(0)
    weight_start(1)
    for slot in range(1, SLOTS):
        x_load(slot).start()
    pl.semaphore_wait(barrier, 3)

    def body(n, carry):
        begin, one, two, stop = plan_of(n)
        receive_rows(n)

        @pl.when(n >= 1)
        def _():
            settle_acts(n - 1)

        @pl.when(n < turn)
        def _():
            forward_up(n)

        @pl.when(n >= turn)
        def _():
            backward_up(n)

        when_step(n - 2, forward_rows)
        share_acts(n)
        settle_rows(n)

        @pl.when(begin < stop)
        def _():
            load_granule(begin)

        @pl.when(n < turn)
        def _():
            forward_down(n)

        @pl.when(n >= turn)
        def _():
            backward_down(n)

        send_diagonal(n)
        run_granules(begin, one, stop)
        when_step(n - 1, finish_step)
        run_granules(one, two, stop)
        reduce_step(n)
        run_granules(two, stop, stop)
        return carry

    lax.fori_loop(0, steps, body, 0)
    forward_rows(steps - 2)

    def last_body(n, carry):
        receive_rows(n)
        settle_acts(n - 1)

        @pl.when(n == steps)
        def _():
            load_granule(ran)

        backward_up(n)

        @pl.when(n == steps)
        def _():
            run_granules(ran, ran + 1, granules)
            finish_step(steps - 1)
            run_granules(ran + 1, granules, granules)

        @pl.when(n == steps + 1)
        def _():
            forward_rows(steps - 1)

        settle_rows(n)
        return carry

    lax.fori_loop(steps, every, last_body, 0)
    settle_acts(every - 1)
    for part in range(2):
        out_copy(tu_part(1, part), part).wait()

    def drain(i, carry):
        layer, slot = i // SLOTS, i % SLOTS
        push_g(layer, slot).wait_send()
        push(PUSH_H, layer, slot, x_ref.at[chunk_rows(slot)], ph_out.at[layer, chunk_rows(slot)]).wait_send()

        @pl.when(layer > 0)
        def _():
            push_a(layer, slot).wait_send()
            push_d(layer, slot).wait_send()

        return carry

    lax.fori_loop(0, layers * SLOTS, drain, 0)
    for slot in range(SLOTS):
        push_a0(slot).wait()
        push_d0(slot).wait_recv()
        push_g(0, slot).wait_recv()
        push_h0(slot).wait_recv()
    for index in range(2 * (layers - 1)):
        for part in range(2):
            out_push(td_part(1, part), index, part).wait()


def run_chain(hidden, targets, w_up, w_down, total_tokens):
    layers, d_model, width = w_up.shape
    tokens = hidden.shape[0]
    rows = tokens // SLOTS
    block = rows // 4
    half = width // 2
    bf16, f32 = jnp.bfloat16, jnp.float32
    flops = 2 * tokens * d_model * width * (6 * layers - 3)
    anywhere = pl.BlockSpec(memory_space=pl.ANY)
    like = jax.ShapeDtypeStruct
    outs = (like((layers - 1, tokens, d_model), bf16), like((layers, tokens, width), bf16), like((layers, tokens, width), bf16),
            like((layers, tokens, d_model), bf16), like((layers, tokens, width), bf16),
            like((layers - 1, width, d_model), f32), like((layers - 1, d_model, width), f32),
            like((layers, tokens, half), bf16), like((layers, tokens, half), bf16),
            like((layers, tokens, d_model), bf16), like((layers, tokens, d_model), bf16),
            like((tokens, width), bf16), like((tokens, width), bf16))
    return pl.pallas_call(
        functools.partial(chain_kernel, layers, total_tokens),
        out_shape=outs,
        in_specs=[anywhere] * 4,
        out_specs=(anywhere,) * len(outs),
        scratch_shapes=[
            pltpu.VMEM((SLOTS, rows, d_model), bf16),
            pltpu.VMEM((rows, width), bf16),
            pltpu.VMEM((2, rows, TILE), bf16),
            pltpu.VMEM((3, TILE, d_model), bf16),
            pltpu.VMEM((2, rows, d_model), f32),
            pltpu.VMEM((2, 2, block // 2, d_model), f32),
            pltpu.VMEM((2, 2, block, d_model), f32),
            pltpu.VMEM((2, half, half), f32),
            pltpu.VMEM((2, 3, rows, half), bf16),
            pltpu.SemaphoreType.DMA((8, SLOTS)),
            pltpu.SemaphoreType.DMA((8, SLOTS)),
            pltpu.SemaphoreType.DMA((4, layers, SLOTS)),
            pltpu.SemaphoreType.DMA((4, layers, SLOTS)),
            pltpu.SemaphoreType.DMA((2 * (layers - 1), 2)),
            pltpu.SemaphoreType.DMA((2 * (layers - 1), 2)),
            pltpu.SemaphoreType.DMA((3,)),
            pltpu.SemaphoreType.DMA((2,)),
            pltpu.SemaphoreType.DMA,
            pltpu.SemaphoreType.DMA((SLOTS,)),
            pltpu.SemaphoreType.DMA((2,)),
            pltpu.SemaphoreType.DMA((2, 3)),
            pltpu.SemaphoreType.DMA((2,)),
        ],
        compiler_params=pltpu.CompilerParams(collective_id=0, has_side_effects=True, vmem_limit_bytes=67043328),
        cost_estimate=pl.CostEstimate(flops=flops, bytes_accessed=layers * tokens * d_model * 16, transcendentals=2 * layers * tokens * width),
        name="step_chain",
    )(hidden, targets, w_up, w_down)


def final_kernel(a_ref, pa_ref, g_ref, pg_ref, x_ref, px_ref, d_ref, pd_ref, td_ref, tu_ref, gd_out, gu_out, acc, lhs, rhs, ring, l_sem, r_sem, o_sem, in_sem, out_sem):
    rows, side_w = lhs.shape[2:]
    strip = ring.shape[1]
    depth = ring.shape[0]
    done_layers, height, _ = td_ref.shape
    per_layer = height // strip
    per_array = done_layers * per_layer
    strips = 2 * per_array
    lag = depth // 2
    core = lax.axis_index("dp")
    a_ref, g_ref, pg_ref, px_ref, d_ref = (ref.at[0] for ref in (a_ref, g_ref, pg_ref, px_ref, d_ref))
    parts = 4
    granules = 4 * SLOTS
    per_grad = granules // 2

    def chunk_rows(slot):
        return pl.ds(pl.multiple_of(slot * rows, rows), rows)

    def half_of(which):
        return pl.ds(pl.multiple_of(which * side_w, side_w), side_w)

    def operand_copies(left, right, slot, stage):
        for part in range(2):
            cols = pl.ds(part * side_w, side_w)
            yield pltpu.make_async_copy(left.at[chunk_rows(slot), cols], lhs.at[stage, part], l_sem.at[stage, part])
            yield pltpu.make_async_copy(right.at[chunk_rows(slot), cols], rhs.at[stage, part], r_sem.at[stage, part])

    def load(q):
        grad, slot, side = q // per_grad, (q % per_grad) // 2, q % 2
        for which, mine, theirs in ((0, (a_ref, g_ref), (pa_ref, pg_ref)), (1, (x_ref, d_ref), (px_ref, pd_ref))):
            @pl.when((grad == which) & (side == core))
            def _():
                for copy in operand_copies(*mine, slot, q % 2):
                    copy.start()

            @pl.when((grad == which) & (side != core))
            def _():
                for copy in operand_copies(*theirs, slot, q % 2):
                    copy.start()

    def out_copy(dst, part):
        return pltpu.make_async_copy(acc.at[part], dst.at[0, half_of(part // 2), half_of(part % 2)], o_sem.at[part])

    def strip_copies(t, src, dst):
        layer, row = (t % per_array) // per_layer, pl.multiple_of((t % per_layer) * strip, strip)
        return (pltpu.make_async_copy(src.at[layer, pl.ds(row, strip)], ring.at[t % depth], in_sem.at[t % depth]),
                pltpu.make_async_copy(ring.at[t % depth], dst.at[layer + 1, pl.ds(row, strip)], out_sem.at[t % depth]))

    def move(t):
        @pl.when((t >= depth) & (t < strips + depth))
        def _():
            strip_copies(t - depth, td_ref, gd_out)[1].wait()

        @pl.when(t < per_array)
        def _():
            strip_copies(t, td_ref, gd_out)[0].start()

        @pl.when((t >= per_array) & (t < strips))
        def _():
            strip_copies(t, tu_ref, gu_out)[0].start()

        late = t - lag

        @pl.when((late >= 0) & (late < per_array))
        def _():
            strip_copies(late, td_ref, gd_out)[0].wait()
            strip_copies(late, td_ref, gd_out)[1].start()

        @pl.when((late >= per_array) & (late < strips))
        def _():
            strip_copies(late, tu_ref, gu_out)[0].wait()
            strip_copies(late, tu_ref, gu_out)[1].start()

    def compute(p):
        q, part = p // parts, p % parts
        stage = q % 2

        @pl.when((part == 0) & (q + 1 < granules))
        def _():
            load(q + 1)

        @pl.when(part == 0)
        def _():
            for copy in operand_copies(a_ref, g_ref, 0, stage):
                copy.wait()

        @pl.when(q == per_grad)
        def _():
            out_copy(gd_out, part).wait()

        @pl.when(q % per_grad == 0)
        def _():
            acc[part] = dot_f32(lhs[stage, part // 2], rhs[stage, part % 2], ROW_CONTRACT)

        @pl.when(q % per_grad > 0)
        def _():
            acc[part] += dot_f32(lhs[stage, part // 2], rhs[stage, part % 2], ROW_CONTRACT)

        @pl.when(q == per_grad - 1)
        def _():
            out_copy(gd_out, part).start()

        @pl.when(q == granules - 1)
        def _():
            out_copy(gu_out, part).start()

    load(0)

    def body(p, carry):
        move(p)
        compute(p)
        return carry

    lax.fori_loop(0, parts * granules, body, 0)

    def flush(t, carry):
        move(t)
        return carry

    lax.fori_loop(parts * granules, max(strips + depth, parts * granules), flush, 0)
    for part in range(parts):
        out_copy(gu_out, part).wait()


def run_final(operands, t_down, t_up):
    layers, width, d_model = t_down.shape[0] + 1, t_down.shape[1], t_down.shape[2]
    tokens = operands[1].shape[0]
    rows, side_w = tokens // SLOTS, width // 2
    bf16, f32 = jnp.bfloat16, jnp.float32
    anywhere = pl.BlockSpec(memory_space=pl.ANY)
    return pl.pallas_call(
        final_kernel,
        out_shape=(jax.ShapeDtypeStruct((layers, width, d_model), f32), jax.ShapeDtypeStruct((layers, d_model, width), f32)),
        in_specs=[anywhere] * 10,
        out_specs=(anywhere,) * 2,
        scratch_shapes=[
            pltpu.VMEM((4, side_w, side_w), f32),
            pltpu.VMEM((2, 2, rows, side_w), bf16),
            pltpu.VMEM((2, 2, rows, side_w), bf16),
            pltpu.VMEM((8, 256, d_model), f32),
            pltpu.SemaphoreType.DMA((2, 2)),
            pltpu.SemaphoreType.DMA((2, 2)),
            pltpu.SemaphoreType.DMA((4,)),
            pltpu.SemaphoreType.DMA((8,)),
            pltpu.SemaphoreType.DMA((8,)),
        ],
        compiler_params=pltpu.CompilerParams(vmem_limit_bytes=67043328),
        cost_estimate=pl.CostEstimate(flops=8 * tokens * d_model * width, bytes_accessed=16 * layers * d_model * width, transcendentals=0),
        name="final_grads",
    )(*operands, t_down, t_up)


def local_step(hidden, targets, w_up, w_down, total_tokens):
    _, _, act_all, g_all, d_all, t_down, t_up, _, _, pg, ph, pa0, pd0 = run_chain(hidden, targets, w_up, w_down, total_tokens)
    grad_down, grad_up = run_final((act_all, pa0, g_all, pg, hidden, ph, d_all, pd0), t_down, t_up)
    return grad_up, grad_down


def solution(mesh):
    def grad_step(hidden_in, targets, w_up, w_down):
        step_fn = functools.partial(local_step, total_tokens=hidden_in.shape[0])
        mapped = jax.shard_map(step_fn, mesh=mesh, in_specs=(P("dp", None), P("dp", None), P(None, None, "tp"), P(None, "tp", None)), out_specs=(P(None, None, "tp"), P(None, "tp", None)), check_vma=False)
        return mapped(hidden_in, targets, w_up, w_down)

    return grad_step
```

```python
import functools
import jax
import jax.numpy as jnp
from jax import lax
from jax.experimental import pallas as pl
from jax.experimental.pallas import tpu as pltpu
from jax.sharding import PartitionSpec as P

ROW_CONTRACT = (((0,), (0,)), ((), ()))
COL_CONTRACT = (((1,), (1,)), ((), ()))
MESH = pl.DeviceIdType.MESH
SLOTS = 4
TILE = 512
RED1_X, RED1_Y, RED2_X, RED2_Y, GAT1_X, GAT1_Y, GAT2_X, GAT2_Y = range(8)


def gelu_tanh(value):
    return jax.nn.gelu(value, approximate=True)


def dot_f32(lhs, rhs, dims=(((1,), (0,)), ((), ()))):
    return lax.dot_general(lhs, rhs, dims, preferred_element_type=jnp.float32)


PUSH_A, PUSH_D, PUSH_G, PUSH_H = range(4)


def chain_kernel(layers, total_tokens, x_ref, t_ref, wu_ref, wd_ref,
                 h_out, u_out, a_out, g_out, du_out, td_out, tu_out, pa_out, pd_out, pg_out, ph_out, pa0_out, pd0_out,
                 hbuf, abuf, ubuf, wbuf, pbuf, red1, red2, acc, ops,
                 send_sem, recv_sem, push_send, push_recv, res_send, res_recv, w_sem, u_sem, a_sem, h_sem, t_sem, l_sem, o_sem):
    rows, d_model = hbuf.shape[1:]
    block = rows // 4
    half = block // 2
    tiles = d_model // TILE
    side_w = d_model // 2
    turn = layers * SLOTS
    steps = turn + (layers - 1) * SLOTS
    every = steps + SLOTS
    top = layers - 1
    granules = 2 * (layers - 1) * 2 * SLOTS
    me = lax.axis_index("tp")
    core = lax.axis_index("dp")
    peer = 1 - core
    mx, my = me % 2, me // 2
    x_nbr = my * 2 + (1 - mx)
    y_nbr = (1 - my) * 2 + mx
    diag = (1 - my) * 2 + (1 - mx)

    def rows_of(owner, part=None):
        if part is None:
            return pl.ds(pl.multiple_of(owner * block, block), block)
        return pl.ds(pl.multiple_of(owner * block + part * half, half), half)

    def chunk_rows(slot):
        return pl.ds(pl.multiple_of(slot * rows, rows), rows)

    def half_of(which):
        return pl.ds(pl.multiple_of(which * side_w, side_w), side_w)

    def tile_of(tile):
        return pl.ds(pl.multiple_of(tile * TILE, TILE), TILE)

    def layer_of(n):
        back = n // turn
        return (1 - back) * (n // SLOTS) + back * (2 * layers - 1 - n // SLOTS)

    def remote(kind, k, src, dst, target):
        return pltpu.make_async_remote_copy(src_ref=src, dst_ref=dst, send_sem=send_sem.at[kind, k % SLOTS], recv_sem=recv_sem.at[kind, k % SLOTS], device_id={"tp": target}, device_id_type=MESH)

    def red1_copies(k):
        return (remote(RED1_X, k, pbuf.at[k % 2, rows_of(diag, 0)], red1.at[k % 2, 0], x_nbr),
                remote(RED1_Y, k, pbuf.at[k % 2, rows_of(diag, 1)], red1.at[k % 2, 1], y_nbr))

    def red1_tiles(tile):
        for kind, part, target in ((RED1_X, 0, x_nbr), (RED1_Y, 1, y_nbr)):
            remote(kind, 0, pbuf.at[0, rows_of(diag, part), tile_of(tile)], red1.at[0, part, :, tile_of(tile)], target).start()

    def red2_copies(k):
        return (remote(RED2_X, k, pbuf.at[k % 2, rows_of(x_nbr)], red2.at[k % 2, 0], x_nbr),
                remote(RED2_Y, k, pbuf.at[k % 2, rows_of(y_nbr)], red2.at[k % 2, 1], y_nbr))

    def gat1_copies(k):
        mine = hbuf.at[k % SLOTS, rows_of(me)]
        return (remote(GAT1_X, k, mine, mine, x_nbr), remote(GAT1_Y, k, mine, mine, y_nbr))

    def gat2_copies(k):
        from_y = hbuf.at[k % SLOTS, rows_of(y_nbr, 0)]
        from_x = hbuf.at[k % SLOTS, rows_of(x_nbr, 1)]
        return (remote(GAT2_X, k, from_y, from_y, x_nbr), remote(GAT2_Y, k, from_x, from_x, y_nbr))

    def push(kind, layer, slot, src, dst):
        return pltpu.make_async_remote_copy(src_ref=src, dst_ref=dst, send_sem=push_send.at[kind, layer, slot], recv_sem=push_recv.at[kind, layer, slot], device_id={"dp": peer}, device_id_type=MESH)

    def push_a(layer, slot):
        return push(PUSH_A, layer, slot, a_out.at[layer, chunk_rows(slot), half_of(peer)], pa_out.at[layer, chunk_rows(slot)])

    def push_d(layer, slot):
        return push(PUSH_D, layer, slot, du_out.at[layer, chunk_rows(slot), half_of(peer)], pd_out.at[layer, chunk_rows(slot)])

    def push_a0(slot):
        return push(PUSH_A, 0, slot, a_out.at[0, chunk_rows(slot)], pa0_out.at[chunk_rows(slot)])

    def d0_tiles(slot, tile):
        part = abuf.at[:, tile_of(tile)]
        push(PUSH_D, 0, slot, part, pd0_out.at[chunk_rows(slot), tile_of(tile)]).start()
        pltpu.make_async_copy(part, du_out.at[0, chunk_rows(slot), tile_of(tile)], a_sem).start()

    def push_d0(slot):
        return push(PUSH_D, 0, slot, abuf, pd0_out.at[chunk_rows(slot)])

    def push_g(layer, slot):
        return push(PUSH_G, layer, slot, g_out.at[layer, chunk_rows(slot)], pg_out.at[layer, chunk_rows(slot)])

    def push_h(layer, slot):
        return push(PUSH_H, layer, slot, h_out.at[layer - 1, chunk_rows(slot)], ph_out.at[layer, chunk_rows(slot)])

    def push_h0(slot):
        return push(PUSH_H, 0, slot, x_ref.at[chunk_rows(slot)], ph_out.at[0, chunk_rows(slot)])

    def weight_copy(ref, layer, tile, stage):
        return pltpu.make_async_copy(ref.at[layer, tile_of(tile)], wbuf.at[stage], w_sem.at[stage])

    def column_copies(ref, layer, tile, stage):
        for i in range(tiles):
            block_rows = pl.ds(i * TILE, TILE)
            pltpu.make_async_copy(ref.at[layer, block_rows, tile_of(tile)], wbuf.at[stage, :, block_rows], w_sem.at[stage]).start()

    def weight_start(index):
        main = steps * 2 * tiles
        n, place = index // (2 * tiles), index % (2 * tiles)
        up = 1 - place // tiles
        use_up = (1 - n // turn) * up + (n // turn) * (1 - up)

        @pl.when((n < turn) & (use_up == 1))
        def _():
            column_copies(wu_ref, layer_of(n), place % tiles, index % 3)

        @pl.when((n < turn) & (use_up == 0))
        def _():
            column_copies(wd_ref, layer_of(n), place % tiles, index % 3)

        @pl.when((n >= turn) & (index < main) & (use_up == 1))
        def _():
            weight_copy(wu_ref, layer_of(n), place % tiles, index % 3).start()

        @pl.when((n >= turn) & (index < main) & (use_up == 0))
        def _():
            weight_copy(wd_ref, layer_of(n), place % tiles, index % 3).start()

        @pl.when((index >= main) & (index < main + SLOTS * tiles))
        def _():
            weight_copy(wd_ref, 0, (index - main) % tiles, index % 3).start()

    def weight_wait(index):
        weight_copy(wu_ref, 0, 0, index % 3).wait()

    def weight_base(n):
        late = (n // steps) * (n - steps)
        return (n - late) * 2 * tiles + late * tiles

    def u_save(n, tile, stage):
        return pltpu.make_async_copy(ubuf.at[stage], u_out.at[layer_of(n), chunk_rows(n % SLOTS), tile_of(tile)], u_sem.at[stage])

    def u_load(n, tile, stage):
        return pltpu.make_async_copy(u_out.at[layer_of(n), chunk_rows(n % SLOTS), tile_of(tile)], ubuf.at[stage], u_sem.at[stage])

    def x_load(slot):
        return pltpu.make_async_copy(x_ref.at[chunk_rows(slot)], hbuf.at[slot], h_sem.at[slot])

    def h_save(layer, slot):
        return pltpu.make_async_copy(hbuf.at[slot], h_out.at[layer - 1, chunk_rows(slot)], h_sem.at[slot])

    def g_save(layer, slot):
        return pltpu.make_async_copy(hbuf.at[slot], g_out.at[layer, chunk_rows(slot)], h_sem.at[slot])

    def a_save(layer, slot):
        return pltpu.make_async_copy(abuf, a_out.at[layer, chunk_rows(slot)], a_sem)

    def d_save(layer, slot):
        return pltpu.make_async_copy(abuf, du_out.at[layer, chunk_rows(slot)], a_sem)

    def t_loads(slot):
        own = pl.ds(pl.multiple_of(slot * rows + me * block, block), block)
        return [pltpu.make_async_copy(t_ref.at[own, pl.ds(part * side_w, side_w)], ops.at[0, 1 + part, pl.ds(0, block)], t_sem.at[part]) for part in range(2)]

    def half_load(src, side):
        return pltpu.make_async_copy(src, ops.at[side, 0], l_sem.at[side, 0])

    def full_load(src, side, part):
        return pltpu.make_async_copy(src.at[:, pl.ds(part * side_w, side_w)], ops.at[side, 1 + part], l_sem.at[side, 1 + part])

    def out_copy(dst, part):
        return pltpu.make_async_copy(acc.at[part], dst, o_sem.at[part])

    def out_push(dst, index, part):
        return pltpu.make_async_remote_copy(src_ref=dst, dst_ref=dst, send_sem=res_send.at[index, part], recv_sem=res_recv.at[index, part], device_id={"dp": peer}, device_id_type=MESH)

    def td_part(layer, part):
        return td_out.at[layer - 1, half_of(core), pl.ds(part * side_w, side_w)]

    def tu_part(layer, part):
        return tu_out.at[layer - 1, pl.ds(part * side_w, side_w), half_of(core)]

    def load_granule(q):
        index = q // (2 * SLOTS)
        kind, layer, slot, side = index % 2, top - index // 2, (q % (2 * SLOTS)) // 2, q % 2

        def start(half_src, full_src):
            half_load(half_src, side).start()
            for part in range(2):
                full_load(full_src, side, part).start()

        @pl.when((kind == 0) & (side == 0))
        def _():
            start(a_out.at[layer, chunk_rows(slot), half_of(core)], g_out.at[layer, chunk_rows(slot)])

        @pl.when((kind == 0) & (side == 1))
        def _():
            push_a(layer, slot).wait_recv()
            push_g(layer, slot).wait_recv()
            start(pa_out.at[layer, chunk_rows(slot)], pg_out.at[layer, chunk_rows(slot)])

        @pl.when((kind == 1) & (side == 0))
        def _():
            start(du_out.at[layer, chunk_rows(slot), half_of(core)], h_out.at[layer - 1, chunk_rows(slot)])

        @pl.when((kind == 1) & (side == 1))
        def _():
            push_d(layer, slot).wait_recv()
            push_h(layer, slot).wait_recv()
            start(pd_out.at[layer, chunk_rows(slot)], ph_out.at[layer, chunk_rows(slot)])

    def last_push(part):
        index = 2 * (layers - 1) - 1
        return pltpu.make_async_remote_copy(src_ref=acc.at[part], dst_ref=tu_part(1, part), send_sem=res_send.at[index, part], recv_sem=res_recv.at[index, part], device_id={"dp": peer}, device_id_type=MESH)

    def hand_over(index):
        kind, layer = index % 2, top - index // 2
        for part in range(2):
            out_copy(td_part(1, part), part).wait()

        @pl.when(kind == 0)
        def _():
            for part in range(2):
                out_push(td_part(layer, part), index, part).start()

        @pl.when(kind == 1)
        def _():
            for part in range(2):
                out_push(tu_part(layer, part), index, part).start()

    def run_granule(q):
        index = q // (2 * SLOTS)
        kind, layer, side = index % 2, top - index // 2, q % 2

        @pl.when((q % (2 * SLOTS) == 0) & (q > 0))
        def _():
            hand_over(index - 1)

        @pl.when(q % (2 * SLOTS) == 0)
        def _():
            def clear(i, carry):
                strip = pl.ds(pl.multiple_of(i * 64, 64), 64)
                acc[:, strip, :] = jnp.zeros((2, 64, side_w), jnp.float32)
                return carry

            lax.fori_loop(0, side_w // 64, clear, 0)

        half_load(pa_out.at[0, chunk_rows(0)], side).wait()
        for part in range(2):
            full_load(pg_out.at[0, chunk_rows(0)], side, part).wait()

        def part_step(i, carry):
            part, strip = i // 2, pl.ds(pl.multiple_of(i % 2 * (side_w // 2), side_w // 2), side_w // 2)
            acc[part, strip] += dot_f32(ops[side, kind * (1 + part), :, strip], ops[side, (1 - kind) * (1 + part)], ROW_CONTRACT)
            return carry

        lax.fori_loop(0, 4, part_step, 0)

        @pl.when((q % (2 * SLOTS) == 2 * SLOTS - 1) & (kind == 0))
        def _():
            for part in range(2):
                out_copy(td_part(layer, part), part).start()

        @pl.when((q % (2 * SLOTS) == 2 * SLOTS - 1) & (kind == 1))
        def _():
            for part in range(2):
                out_copy(tu_part(layer, part), part).start()

        @pl.when(q == granules - 1)
        def _():
            for part in range(2):
                last_push(part).start()

    plan = {1: (2, 2, 0), 2: (1, 0, 0), 3: (2, 1, 1), 4: (2, 1, 0), 5: (2, 2, 0), 6: (2, 2, 0), 7: (2, 2, 0), 8: (2, 2, 0), 9: (2, 2, 0), 10: (2, 4, 0), 11: (2, 4, 2)}
    ran = sum(sum(groups) for groups in plan.values())

    def plan_of(n):
        ends = [0, 0, 0, 0]
        for b, groups in plan.items():
            reached, passed = (n - b) // turn, (n - b - 1) // turn
            here = (n // turn) * (reached - passed)
            ends[0] = ends[0] + sum(groups) * passed
            for i, number in enumerate(groups):
                ends[i + 1] = ends[i + 1] + number * here
        for i in range(3):
            ends[i + 1] = ends[i + 1] + ends[i]
        return ends

    def run_granules(begin, end, stop):
        def step(q, carry):
            @pl.when(q + 1 < stop)
            def _():
                load_granule(q + 1)

            run_granule(q)
            return carry

        lax.fori_loop(begin, end, step, 0)

    def receive_rows(n):
        layer, slot = layer_of(n), n % SLOTS

        @pl.when(n < SLOTS)
        def _():
            push_h0(slot).start()
            x_load(slot).wait()

        @pl.when(n >= SLOTS)
        def _():
            for copy in gat2_copies(n):
                copy.wait()
            for copy in gat1_copies(n):
                copy.wait_send()

        @pl.when((n >= SLOTS) & (n < turn))
        def _():
            h_save(layer, slot).start()

        @pl.when(n >= turn)
        def _():
            g_save(layer, slot).start()

    def settle_rows(n):
        layer, slot = layer_of(n), n % SLOTS

        @pl.when((n >= SLOTS) & (n < turn))
        def _():
            h_save(layer, slot).wait()
            push_h(layer, slot).start()

        @pl.when(n >= turn)
        def _():
            g_save(layer, slot).wait()
            push_g(layer, slot).start()

    def share_acts(n):
        layer, slot = layer_of(n), n % SLOTS

        @pl.when(n < turn)
        def _():
            a_save(layer, slot).start()

        @pl.when((n >= turn) & (n < steps))
        def _():
            d_save(layer, slot).start()

    def settle_acts(n):
        layer, slot = layer_of(n), n % SLOTS
        a_save(layer, slot).wait()

        @pl.when(n < SLOTS)
        def _():
            push_a0(slot).start()

        @pl.when((n >= SLOTS) & (n < turn))
        def _():
            push_a(layer, slot).start()

        @pl.when((n >= turn) & (n < steps))
        def _():
            push_d(layer, slot).start()

        @pl.when(n >= steps)
        def _():
            push_d0(slot).wait_send()

    def times_columns(source, stage):
        total = None
        for i in range(tiles):
            cols = pl.ds(i * TILE, TILE)
            part = dot_f32(source(cols), wbuf[stage, :, cols])
            total = part if total is None else total + part
        return total

    def forward_up(n):
        slot = n % SLOTS

        def tile_step(tile, carry):
            index = weight_base(n) + tile
            count = n * tiles + tile
            weight_start(index + 2)
            weight_wait(index)
            pre = times_columns(lambda cols: hbuf[slot, :, cols], index % 3).astype(jnp.bfloat16)

            @pl.when(count >= 2)
            def _():
                u_save(0, 0, count % 2).wait()

            ubuf[count % 2] = pre
            abuf[:, tile_of(tile)] = gelu_tanh(pre.astype(jnp.float32)).astype(jnp.bfloat16)
            u_save(n, tile, count % 2).start()
            return carry

        lax.fori_loop(0, tiles, tile_step, 0)

    def forward_down(n):
        def tile_step(tile, carry):
            index = weight_base(n) + tiles + tile
            weight_start(index + 2)
            weight_wait(index)
            pbuf[n % 2, :, tile_of(tile)] = times_columns(lambda cols: abuf[:, cols], index % 3)

            @pl.when(n == 0)
            def _():
                red1_tiles(tile)

            return carry

        lax.fori_loop(0, tiles, tile_step, 0)

    def backward_up(n):
        slot = n % SLOTS

        @pl.when(n == turn)
        def _():
            for stage in range(2):
                u_save(0, 0, stage).wait()
            u_load(n, 0, n * tiles % 2).start()

        def tile_step(tile, carry):
            index = weight_base(n) + tile
            count = n * tiles + tile
            weight_start(index + 2)

            @pl.when(count + 1 < every * tiles)
            def _():
                u_load((count + 1) // tiles, (count + 1) % tiles, (count + 1) % 2).start()

            weight_wait(index)
            u_load(n, tile, count % 2).wait()
            d_act = dot_f32(hbuf[slot], wbuf[index % 3], COL_CONTRACT)
            _, gelu_vjp = jax.vjp(gelu_tanh, ubuf[count % 2].astype(jnp.float32))
            abuf[:, tile_of(tile)] = gelu_vjp(d_act)[0].astype(jnp.bfloat16)

            @pl.when(n >= steps)
            def _():
                d0_tiles(slot, tile)

            return carry

        lax.fori_loop(0, tiles, tile_step, 0)

    def backward_down(n):
        def tile_step(tile, carry):
            index = weight_base(n) + tiles + tile
            weight_start(index + 2)
            weight_wait(index)
            pbuf[n % 2, :, tile_of(tile)] = dot_f32(abuf[...], wbuf[index % 3], COL_CONTRACT)
            return carry

        lax.fori_loop(0, tiles, tile_step, 0)

    def send_diagonal(n):
        @pl.when(n > 0)
        def _():
            for copy in red1_copies(n):
                copy.start()

    def reduce_step(k):
        first, second = red1_copies(k)
        first.wait_recv()
        pbuf[k % 2, rows_of(y_nbr, 0)] += red1[k % 2, 0]
        second.wait_recv()
        pbuf[k % 2, rows_of(x_nbr, 1)] += red1[k % 2, 1]
        for copy in red2_copies(k):
            copy.start()

        @pl.when((k >= turn - SLOTS) & (k < turn))
        def _():
            for copy in t_loads(k % SLOTS):
                copy.start()

    def finish_step(k):
        slot = k % SLOTS
        for copy in red2_copies(k):
            copy.wait()
        for copy in red1_copies(k):
            copy.wait_send()

        def total():
            return pbuf[k % 2, rows_of(me)] + red2[k % 2, 0] + red2[k % 2, 1]

        def h_new():
            return (hbuf[slot, rows_of(me)].astype(jnp.float32) + total().astype(jnp.bfloat16).astype(jnp.float32)).astype(jnp.bfloat16)

        @pl.when(k < turn - SLOTS)
        def _():
            hbuf[slot, rows_of(me)] = h_new()

        @pl.when((k >= turn - SLOTS) & (k < turn))
        def _():
            for copy in t_loads(slot):
                copy.wait()
            target = jnp.concatenate([ops[0, 1, :block], ops[0, 2, :block]], 1)
            err = (h_new().astype(jnp.float32) - target.astype(jnp.float32)) * (1.0 / total_tokens)
            hbuf[slot, rows_of(me)] = err.astype(jnp.bfloat16)

        @pl.when(k >= turn)
        def _():
            hbuf[slot, rows_of(me)] = (hbuf[slot, rows_of(me)].astype(jnp.float32) + total()).astype(jnp.bfloat16)

        for copy in gat1_copies(k):
            copy.start()

    def forward_rows(k):
        for copy in gat1_copies(k):
            copy.wait_recv()
        for copy in gat2_copies(k):
            copy.start()

    def when_step(k, fn):
        @pl.when((k >= 0) & (k < steps))
        def _():
            fn(k)

    barrier = pltpu.get_barrier_semaphore()
    for target in ({"tp": x_nbr}, {"tp": y_nbr}, {"dp": peer}):
        pl.semaphore_signal(barrier, inc=1, device_id=target, device_id_type=MESH)
    x_load(0).start()
    weight_start(0)
    weight_start(1)
    for slot in range(1, SLOTS):
        x_load(slot).start()
    pl.semaphore_wait(barrier, 3)

    def body(n, carry):
        begin, one, two, stop = plan_of(n)
        receive_rows(n)

        @pl.when(n >= 1)
        def _():
            settle_acts(n - 1)

        @pl.when(n < turn)
        def _():
            forward_up(n)

        @pl.when(n >= turn)
        def _():
            backward_up(n)

        share_acts(n)
        settle_rows(n)

        @pl.when(begin < stop)
        def _():
            load_granule(begin)

        @pl.when(n < turn)
        def _():
            forward_down(n)

        @pl.when(n >= turn)
        def _():
            backward_down(n)

        send_diagonal(n)
        when_step(n - 2, forward_rows)
        run_granules(begin, one, stop)

        @pl.when(n == steps - 1)
        def _():
            reduce_step(n)

        when_step(n - 1, finish_step)
        run_granules(one, two, stop)

        @pl.when(n < steps - 1)
        def _():
            reduce_step(n)

        run_granules(two, stop, stop)
        return carry

    lax.fori_loop(0, steps, body, 0)

    def last_body(n, carry):
        receive_rows(n)
        settle_acts(n - 1)

        @pl.when(n == steps)
        def _():
            load_granule(ran)

        backward_up(n)

        @pl.when(n == steps)
        def _():
            finish_step(steps - 1)
            forward_rows(steps - 2)
            run_granules(ran, granules, granules)

        @pl.when(n == steps + 1)
        def _():
            forward_rows(steps - 1)

        settle_rows(n)
        return carry

    lax.fori_loop(steps, every, last_body, 0)
    settle_acts(every - 1)
    for part in range(2):
        out_copy(tu_part(1, part), part).wait()

    def drain(i, carry):
        layer, slot = i // SLOTS, i % SLOTS
        push_g(layer, slot).wait_send()
        push(PUSH_H, layer, slot, x_ref.at[chunk_rows(slot)], ph_out.at[layer, chunk_rows(slot)]).wait_send()

        @pl.when(layer > 0)
        def _():
            push_a(layer, slot).wait_send()
            push_d(layer, slot).wait_send()

        return carry

    lax.fori_loop(0, layers * SLOTS, drain, 0)
    for slot in range(SLOTS):
        push_a0(slot).wait()
        push_d0(slot).wait_recv()
        push_g(0, slot).wait_recv()
        push_h0(slot).wait_recv()
    for index in range(2 * (layers - 1)):
        for part in range(2):
            out_push(td_part(1, part), index, part).wait()


def run_chain(hidden, targets, w_up, w_down, total_tokens):
    layers, d_model, width = w_up.shape
    tokens = hidden.shape[0]
    rows = tokens // SLOTS
    block = rows // 4
    half = width // 2
    bf16, f32 = jnp.bfloat16, jnp.float32
    flops = 2 * tokens * d_model * width * (6 * layers - 3)
    anywhere = pl.BlockSpec(memory_space=pl.ANY)
    like = jax.ShapeDtypeStruct
    outs = (like((layers - 1, tokens, d_model), bf16), like((layers, tokens, width), bf16), like((layers, tokens, width), bf16),
            like((layers, tokens, d_model), bf16), like((layers, tokens, width), bf16),
            like((layers - 1, width, d_model), f32), like((layers - 1, d_model, width), f32),
            like((layers, tokens, half), bf16), like((layers, tokens, half), bf16),
            like((layers, tokens, d_model), bf16), like((layers, tokens, d_model), bf16),
            like((tokens, width), bf16), like((tokens, width), bf16))
    return pl.pallas_call(
        functools.partial(chain_kernel, layers, total_tokens),
        out_shape=outs,
        in_specs=[anywhere] * 4,
        out_specs=(anywhere,) * len(outs),
        scratch_shapes=[
            pltpu.VMEM((SLOTS, rows, d_model), bf16),
            pltpu.VMEM((rows, width), bf16),
            pltpu.VMEM((2, rows, TILE), bf16),
            pltpu.VMEM((3, TILE, d_model), bf16),
            pltpu.VMEM((2, rows, d_model), f32),
            pltpu.VMEM((2, 2, block // 2, d_model), f32),
            pltpu.VMEM((2, 2, block, d_model), f32),
            pltpu.VMEM((2, half, half), f32),
            pltpu.VMEM((2, 3, rows, half), bf16),
            pltpu.SemaphoreType.DMA((8, SLOTS)),
            pltpu.SemaphoreType.DMA((8, SLOTS)),
            pltpu.SemaphoreType.DMA((4, layers, SLOTS)),
            pltpu.SemaphoreType.DMA((4, layers, SLOTS)),
            pltpu.SemaphoreType.DMA((2 * (layers - 1), 2)),
            pltpu.SemaphoreType.DMA((2 * (layers - 1), 2)),
            pltpu.SemaphoreType.DMA((3,)),
            pltpu.SemaphoreType.DMA((2,)),
            pltpu.SemaphoreType.DMA,
            pltpu.SemaphoreType.DMA((SLOTS,)),
            pltpu.SemaphoreType.DMA((2,)),
            pltpu.SemaphoreType.DMA((2, 3)),
            pltpu.SemaphoreType.DMA((2,)),
        ],
        compiler_params=pltpu.CompilerParams(collective_id=0, has_side_effects=True, vmem_limit_bytes=67043328),
        cost_estimate=pl.CostEstimate(flops=flops, bytes_accessed=layers * tokens * d_model * 16, transcendentals=2 * layers * tokens * width),
        name="step_chain",
    )(hidden, targets, w_up, w_down)


def final_kernel(a_ref, pa_ref, g_ref, pg_ref, x_ref, px_ref, d_ref, pd_ref, td_ref, tu_ref, gd_out, gu_out, acc, lhs, rhs, ring, l_sem, r_sem, o_sem, in_sem, out_sem):
    rows, side_w = lhs.shape[2:]
    strip = ring.shape[1]
    depth = ring.shape[0]
    done_layers, height, _ = td_ref.shape
    per_layer = height // strip
    per_array = done_layers * per_layer
    strips = 2 * per_array
    lag = depth // 2
    core = lax.axis_index("dp")
    a_ref, g_ref, pg_ref, px_ref, d_ref = (ref.at[0] for ref in (a_ref, g_ref, pg_ref, px_ref, d_ref))
    parts = 4
    granules = 4 * SLOTS
    per_grad = granules // 2

    def chunk_rows(slot):
        return pl.ds(pl.multiple_of(slot * rows, rows), rows)

    def half_of(which):
        return pl.ds(pl.multiple_of(which * side_w, side_w), side_w)

    def operand_copies(left, right, slot, stage):
        for part in range(2):
            cols = pl.ds(part * side_w, side_w)
            yield pltpu.make_async_copy(left.at[chunk_rows(slot), cols], lhs.at[stage, part], l_sem.at[stage, part])
            yield pltpu.make_async_copy(right.at[chunk_rows(slot), cols], rhs.at[stage, part], r_sem.at[stage, part])

    def load(q):
        grad, slot, side = q // per_grad, (q % per_grad) // 2, q % 2
        for which, mine, theirs in ((0, (a_ref, g_ref), (pa_ref, pg_ref)), (1, (x_ref, d_ref), (px_ref, pd_ref))):
            @pl.when((grad == which) & (side == core))
            def _():
                for copy in operand_copies(*mine, slot, q % 2):
                    copy.start()

            @pl.when((grad == which) & (side != core))
            def _():
                for copy in operand_copies(*theirs, slot, q % 2):
                    copy.start()

    def out_copy(dst, part):
        return pltpu.make_async_copy(acc.at[part], dst.at[0, half_of(part // 2), half_of(part % 2)], o_sem.at[part])

    def strip_copies(t, src, dst):
        layer, row = (t % per_array) // per_layer, pl.multiple_of((t % per_layer) * strip, strip)
        return (pltpu.make_async_copy(src.at[layer, pl.ds(row, strip)], ring.at[t % depth], in_sem.at[t % depth]),
                pltpu.make_async_copy(ring.at[t % depth], dst.at[layer + 1, pl.ds(row, strip)], out_sem.at[t % depth]))

    def move(t):
        @pl.when((t >= depth) & (t < strips + depth))
        def _():
            strip_copies(t - depth, td_ref, gd_out)[1].wait()

        @pl.when(t < per_array)
        def _():
            strip_copies(t, td_ref, gd_out)[0].start()

        @pl.when((t >= per_array) & (t < strips))
        def _():
            strip_copies(t, tu_ref, gu_out)[0].start()

        late = t - lag

        @pl.when((late >= 0) & (late < per_array))
        def _():
            strip_copies(late, td_ref, gd_out)[0].wait()
            strip_copies(late, td_ref, gd_out)[1].start()

        @pl.when((late >= per_array) & (late < strips))
        def _():
            strip_copies(late, tu_ref, gu_out)[0].wait()
            strip_copies(late, tu_ref, gu_out)[1].start()

    def compute(p):
        q, part = p // parts, p % parts
        stage = q % 2

        @pl.when((part == 0) & (q + 1 < granules))
        def _():
            load(q + 1)

        @pl.when(part == 0)
        def _():
            for copy in operand_copies(a_ref, g_ref, 0, stage):
                copy.wait()

        @pl.when(q == per_grad)
        def _():
            out_copy(gd_out, part).wait()

        @pl.when(q % per_grad == 0)
        def _():
            acc[part] = dot_f32(lhs[stage, part // 2], rhs[stage, part % 2], ROW_CONTRACT)

        @pl.when(q % per_grad > 0)
        def _():
            acc[part] += dot_f32(lhs[stage, part // 2], rhs[stage, part % 2], ROW_CONTRACT)

        @pl.when(q == per_grad - 1)
        def _():
            out_copy(gd_out, part).start()

        @pl.when(q == granules - 1)
        def _():
            out_copy(gu_out, part).start()

    load(0)

    def body(p, carry):
        move(p)
        compute(p)
        return carry

    lax.fori_loop(0, parts * granules, body, 0)

    def flush(t, carry):
        move(t)
        return carry

    lax.fori_loop(parts * granules, max(strips + depth, parts * granules), flush, 0)
    for part in range(parts):
        out_copy(gu_out, part).wait()


def run_final(operands, t_down, t_up):
    layers, width, d_model = t_down.shape[0] + 1, t_down.shape[1], t_down.shape[2]
    tokens = operands[1].shape[0]
    rows, side_w = tokens // SLOTS, width // 2
    bf16, f32 = jnp.bfloat16, jnp.float32
    anywhere = pl.BlockSpec(memory_space=pl.ANY)
    return pl.pallas_call(
        final_kernel,
        out_shape=(jax.ShapeDtypeStruct((layers, width, d_model), f32), jax.ShapeDtypeStruct((layers, d_model, width), f32)),
        in_specs=[anywhere] * 10,
        out_specs=(anywhere,) * 2,
        scratch_shapes=[
            pltpu.VMEM((4, side_w, side_w), f32),
            pltpu.VMEM((2, 2, rows, side_w), bf16),
            pltpu.VMEM((2, 2, rows, side_w), bf16),
            pltpu.VMEM((8, 256, d_model), f32),
            pltpu.SemaphoreType.DMA((2, 2)),
            pltpu.SemaphoreType.DMA((2, 2)),
            pltpu.SemaphoreType.DMA((4,)),
            pltpu.SemaphoreType.DMA((8,)),
            pltpu.SemaphoreType.DMA((8,)),
        ],
        compiler_params=pltpu.CompilerParams(vmem_limit_bytes=67043328),
        cost_estimate=pl.CostEstimate(flops=8 * tokens * d_model * width, bytes_accessed=16 * layers * d_model * width, transcendentals=0),
        name="final_grads",
    )(*operands, t_down, t_up)


def local_step(hidden, targets, w_up, w_down, total_tokens):
    _, _, act_all, g_all, d_all, t_down, t_up, _, _, pg, ph, pa0, pd0 = run_chain(hidden, targets, w_up, w_down, total_tokens)
    grad_down, grad_up = run_final((act_all, pa0, g_all, pg, hidden, ph, d_all, pd0), t_down, t_up)
    return grad_up, grad_down


def solution(mesh):
    def grad_step(hidden_in, targets, w_up, w_down):
        step_fn = functools.partial(local_step, total_tokens=hidden_in.shape[0])
        mapped = jax.shard_map(step_fn, mesh=mesh, in_specs=(P("dp", None), P("dp", None), P(None, None, "tp"), P(None, "tp", None)), out_specs=(P(None, None, "tp"), P(None, "tp", None)), check_vma=False)
        return mapped(hidden_in, targets, w_up, w_down)

    return grad_step
```

```python
import functools
import jax
import jax.numpy as jnp
from jax import lax
from jax.experimental import pallas as pl
from jax.experimental.pallas import tpu as pltpu
from jax.sharding import PartitionSpec as P

ROW_CONTRACT = (((0,), (0,)), ((), ()))
COL_CONTRACT = (((1,), (1,)), ((), ()))
MESH = pl.DeviceIdType.MESH
SLOTS = 4
TILE = 512
RED1_X, RED1_Y, RED2_X, RED2_Y, GAT1_X, GAT1_Y, GAT2_X, GAT2_Y = range(8)


def gelu_tanh(value):
    return jax.nn.gelu(value, approximate=True)


def dot_f32(lhs, rhs, dims=(((1,), (0,)), ((), ()))):
    return lax.dot_general(lhs, rhs, dims, preferred_element_type=jnp.float32)


PUSH_A, PUSH_D, PUSH_G, PUSH_H = range(4)


def chain_kernel(layers, total_tokens, x_ref, t_ref, wu_ref, wd_ref,
                 h_out, u_out, a_out, g_out, du_out, td_out, tu_out, pa_out, pd_out, pg_out, ph_out, pa0_out, pd0_out,
                 hbuf, abuf, ubuf, wbuf, pbuf, red1, red2, acc, ops,
                 send_sem, recv_sem, push_send, push_recv, res_send, res_recv, w_sem, u_sem, a_sem, h_sem, t_sem, l_sem, o_sem):
    rows, d_model = hbuf.shape[1:]
    block = rows // 4
    half = block // 2
    tiles = d_model // TILE
    side_w = d_model // 2
    turn = layers * SLOTS
    steps = turn + (layers - 1) * SLOTS
    every = steps + SLOTS
    top = layers - 1
    granules = 2 * (layers - 1) * 2 * SLOTS
    me = lax.axis_index("tp")
    core = lax.axis_index("dp")
    peer = 1 - core
    mx, my = me % 2, me // 2
    x_nbr = my * 2 + (1 - mx)
    y_nbr = (1 - my) * 2 + mx
    diag = (1 - my) * 2 + (1 - mx)

    def rows_of(owner, part=None):
        if part is None:
            return pl.ds(pl.multiple_of(owner * block, block), block)
        return pl.ds(pl.multiple_of(owner * block + part * half, half), half)

    def chunk_rows(slot):
        return pl.ds(pl.multiple_of(slot * rows, rows), rows)

    def half_of(which):
        return pl.ds(pl.multiple_of(which * side_w, side_w), side_w)

    def tile_of(tile):
        return pl.ds(pl.multiple_of(tile * TILE, TILE), TILE)

    def layer_of(n):
        back = n // turn
        return (1 - back) * (n // SLOTS) + back * (2 * layers - 1 - n // SLOTS)

    def remote(kind, k, src, dst, target):
        return pltpu.make_async_remote_copy(src_ref=src, dst_ref=dst, send_sem=send_sem.at[kind, k % SLOTS], recv_sem=recv_sem.at[kind, k % SLOTS], device_id={"tp": target}, device_id_type=MESH)

    def red1_copies(k):
        return (remote(RED1_X, k, pbuf.at[k % 2, rows_of(diag, 0)], red1.at[k % 2, 0], x_nbr),
                remote(RED1_Y, k, pbuf.at[k % 2, rows_of(diag, 1)], red1.at[k % 2, 1], y_nbr))

    def red1_tiles(tile):
        for kind, part, target in ((RED1_X, 0, x_nbr), (RED1_Y, 1, y_nbr)):
            remote(kind, 0, pbuf.at[0, rows_of(diag, part), tile_of(tile)], red1.at[0, part, :, tile_of(tile)], target).start()

    def red2_copies(k):
        return (remote(RED2_X, k, pbuf.at[k % 2, rows_of(x_nbr)], red2.at[k % 2, 0], x_nbr),
                remote(RED2_Y, k, pbuf.at[k % 2, rows_of(y_nbr)], red2.at[k % 2, 1], y_nbr))

    def gat1_copies(k):
        mine = hbuf.at[k % SLOTS, rows_of(me)]
        return (remote(GAT1_X, k, mine, mine, x_nbr), remote(GAT1_Y, k, mine, mine, y_nbr))

    def gat2_copies(k):
        from_y = hbuf.at[k % SLOTS, rows_of(y_nbr, 0)]
        from_x = hbuf.at[k % SLOTS, rows_of(x_nbr, 1)]
        return (remote(GAT2_X, k, from_y, from_y, x_nbr), remote(GAT2_Y, k, from_x, from_x, y_nbr))

    def push(kind, layer, slot, src, dst):
        return pltpu.make_async_remote_copy(src_ref=src, dst_ref=dst, send_sem=push_send.at[kind, layer, slot], recv_sem=push_recv.at[kind, layer, slot], device_id={"dp": peer}, device_id_type=MESH)

    def push_a(layer, slot):
        return push(PUSH_A, layer, slot, a_out.at[layer, chunk_rows(slot), half_of(peer)], pa_out.at[layer, chunk_rows(slot)])

    def push_d(layer, slot):
        return push(PUSH_D, layer, slot, du_out.at[layer, chunk_rows(slot), half_of(peer)], pd_out.at[layer, chunk_rows(slot)])

    def push_a0(slot):
        return push(PUSH_A, 0, slot, a_out.at[0, chunk_rows(slot)], pa0_out.at[chunk_rows(slot)])

    def d0_tiles(slot, tile):
        part = abuf.at[:, tile_of(tile)]
        push(PUSH_D, 0, slot, part, pd0_out.at[chunk_rows(slot), tile_of(tile)]).start()
        pltpu.make_async_copy(part, du_out.at[0, chunk_rows(slot), tile_of(tile)], a_sem).start()

    def push_d0(slot):
        return push(PUSH_D, 0, slot, abuf, pd0_out.at[chunk_rows(slot)])

    def push_g(layer, slot):
        return push(PUSH_G, layer, slot, g_out.at[layer, chunk_rows(slot)], pg_out.at[layer, chunk_rows(slot)])

    def push_h(layer, slot):
        return push(PUSH_H, layer, slot, h_out.at[layer - 1, chunk_rows(slot)], ph_out.at[layer, chunk_rows(slot)])

    def push_h0(slot):
        return push(PUSH_H, 0, slot, x_ref.at[chunk_rows(slot)], ph_out.at[0, chunk_rows(slot)])

    def weight_copy(ref, layer, tile, stage):
        return pltpu.make_async_copy(ref.at[layer, tile_of(tile)], wbuf.at[stage], w_sem.at[stage])

    def column_copies(ref, layer, tile, stage):
        for i in range(tiles):
            block_rows = pl.ds(i * TILE, TILE)
            pltpu.make_async_copy(ref.at[layer, block_rows, tile_of(tile)], wbuf.at[stage, :, block_rows], w_sem.at[stage]).start()

    def weight_start(index):
        main = steps * 2 * tiles
        n, place = index // (2 * tiles), index % (2 * tiles)
        up = 1 - place // tiles
        use_up = (1 - n // turn) * up + (n // turn) * (1 - up)

        @pl.when((n < turn) & (use_up == 1))
        def _():
            column_copies(wu_ref, layer_of(n), place % tiles, index % 3)

        @pl.when((n < turn) & (use_up == 0))
        def _():
            column_copies(wd_ref, layer_of(n), place % tiles, index % 3)

        @pl.when((n >= turn) & (index < main) & (use_up == 1))
        def _():
            weight_copy(wu_ref, layer_of(n), place % tiles, index % 3).start()

        @pl.when((n >= turn) & (index < main) & (use_up == 0))
        def _():
            weight_copy(wd_ref, layer_of(n), place % tiles, index % 3).start()

        @pl.when((index >= main) & (index < main + SLOTS * tiles))
        def _():
            weight_copy(wd_ref, 0, (index - main) % tiles, index % 3).start()

    def weight_wait(index):
        weight_copy(wu_ref, 0, 0, index % 3).wait()

    def weight_base(n):
        late = (n // steps) * (n - steps)
        return (n - late) * 2 * tiles + late * tiles

    def u_save(n, tile, stage):
        return pltpu.make_async_copy(ubuf.at[stage], u_out.at[layer_of(n), chunk_rows(n % SLOTS), tile_of(tile)], u_sem.at[stage])

    def u_load(n, tile, stage):
        return pltpu.make_async_copy(u_out.at[layer_of(n), chunk_rows(n % SLOTS), tile_of(tile)], ubuf.at[stage], u_sem.at[stage])

    def x_load(slot):
        return pltpu.make_async_copy(x_ref.at[chunk_rows(slot)], hbuf.at[slot], h_sem.at[slot])

    def h_save(layer, slot):
        return pltpu.make_async_copy(hbuf.at[slot], h_out.at[layer - 1, chunk_rows(slot)], h_sem.at[slot])

    def g_save(layer, slot):
        return pltpu.make_async_copy(hbuf.at[slot], g_out.at[layer, chunk_rows(slot)], h_sem.at[slot])

    def a_save(layer, slot):
        return pltpu.make_async_copy(abuf, a_out.at[layer, chunk_rows(slot)], a_sem)

    def d_save(layer, slot):
        return pltpu.make_async_copy(abuf, du_out.at[layer, chunk_rows(slot)], a_sem)

    def t_loads(slot):
        own = pl.ds(pl.multiple_of(slot * rows + me * block, block), block)
        return [pltpu.make_async_copy(t_ref.at[own, pl.ds(part * side_w, side_w)], ops.at[0, 1 + part, pl.ds(0, block)], t_sem.at[part]) for part in range(2)]

    def half_load(src, side):
        return pltpu.make_async_copy(src, ops.at[side, 0], l_sem.at[side, 0])

    def full_load(src, side, part):
        return pltpu.make_async_copy(src.at[:, pl.ds(part * side_w, side_w)], ops.at[side, 1 + part], l_sem.at[side, 1 + part])

    def out_copy(dst, part):
        return pltpu.make_async_copy(acc.at[part], dst, o_sem.at[part])

    def out_push(dst, index, part):
        return pltpu.make_async_remote_copy(src_ref=dst, dst_ref=dst, send_sem=res_send.at[index, part], recv_sem=res_recv.at[index, part], device_id={"dp": peer}, device_id_type=MESH)

    def td_part(layer, part):
        return td_out.at[layer - 1, half_of(core), pl.ds(part * side_w, side_w)]

    def tu_part(layer, part):
        return tu_out.at[layer - 1, pl.ds(part * side_w, side_w), half_of(core)]

    def load_granule(q):
        index = q // (2 * SLOTS)
        kind, layer, slot, side = index % 2, top - index // 2, (q % (2 * SLOTS)) // 2, q % 2

        def start(half_src, full_src):
            half_load(half_src, side).start()
            for part in range(2):
                full_load(full_src, side, part).start()

        @pl.when((kind == 0) & (side == 0))
        def _():
            start(a_out.at[layer, chunk_rows(slot), half_of(core)], g_out.at[layer, chunk_rows(slot)])

        @pl.when((kind == 0) & (side == 1))
        def _():
            push_a(layer, slot).wait_recv()
            push_g(layer, slot).wait_recv()
            start(pa_out.at[layer, chunk_rows(slot)], pg_out.at[layer, chunk_rows(slot)])

        @pl.when((kind == 1) & (side == 0))
        def _():
            start(du_out.at[layer, chunk_rows(slot), half_of(core)], h_out.at[layer - 1, chunk_rows(slot)])

        @pl.when((kind == 1) & (side == 1))
        def _():
            push_d(layer, slot).wait_recv()
            push_h(layer, slot).wait_recv()
            start(pd_out.at[layer, chunk_rows(slot)], ph_out.at[layer, chunk_rows(slot)])

    def last_push(part):
        index = 2 * (layers - 1) - 1
        return pltpu.make_async_remote_copy(src_ref=acc.at[part], dst_ref=tu_part(1, part), send_sem=res_send.at[index, part], recv_sem=res_recv.at[index, part], device_id={"dp": peer}, device_id_type=MESH)

    def hand_over(index):
        kind, layer = index % 2, top - index // 2
        for part in range(2):
            out_copy(td_part(1, part), part).wait()

        @pl.when(kind == 0)
        def _():
            for part in range(2):
                out_push(td_part(layer, part), index, part).start()

        @pl.when(kind == 1)
        def _():
            for part in range(2):
                out_push(tu_part(layer, part), index, part).start()

    def run_granule(q):
        index = q // (2 * SLOTS)
        kind, layer, side = index % 2, top - index // 2, q % 2

        @pl.when((q % (2 * SLOTS) == 0) & (q > 0))
        def _():
            hand_over(index - 1)

        @pl.when(q % (2 * SLOTS) == 0)
        def _():
            def clear(i, carry):
                strip = pl.ds(pl.multiple_of(i * 64, 64), 64)
                acc[:, strip, :] = jnp.zeros((2, 64, side_w), jnp.float32)
                return carry

            lax.fori_loop(0, side_w // 64, clear, 0)

        half_load(pa_out.at[0, chunk_rows(0)], side).wait()
        for part in range(2):
            full_load(pg_out.at[0, chunk_rows(0)], side, part).wait()

        def part_step(i, carry):
            part, strip = i // 2, pl.ds(pl.multiple_of(i % 2 * (side_w // 2), side_w // 2), side_w // 2)
            acc[part, strip] += dot_f32(ops[side, kind * (1 + part), :, strip], ops[side, (1 - kind) * (1 + part)], ROW_CONTRACT)
            return carry

        lax.fori_loop(0, 4, part_step, 0)

        @pl.when((q % (2 * SLOTS) == 2 * SLOTS - 1) & (kind == 0))
        def _():
            for part in range(2):
                out_copy(td_part(layer, part), part).start()

        @pl.when((q % (2 * SLOTS) == 2 * SLOTS - 1) & (kind == 1))
        def _():
            for part in range(2):
                out_copy(tu_part(layer, part), part).start()

        @pl.when(q == granules - 1)
        def _():
            for part in range(2):
                last_push(part).start()

    plan = {1: (2, 2, 0), 2: (1, 0, 0), 3: (2, 1, 1), 4: (2, 1, 0), 5: (2, 2, 0), 6: (2, 2, 0), 7: (2, 2, 0), 8: (2, 2, 0), 9: (2, 2, 0), 10: (2, 4, 0), 11: (2, 4, 2)}
    ran = sum(sum(groups) for groups in plan.values())

    def plan_of(n):
        ends = [0, 0, 0, 0]
        for b, groups in plan.items():
            reached, passed = (n - b) // turn, (n - b - 1) // turn
            here = (n // turn) * (reached - passed)
            ends[0] = ends[0] + sum(groups) * passed
            for i, number in enumerate(groups):
                ends[i + 1] = ends[i + 1] + number * here
        for i in range(3):
            ends[i + 1] = ends[i + 1] + ends[i]
        return ends

    def run_granules(begin, end, stop):
        def step(q, carry):
            @pl.when(q + 1 < stop)
            def _():
                load_granule(q + 1)

            run_granule(q)
            return carry

        lax.fori_loop(begin, end, step, 0)

    def receive_rows(n):
        layer, slot = layer_of(n), n % SLOTS

        @pl.when(n < SLOTS)
        def _():
            push_h0(slot).start()
            x_load(slot).wait()

        @pl.when(n >= SLOTS)
        def _():
            for copy in gat2_copies(n):
                copy.wait()
            for copy in gat1_copies(n):
                copy.wait_send()

        @pl.when((n >= SLOTS) & (n < turn))
        def _():
            h_save(layer, slot).start()

        @pl.when(n >= turn)
        def _():
            g_save(layer, slot).start()

    def settle_rows(n):
        layer, slot = layer_of(n), n % SLOTS

        @pl.when((n >= SLOTS) & (n < turn))
        def _():
            h_save(layer, slot).wait()
            push_h(layer, slot).start()

        @pl.when(n >= turn)
        def _():
            g_save(layer, slot).wait()
            push_g(layer, slot).start()

    def share_acts(n):
        layer, slot = layer_of(n), n % SLOTS

        @pl.when(n < turn)
        def _():
            a_save(layer, slot).start()

        @pl.when((n >= turn) & (n < steps))
        def _():
            d_save(layer, slot).start()

    def settle_acts(n):
        layer, slot = layer_of(n), n % SLOTS
        a_save(layer, slot).wait()

        @pl.when(n < SLOTS)
        def _():
            push_a0(slot).start()

        @pl.when((n >= SLOTS) & (n < turn))
        def _():
            push_a(layer, slot).start()

        @pl.when((n >= turn) & (n < steps))
        def _():
            push_d(layer, slot).start()

        @pl.when(n >= steps)
        def _():
            push_d0(slot).wait_send()

    def times_columns(source, stage):
        total = None
        for i in range(tiles):
            cols = pl.ds(i * TILE, TILE)
            part = dot_f32(source(cols), wbuf[stage, :, cols])
            total = part if total is None else total + part
        return total

    def forward_up(n):
        slot = n % SLOTS

        def tile_step(tile, carry):
            index = weight_base(n) + tile
            count = n * tiles + tile
            weight_start(index + 2)
            weight_wait(index)
            pre = times_columns(lambda cols: hbuf[slot, :, cols], index % 3).astype(jnp.bfloat16)

            @pl.when(count >= 2)
            def _():
                u_save(0, 0, count % 2).wait()

            ubuf[count % 2] = pre
            abuf[:, tile_of(tile)] = gelu_tanh(pre.astype(jnp.float32)).astype(jnp.bfloat16)
            u_save(n, tile, count % 2).start()
            return carry

        lax.fori_loop(0, tiles, tile_step, 0)

    def forward_down(n):
        def tile_step(tile, carry):
            index = weight_base(n) + tiles + tile
            weight_start(index + 2)
            weight_wait(index)
            pbuf[n % 2, :, tile_of(tile)] = times_columns(lambda cols: abuf[:, cols], index % 3)

            @pl.when(n == 0)
            def _():
                red1_tiles(tile)

            return carry

        lax.fori_loop(0, tiles, tile_step, 0)

    def backward_up(n):
        slot = n % SLOTS

        @pl.when(n == turn)
        def _():
            for stage in range(2):
                u_save(0, 0, stage).wait()
            u_load(n, 0, n * tiles % 2).start()

        def tile_step(tile, carry):
            index = weight_base(n) + tile
            count = n * tiles + tile
            weight_start(index + 2)

            @pl.when(count + 1 < every * tiles)
            def _():
                u_load((count + 1) // tiles, (count + 1) % tiles, (count + 1) % 2).start()

            weight_wait(index)
            u_load(n, tile, count % 2).wait()
            d_act = dot_f32(hbuf[slot], wbuf[index % 3], COL_CONTRACT)
            _, gelu_vjp = jax.vjp(gelu_tanh, ubuf[count % 2].astype(jnp.float32))
            abuf[:, tile_of(tile)] = gelu_vjp(d_act)[0].astype(jnp.bfloat16)

            @pl.when(n >= steps)
            def _():
                d0_tiles(slot, tile)

            return carry

        lax.fori_loop(0, tiles, tile_step, 0)

    def backward_down(n):
        def tile_step(tile, carry):
            index = weight_base(n) + tiles + tile
            weight_start(index + 2)
            weight_wait(index)
            pbuf[n % 2, :, tile_of(tile)] = dot_f32(abuf[...], wbuf[index % 3], COL_CONTRACT)
            return carry

        lax.fori_loop(0, tiles, tile_step, 0)

    def send_diagonal(n):
        @pl.when(n > 0)
        def _():
            for copy in red1_copies(n):
                copy.start()

    def reduce_step(k):
        first, second = red1_copies(k)
        first.wait_recv()
        pbuf[k % 2, rows_of(y_nbr, 0)] += red1[k % 2, 0]
        second.wait_recv()
        pbuf[k % 2, rows_of(x_nbr, 1)] += red1[k % 2, 1]
        for copy in red2_copies(k):
            copy.start()

        @pl.when((k >= turn - SLOTS) & (k < turn))
        def _():
            for copy in t_loads(k % SLOTS):
                copy.start()

    def finish_step(k):
        slot = k % SLOTS
        for copy in red2_copies(k):
            copy.wait()
        for copy in red1_copies(k):
            copy.wait_send()

        def total():
            return pbuf[k % 2, rows_of(me)] + red2[k % 2, 0] + red2[k % 2, 1]

        def h_new():
            return (hbuf[slot, rows_of(me)].astype(jnp.float32) + total().astype(jnp.bfloat16).astype(jnp.float32)).astype(jnp.bfloat16)

        @pl.when(k < turn - SLOTS)
        def _():
            hbuf[slot, rows_of(me)] = h_new()

        @pl.when((k >= turn - SLOTS) & (k < turn))
        def _():
            for copy in t_loads(slot):
                copy.wait()
            target = jnp.concatenate([ops[0, 1, :block], ops[0, 2, :block]], 1)
            err = (h_new().astype(jnp.float32) - target.astype(jnp.float32)) * (1.0 / total_tokens)
            hbuf[slot, rows_of(me)] = err.astype(jnp.bfloat16)

        @pl.when(k >= turn)
        def _():
            hbuf[slot, rows_of(me)] = (hbuf[slot, rows_of(me)].astype(jnp.float32) + total()).astype(jnp.bfloat16)

        for copy in gat1_copies(k):
            copy.start()

    def forward_rows(k):
        for copy in gat1_copies(k):
            copy.wait_recv()
        for copy in gat2_copies(k):
            copy.start()

    def when_step(k, fn):
        @pl.when((k >= 0) & (k < steps))
        def _():
            fn(k)

    barrier = pltpu.get_barrier_semaphore()
    for target in ({"tp": x_nbr}, {"tp": y_nbr}, {"dp": peer}):
        pl.semaphore_signal(barrier, inc=1, device_id=target, device_id_type=MESH)
    x_load(0).start()
    weight_start(0)
    weight_start(1)
    for slot in range(1, SLOTS):
        x_load(slot).start()
    pl.semaphore_wait(barrier, 3)

    def body(n, carry):
        begin, one, two, stop = plan_of(n)
        receive_rows(n)

        @pl.when(n >= 1)
        def _():
            settle_acts(n - 1)

        when_step(n - 2, forward_rows)

        @pl.when(n < turn)
        def _():
            forward_up(n)

        @pl.when(n >= turn)
        def _():
            backward_up(n)

        share_acts(n)
        settle_rows(n)

        @pl.when(begin < stop)
        def _():
            load_granule(begin)

        @pl.when(n < turn)
        def _():
            forward_down(n)

        @pl.when(n >= turn)
        def _():
            backward_down(n)

        send_diagonal(n)
        run_granules(begin, one, stop)
        when_step(n - 1, finish_step)
        run_granules(one, two, stop)
        reduce_step(n)
        run_granules(two, stop, stop)
        return carry

    lax.fori_loop(0, steps, body, 0)
    forward_rows(steps - 2)

    def last_body(n, carry):
        receive_rows(n)
        settle_acts(n - 1)

        @pl.when(n == steps)
        def _():
            load_granule(ran)

        backward_up(n)

        @pl.when(n == steps)
        def _():
            run_granules(ran, ran + 1, granules)
            finish_step(steps - 1)
            run_granules(ran + 1, granules, granules)

        @pl.when(n == steps + 1)
        def _():
            forward_rows(steps - 1)

        settle_rows(n)
        return carry

    lax.fori_loop(steps, every, last_body, 0)
    settle_acts(every - 1)
    for part in range(2):
        out_copy(tu_part(1, part), part).wait()

    def drain(i, carry):
        layer, slot = i // SLOTS, i % SLOTS
        push_g(layer, slot).wait_send()
        push(PUSH_H, layer, slot, x_ref.at[chunk_rows(slot)], ph_out.at[layer, chunk_rows(slot)]).wait_send()

        @pl.when(layer > 0)
        def _():
            push_a(layer, slot).wait_send()
            push_d(layer, slot).wait_send()

        return carry

    lax.fori_loop(0, layers * SLOTS, drain, 0)
    for slot in range(SLOTS):
        push_a0(slot).wait()
        push_d0(slot).wait_recv()
        push_g(0, slot).wait_recv()
        push_h0(slot).wait_recv()
    for index in range(2 * (layers - 1)):
        for part in range(2):
            out_push(td_part(1, part), index, part).wait()


def run_chain(hidden, targets, w_up, w_down, total_tokens):
    layers, d_model, width = w_up.shape
    tokens = hidden.shape[0]
    rows = tokens // SLOTS
    block = rows // 4
    half = width // 2
    bf16, f32 = jnp.bfloat16, jnp.float32
    flops = 2 * tokens * d_model * width * (6 * layers - 3)
    anywhere = pl.BlockSpec(memory_space=pl.ANY)
    like = jax.ShapeDtypeStruct
    outs = (like((layers - 1, tokens, d_model), bf16), like((layers, tokens, width), bf16), like((layers, tokens, width), bf16),
            like((layers, tokens, d_model), bf16), like((layers, tokens, width), bf16),
            like((layers - 1, width, d_model), f32), like((layers - 1, d_model, width), f32),
            like((layers, tokens, half), bf16), like((layers, tokens, half), bf16),
            like((layers, tokens, d_model), bf16), like((layers, tokens, d_model), bf16),
            like((tokens, width), bf16), like((tokens, width), bf16))
    return pl.pallas_call(
        functools.partial(chain_kernel, layers, total_tokens),
        out_shape=outs,
        in_specs=[anywhere] * 4,
        out_specs=(anywhere,) * len(outs),
        scratch_shapes=[
            pltpu.VMEM((SLOTS, rows, d_model), bf16),
            pltpu.VMEM((rows, width), bf16),
            pltpu.VMEM((2, rows, TILE), bf16),
            pltpu.VMEM((3, TILE, d_model), bf16),
            pltpu.VMEM((2, rows, d_model), f32),
            pltpu.VMEM((2, 2, block // 2, d_model), f32),
            pltpu.VMEM((2, 2, block, d_model), f32),
            pltpu.VMEM((2, half, half), f32),
            pltpu.VMEM((2, 3, rows, half), bf16),
            pltpu.SemaphoreType.DMA((8, SLOTS)),
            pltpu.SemaphoreType.DMA((8, SLOTS)),
            pltpu.SemaphoreType.DMA((4, layers, SLOTS)),
            pltpu.SemaphoreType.DMA((4, layers, SLOTS)),
            pltpu.SemaphoreType.DMA((2 * (layers - 1), 2)),
            pltpu.SemaphoreType.DMA((2 * (layers - 1), 2)),
            pltpu.SemaphoreType.DMA((3,)),
            pltpu.SemaphoreType.DMA((2,)),
            pltpu.SemaphoreType.DMA,
            pltpu.SemaphoreType.DMA((SLOTS,)),
            pltpu.SemaphoreType.DMA((2,)),
            pltpu.SemaphoreType.DMA((2, 3)),
            pltpu.SemaphoreType.DMA((2,)),
        ],
        compiler_params=pltpu.CompilerParams(collective_id=0, has_side_effects=True, vmem_limit_bytes=67043328),
        cost_estimate=pl.CostEstimate(flops=flops, bytes_accessed=layers * tokens * d_model * 16, transcendentals=2 * layers * tokens * width),
        name="step_chain",
    )(hidden, targets, w_up, w_down)


def final_kernel(a_ref, pa_ref, g_ref, pg_ref, x_ref, px_ref, d_ref, pd_ref, td_ref, tu_ref, gd_out, gu_out, acc, lhs, rhs, ring, l_sem, r_sem, o_sem, in_sem, out_sem):
    rows, side_w = lhs.shape[2:]
    strip = ring.shape[1]
    depth = ring.shape[0]
    done_layers, height, _ = td_ref.shape
    per_layer = height // strip
    per_array = done_layers * per_layer
    strips = 2 * per_array
    lag = depth // 2
    core = lax.axis_index("dp")
    a_ref, g_ref, pg_ref, px_ref, d_ref = (ref.at[0] for ref in (a_ref, g_ref, pg_ref, px_ref, d_ref))
    parts = 4
    granules = 4 * SLOTS
    per_grad = granules // 2

    def chunk_rows(slot):
        return pl.ds(pl.multiple_of(slot * rows, rows), rows)

    def half_of(which):
        return pl.ds(pl.multiple_of(which * side_w, side_w), side_w)

    def operand_copies(left, right, slot, stage):
        for part in range(2):
            cols = pl.ds(part * side_w, side_w)
            yield pltpu.make_async_copy(left.at[chunk_rows(slot), cols], lhs.at[stage, part], l_sem.at[stage, part])
            yield pltpu.make_async_copy(right.at[chunk_rows(slot), cols], rhs.at[stage, part], r_sem.at[stage, part])

    def load(q):
        grad, slot, side = q // per_grad, (q % per_grad) // 2, q % 2
        for which, mine, theirs in ((0, (a_ref, g_ref), (pa_ref, pg_ref)), (1, (x_ref, d_ref), (px_ref, pd_ref))):
            @pl.when((grad == which) & (side == core))
            def _():
                for copy in operand_copies(*mine, slot, q % 2):
                    copy.start()

            @pl.when((grad == which) & (side != core))
            def _():
                for copy in operand_copies(*theirs, slot, q % 2):
                    copy.start()

    def out_copy(dst, part):
        return pltpu.make_async_copy(acc.at[part], dst.at[0, half_of(part // 2), half_of(part % 2)], o_sem.at[part])

    def strip_copies(t, src, dst):
        layer, row = (t % per_array) // per_layer, pl.multiple_of((t % per_layer) * strip, strip)
        return (pltpu.make_async_copy(src.at[layer, pl.ds(row, strip)], ring.at[t % depth], in_sem.at[t % depth]),
                pltpu.make_async_copy(ring.at[t % depth], dst.at[layer + 1, pl.ds(row, strip)], out_sem.at[t % depth]))

    def move(t):
        @pl.when((t >= depth) & (t < strips + depth))
        def _():
            strip_copies(t - depth, td_ref, gd_out)[1].wait()

        @pl.when(t < per_array)
        def _():
            strip_copies(t, td_ref, gd_out)[0].start()

        @pl.when((t >= per_array) & (t < strips))
        def _():
            strip_copies(t, tu_ref, gu_out)[0].start()

        late = t - lag

        @pl.when((late >= 0) & (late < per_array))
        def _():
            strip_copies(late, td_ref, gd_out)[0].wait()
            strip_copies(late, td_ref, gd_out)[1].start()

        @pl.when((late >= per_array) & (late < strips))
        def _():
            strip_copies(late, tu_ref, gu_out)[0].wait()
            strip_copies(late, tu_ref, gu_out)[1].start()

    def compute(p):
        q, part = p // parts, p % parts
        stage = q % 2

        @pl.when((part == 0) & (q + 1 < granules))
        def _():
            load(q + 1)

        @pl.when(part == 0)
        def _():
            for copy in operand_copies(a_ref, g_ref, 0, stage):
                copy.wait()

        @pl.when(q == per_grad)
        def _():
            out_copy(gd_out, part).wait()

        @pl.when(q % per_grad == 0)
        def _():
            acc[part] = dot_f32(lhs[stage, part // 2], rhs[stage, part % 2], ROW_CONTRACT)

        @pl.when(q % per_grad > 0)
        def _():
            acc[part] += dot_f32(lhs[stage, part // 2], rhs[stage, part % 2], ROW_CONTRACT)

        @pl.when(q == per_grad - 1)
        def _():
            out_copy(gd_out, part).start()

        @pl.when(q == granules - 1)
        def _():
            out_copy(gu_out, part).start()

    load(0)

    def body(p, carry):
        move(p)
        compute(p)
        return carry

    lax.fori_loop(0, parts * granules, body, 0)

    def flush(t, carry):
        move(t)
        return carry

    lax.fori_loop(parts * granules, max(strips + depth, parts * granules), flush, 0)
    for part in range(parts):
        out_copy(gu_out, part).wait()


def run_final(operands, t_down, t_up):
    layers, width, d_model = t_down.shape[0] + 1, t_down.shape[1], t_down.shape[2]
    tokens = operands[1].shape[0]
    rows, side_w = tokens // SLOTS, width // 2
    bf16, f32 = jnp.bfloat16, jnp.float32
    anywhere = pl.BlockSpec(memory_space=pl.ANY)
    return pl.pallas_call(
        final_kernel,
        out_shape=(jax.ShapeDtypeStruct((layers, width, d_model), f32), jax.ShapeDtypeStruct((layers, d_model, width), f32)),
        in_specs=[anywhere] * 10,
        out_specs=(anywhere,) * 2,
        scratch_shapes=[
            pltpu.VMEM((4, side_w, side_w), f32),
            pltpu.VMEM((2, 2, rows, side_w), bf16),
            pltpu.VMEM((2, 2, rows, side_w), bf16),
            pltpu.VMEM((8, 256, d_model), f32),
            pltpu.SemaphoreType.DMA((2, 2)),
            pltpu.SemaphoreType.DMA((2, 2)),
            pltpu.SemaphoreType.DMA((4,)),
            pltpu.SemaphoreType.DMA((8,)),
            pltpu.SemaphoreType.DMA((8,)),
        ],
        compiler_params=pltpu.CompilerParams(vmem_limit_bytes=67043328),
        cost_estimate=pl.CostEstimate(flops=8 * tokens * d_model * width, bytes_accessed=16 * layers * d_model * width, transcendentals=0),
        name="final_grads",
    )(*operands, t_down, t_up)


def local_step(hidden, targets, w_up, w_down, total_tokens):
    _, _, act_all, g_all, d_all, t_down, t_up, _, _, pg, ph, pa0, pd0 = run_chain(hidden, targets, w_up, w_down, total_tokens)
    grad_down, grad_up = run_final((act_all, pa0, g_all, pg, hidden, ph, d_all, pd0), t_down, t_up)
    return grad_up, grad_down


def solution(mesh):
    def grad_step(hidden_in, targets, w_up, w_down):
        step_fn = functools.partial(local_step, total_tokens=hidden_in.shape[0])
        mapped = jax.shard_map(step_fn, mesh=mesh, in_specs=(P("dp", None), P("dp", None), P(None, None, "tp"), P(None, "tp", None)), out_specs=(P(None, None, "tp"), P(None, "tp", None)), check_vma=False)
        return mapped(hidden_in, targets, w_up, w_down)

    return grad_step
```
